32 devices in a mesh: batch: 2 (over x), col: 4 (over z), row: 4 (over y, core).
Axes of the slice: x: 2, y: 2, z: 4, core: 2. Of those that a mesh axis runs over, the one named last changes fastest.
Arguments:
- x: bfloat16 [32, 1024, 32, 64], P('batch', 'row', 'col'), parts along dimension 0
- w_down_1: bfloat16 [3, 3, 64, 128], replicated
- b_down_1: float32 [128], replicated
- w_conv_1: bfloat16 [3, 3, 128, 128], replicated
- b_conv_1: float32 [128], replicated
- w_proj_1: bfloat16 [64, 128], replicated
- w_down_2: bfloat16 [3, 3, 128, 256], replicated
- b_down_2: float32 [256], replicated
- w_conv_2: bfloat16 [3, 3, 256, 256], replicated
- b_conv_2: float32 [256], replicated
- w_proj_2: bfloat16 [128, 256], replicated
- w_down_3: bfloat16 [3, 3, 256, 320], replicated
- b_down_3: float32 [320], replicated
- w_conv_3: bfloat16 [3, 3, 320, 320], replicated
- b_conv_3: float32 [320], replicated
- w_proj_3: bfloat16 [256, 320], replicated
Outputs:
- output: bfloat16 [32, 128, 4, 320], P('batch', 'row', 'col'), parts along dimension 0
There are 2 independent parts. The reference program is written for one: setup_inputs(seed, part) draws one part's arguments, and reference() takes and returns one part's arrays. A program takes and returns all parts, laid end to end along the dimension named above; an argument that names none is the same for every part.
All inputs are finite; a program needn't handle non-finite values.
Results may differ from the reference program's by a relative error of at most 0.00368202.
Values are sent between devices in bfloat16 or wider.
A program may use at most 1 GiB of HBM per device.

```python
import jax
import jax.numpy as jnp
from jax import lax

IMAGES = 16
TILE_H = 256
TILE_W = 8
ROW_DEVS = 4
COL_DEVS = 4
CHAN_0 = 64
CHAN_1 = 128
CHAN_2 = 256
CHAN_3 = 320
HEIGHT = TILE_H * ROW_DEVS
WIDTH = TILE_W * COL_DEVS
CONV_DIMS = ("NHWC", "HWIO", "NHWC")


def setup_inputs(seed: int = 0, part: int = 0) -> dict:
    root_key = jax.random.key(seed)
    image_key = jax.random.fold_in(jax.random.fold_in(root_key, 1), part)
    inputs = {"x": jax.random.normal(image_key, (IMAGES, HEIGHT, WIDTH, CHAN_0), jnp.float32).astype(jnp.bfloat16)}
    widths = (CHAN_0, CHAN_1, CHAN_2, CHAN_3)
    for stage in range(3):
        c_in = widths[stage]
        c_out = widths[stage + 1]
        stage_keys = jax.random.split(jax.random.fold_in(root_key, 10 + stage), 5)
        suffix = str(stage + 1)
        inputs["w_down_" + suffix] = (jax.random.normal(stage_keys[0], (3, 3, c_in, c_out), jnp.float32) * (9 * c_in) ** -0.5).astype(jnp.bfloat16)
        inputs["b_down_" + suffix] = 0.5 * jax.random.normal(stage_keys[1], (c_out,), jnp.float32)
        inputs["w_conv_" + suffix] = (jax.random.normal(stage_keys[2], (3, 3, c_out, c_out), jnp.float32) * (9 * c_out) ** -0.5).astype(jnp.bfloat16)
        inputs["b_conv_" + suffix] = 0.5 * jax.random.normal(stage_keys[3], (c_out,), jnp.float32)
        inputs["w_proj_" + suffix] = (jax.random.normal(stage_keys[4], (c_in, c_out), jnp.float32) * c_in ** -0.5).astype(jnp.bfloat16)
    return inputs


def conv_same(act_in, weight, stride):
    return lax.conv_general_dilated(act_in.astype(jnp.float32), weight.astype(jnp.float32), (stride, stride), ((1, 1), (1, 1)), dimension_numbers=CONV_DIMS)


def basic_block(z_prev, w_down, b_down, w_conv, b_conv, w_proj):
    y_act = jax.nn.relu(conv_same(z_prev, w_down, 2) + b_down).astype(jnp.bfloat16)
    shortcut = jnp.einsum("bhwc,cd->bhwd", z_prev[:, ::2, ::2].astype(jnp.float32), w_proj.astype(jnp.float32))
    return jax.nn.relu(conv_same(y_act, w_conv, 1) + shortcut + b_conv).astype(jnp.bfloat16)


def reference(x, w_down_1, b_down_1, w_conv_1, b_conv_1, w_proj_1, w_down_2, b_down_2, w_conv_2, b_conv_2, w_proj_2, w_down_3, b_down_3, w_conv_3, b_conv_3, w_proj_3):
    params = ((w_down_1, b_down_1, w_conv_1, b_conv_1, w_proj_1), (w_down_2, b_down_2, w_conv_2, b_conv_2, w_proj_2), (w_down_3, b_down_3, w_conv_3, b_conv_3, w_proj_3))

    def one_image(image):
        act_out = image[None]
        for stage_params in params:
            act_out = basic_block(act_out, stage_params[0], stage_params[1], stage_params[2], stage_params[3], stage_params[4])
        return act_out[0]

    return lax.map(one_image, x)
```

```python
import functools

import jax
import jax.numpy as jnp
from jax import lax
from jax.experimental import pallas as pl
from jax.experimental.pallas import tpu as pltpu
from jax.sharding import PartitionSpec as P

BF16 = jnp.bfloat16
F32 = jnp.float32
SHIFTS = (0, 1)
NCH = 4
NCH3 = 2
PAIRS = 4
MAX_PLAN = 5
OWN, HALO = range(2)
NT = (((1,), (1,)), ((), ()))


def loop(count, body):
    lax.fori_loop(0, count, body, 0)


def row_plan(kind, width, s_send, s_recv):
    if kind == "x":
        own = (0, width - 1)
        need = (-1, width - 1) if s_recv == 0 else (0, width)
        src_at, dst_at = 2 - s_send, 2 - s_recv
    elif kind == "y":
        own = (s_send, width - 1 + s_send)
        need = (s_recv - 1, s_recv + width)
        src_at, dst_at = 2 - s_send, 2 - s_recv
    else:
        own = (s_send, width - 1 + s_send)
        need = (-1, width - 1) if s_recv == 0 else (0, width + 1)
        src_at, dst_at = 3 - 2 * s_send, 3 - 2 * s_recv
    plan = []
    for dist in range(-2, 3):
        lo = max(own[0], width * dist + need[0])
        hi = min(own[1], width * dist + need[1])
        if lo <= hi:
            plan.append((dist, lo + src_at, lo - width * dist + dst_at, hi - lo + 1, False))
        if kind != "x" and s_send == 1 and s_recv == 0 and dist >= 0 and need[0] + width * dist <= 0 <= need[1] + width * dist:
            plan.append((dist, src_at, dst_at - width * dist, 1, True))
    return plan


def kernel(dims, x_hbm, w1d_h, w1c_h, wp1_h, w2d_h, w2c_h, wp2_h, w3d_h, w3c_h, wp3_h, b1d_h, b1c_h, b2d_h, b2c_h, b3d_h, b3c_h, out_hbm,
           raw, xh, stage_f, eye, xs, y1, z1, y2, z2, y3, zo, w1d, w1c, w2d, w2c, w3r, w3d, w3c, wp3r, wp3,
           b1d, b1c, b2d, b2c, b3d, b3c, load_sem, x_sem, col_send, col_recv, row_send, row_recv, out_sem):
    n, h, c0, c1, c2, c3, rows, cols = dims
    h4, h8 = h // 4, h // 8
    ch, ch3 = h4 // NCH, h8 // NCH3
    hh = h // 2
    row = lax.axis_index("row")
    col = lax.axis_index("col")
    s = lax.rem(row, 2)
    is0 = s == 0
    first_extra = (s == 1) & (col == 0)
    last_void = (s == 1) & (col == cols - 1)
    t_first = jnp.where(first_extra, -1, 0)
    fwd_col = jnp.where(is0, col + 1, col - 1)
    bwd_col = jnp.where(is0, col - 1, col + 1)
    has_fwd = (fwd_col >= 0) & (fwd_col < cols)
    has_bwd = (bwd_col >= 0) & (bwd_col < cols)

    load_count = []

    def load(src, dst):
        load_count.append(dst)
        return pltpu.make_async_copy(src, dst, load_sem.at[len(load_count) - 1])

    k1, k2 = 9 * c1, 9 * c2
    pair = 2 * c0
    x_loads = [load(x_hbm.at[:, q], raw.at[q]) for q in range(PAIRS)]
    w1d_loads = [load(b1d_h, b1d), load(b1c_h, b1c)]
    w1c_loads = []
    for p in range(2):
        lanes = pl.ds(p * c1, c1)
        for kh in range(3):
            w1d_loads.append(load(w1d_h.at[kh], w1d.at[pl.ds((kh + 2 * p) * 2 * pair + c0, 3 * c0), lanes]))
        w1c_loads.append(load(w1c_h, w1c.at[pl.ds(p * 3 * c1, k1), lanes]))
        w1c_loads.append(load(wp1_h, w1c.at[pl.ds(12 * c1 + p * pair, c0), lanes]))
    w2d_loads = [load(w2d_h, w2d), load(b2d_h, b2d)]
    w2c_loads = [load(w2c_h, w2c.at[pl.ds(0, k2)]), load(wp2_h, w2c.at[pl.ds(k2, c1)]), load(b2c_h, b2c)]
    w3d_loads = [load(w3d_h, w3r), load(b3d_h, b3d), load(wp3_h, wp3r)]
    w3c_loads = [load(w3c_h, w3c), load(b3c_h, b3c)]
    for copy in x_loads + w1d_loads + w1c_loads + w2d_loads + w2c_loads + w3d_loads + w3c_loads:
        copy.start()

    def row_refs(name, slots, down, side):
        ref = refs[name]
        last = ref.shape[1] - (2 if ROW_SEM[name][0] == "y" else 1)
        own_at, halo_at = (last, 0) if down else (1, last + 1)
        at = own_at if side == OWN else halo_at
        subs = 1 if len(ref.shape) == 4 else ref.shape[2]
        if subs == 1:
            return ref.at[slots, at]
        return ref.at[slots, at, subs - 1 if down else 0]

    refs = dict(x=xs, y1=y1, z1=z1, y2=y2, z2=z2, y3=y3)
    ROW_SEM = {}
    for name, kind, width in (("x", "x", PAIRS), ("y1", "y", PAIRS), ("z1", "z", PAIRS), ("y2", "y", 2), ("z2", "z", 2), ("y3", "y", 1)):
        ROW_SEM[name] = (kind, width, 2 * MAX_PLAN * len(ROW_SEM))

    def directions(name):
        return (True, False) if ROW_SEM[name][0] == "y" else (True,)

    def zero_slot(ref, idx):
        def body(i, carry):
            ref[idx, i] = jnp.zeros(ref.shape[2:], ref.dtype)
            return carry
        loop(ref.shape[1], body)

    for name in ROW_SEM:
        for down in directions(name):
            edge = row_refs(name, slice(None), down, HALO)
            edge[...] = jnp.zeros(edge.shape, BF16)

    @pl.when(col == 0)
    def _():
        for slots, group in enumerate(((xs, y1, z1, y2, z2, y3), (y1, z1, y2, z2, y3), (z1, z2))):
            for ref in group:
                zero_slot(ref, slots)

    @pl.when(col == cols - 1)
    def _():
        for ref in (y1, z1, y2, z2, y3):
            zero_slot(ref, ref.shape[0] - 1)

    @pl.when(is0 | jnp.logical_not(has_bwd))
    def _():
        def body(i, carry):
            xh[0, i] = jnp.zeros((2 * c0, hh), BF16)
            xh[1, i] = jnp.zeros((2 * c0, hh), BF16)
            return carry
        loop(n, body)

    barrier = pltpu.get_barrier_semaphore()
    for rr in range(rows):
        for cc in range(cols):
            pl.semaphore_signal(barrier, inc=1, device_id={"row": jnp.int32(rr), "col": jnp.int32(cc)}, device_id_type=pl.DeviceIdType.MESH)
    pl.semaphore_wait(barrier, rows * cols)

    def remote(src, dst, send_sem, recv_sem, to_row, to_col):
        return pltpu.make_async_remote_copy(src_ref=src, dst_ref=dst, send_sem=send_sem, recv_sem=recv_sem,
                                            device_id={"row": to_row, "col": to_col}, device_id_type=pl.DeviceIdType.MESH)

    def x_copy(shift, half):
        lanes = pl.ds(half * hh, hh)
        if shift == 0:
            src, dst = x_hbm.at[:, 3, pl.ds(c0, c0), lanes], xh.at[half, :, pl.ds(c0, c0)]
        else:
            src, dst = x_hbm.at[:, 0, :, lanes], xh.at[half]
        return remote(src, dst, x_sem.at[half], x_sem.at[2 + half], row, fwd_col)

    for shift in SHIFTS:
        @pl.when(has_fwd & (s == shift))
        def _():
            for half in range(2):
                x_copy(shift, half).start()

    def y_copy(ref, width, rows_per, sem0, forward, chunk, nch):
        to_right = is0 if forward else jnp.logical_not(is0)
        src_slot = jnp.where(to_right, width + 1, 2)
        dst_slot = jnp.where(to_right, 1, width + 2)
        part = pl.ds(1 + chunk * rows_per, rows_per)
        sem = sem0 + (0 if forward else nch) + chunk
        return remote(ref.at[src_slot, part], ref.at[dst_slot, part], col_send.at[sem], col_recv.at[sem], row, fwd_col if forward else bwd_col)

    def y_recv(ref, width, rows_per, sem0, forward, chunk, nch):
        to_right = is0 if forward else jnp.logical_not(is0)
        dst_slot = jnp.where(to_right, 1, width + 2)
        part = pl.ds(1 + chunk * rows_per, rows_per)
        sem = sem0 + (0 if forward else nch) + chunk
        return remote(ref.at[dst_slot, part], ref.at[dst_slot, part], col_send.at[sem], col_recv.at[sem], row, bwd_col if forward else fwd_col)

    def z_copy(ref, width, rows_per, sem0, chunk):
        src_slot = jnp.where(is0, width + 2, 2)
        dst_slot = jnp.where(is0, 2, width + 2)
        part = pl.ds(1 + chunk * rows_per, rows_per)
        sem = sem0 + chunk
        return remote(ref.at[src_slot, part], ref.at[dst_slot, part], col_send.at[sem], col_recv.at[sem], row, fwd_col)

    def z_recv(ref, width, rows_per, sem0, chunk):
        dst_slot = jnp.where(is0, 2, width + 2)
        part = pl.ds(1 + chunk * rows_per, rows_per)
        sem = sem0 + chunk
        return remote(ref.at[dst_slot, part], ref.at[dst_slot, part], col_send.at[sem], col_recv.at[sem], row, bwd_col)

    SEM_Y1, SEM_Z1, SEM_Y2, SEM_Z2, SEM_Y3 = (i * 2 * NCH for i in range(5))

    def row_messages(name, act):
        kind, width, sem0 = ROW_SEM[name]
        for down in directions(name):
            for s_send, s_recv in zip(SHIFTS, reversed(SHIFTS)):
                step = 1 if down else -1
                for i, (dist, src, dst, count, extra) in enumerate(row_plan(kind, width, s_send, s_recv)):
                    sem = sem0 + i + (0 if down else MAX_PLAN)
                    if act == "recv":
                        from_row, from_col = row - step, col - dist
                        ok = (s == s_recv) & (from_row >= 0) & (from_row < rows) & (from_col >= 0) & (from_col < cols)
                        if extra:
                            ok = ok & (from_col == 0)

                        @pl.when(ok)
                        def _():
                            ref = row_refs(name, pl.ds(dst, count), down, HALO)
                            remote(ref, ref, row_send.at[sem], row_recv.at[sem], from_row, from_col).wait_recv()
                    else:
                        to_row, to_col = row + step, col + dist
                        ok = (s == s_send) & (to_row >= 0) & (to_row < rows) & (to_col >= 0) & (to_col < cols)
                        if extra:
                            ok = ok & (col == 0)

                        @pl.when(ok)
                        def _():
                            copy = remote(row_refs(name, pl.ds(src, count), down, OWN), row_refs(name, pl.ds(dst, count), down, HALO),
                                          row_send.at[sem], row_recv.at[sem], to_row, to_col)
                            if act == "send":
                                copy.start()
                            else:
                                copy.wait_send()

    eye[...] = (lax.broadcasted_iota(jnp.int32, (h, h), 0) == lax.broadcasted_iota(jnp.int32, (h, h), 1)).astype(F32).astype(BF16)

    def transpose_pair(read, size, slot, h4_first):
        unit = eye[0:size, 0:size]

        def turn(i, carry):
            block = read(2 * i).reshape(2 * pair, size)
            turned = lax.dot_general(unit, block, NT, preferred_element_type=F32)
            for j in range(2):
                stage_f[pl.ds(2 * i + j, size, stride=n), :] = turned[:, j * pair:(j + 1) * pair]
            return carry
        loop(n // 2, turn)
        step = 4

        def pack(i, carry):
            part = stage_f[pl.ds(i * (step * 4 * n), step * 4 * n), :]
            xs[slot, pl.ds(h4_first + i * step, step)] = part.reshape(step, 4, n, 2 * c0).astype(BF16)
            return carry
        loop(size // 4 // step, pack)

    def zero_part(ref, first, size, p):
        ref[pl.ds(first, size), pl.ds(p * c1, c1)] = jnp.zeros((size, c1), BF16)

    def zero_weights():
        for p in range(2):
            for kh in range(5):
                tap_at = kh * 2 * pair
                used = 2 * p <= kh < 2 * p + 3
                zero_part(w1d, tap_at, c0 if used else 2 * pair, p)
            zero_part(w1c, (1 - p) * k1, 3 * c1, p)
            proj_at = 12 * c1
            zero_part(w1c, proj_at + (1 - p) * pair, pair, p)
            zero_part(w1c, proj_at + p * pair + c0, c0, p)

    zero_weights()
    for q in range(4):
        x_loads[q].wait()

    def own_pair(q, carry):
        transpose_pair(lambda i: raw[q, pl.ds(i, 2)], h, q + 2 - s, 1)
        return carry
    loop(4, own_pair)
    row_messages("x", "send")
    for copy in w1d_loads:
        copy.wait()

    def flat(value):
        return value.reshape(value.shape[0] * n, value.shape[-1])

    def dot(lhs, rhs):
        return jnp.dot(lhs, rhs, preferred_element_type=F32)

    def own_col(t, width):
        return jnp.where(is0, width - 1 - t, t)

    def phase(width, nch, item):
        def body(at, carry):
            item(lax.div(at, nch) - 1, lax.rem(at, nch))
            return carry
        lax.fori_loop((t_first + 1) * nch, (width + 1) * nch, body, 0)

    def y1_item(t, i):
        c = jnp.where(t < 3, lax.rem(i + 1, NCH), i)
        k = own_col(t, 4)

        @pl.when((t == t_first) & (i == NCH - 1))
        def _():
            row_messages("x", "recv")

        @pl.when((t == 3) & (lax.rem(i, NCH // 2) == 0))
        def _():
            half = lax.div(i, NCH // 2)
            for shift in SHIFTS:
                @pl.when(has_bwd & (s == shift))
                def _():
                    ref = xh.at[half, :, pl.ds(c0, c0)] if shift == 0 else xh.at[half]
                    remote(ref, ref, x_sem.at[half], x_sem.at[2 + half], row, bwd_col).wait_recv()
            transpose_pair(lambda j: xh[half, pl.ds(j, 2)], hh, jnp.where(is0, 1, 5), 1 + half * (h4 // 2))

        at = 1 + c * ch
        taps = []
        for kh in range(5):
            first, sub = (at - 1, 3) if kh == 0 else (at, kh - 1)
            for side in (1, 2):
                taps.append(flat(xs[k + side, pl.ds(first, ch), sub]))
        acc = dot(jnp.concatenate(taps, axis=1), w1d[...])
        void = last_void & (t == 3)
        for p in range(2):
            val = jnp.maximum(acc[:, p * c1:(p + 1) * c1] + b1d[...], 0.0)
            val = jnp.where(void, 0.0, val)
            y1[k + 2, pl.ds(at, ch), p] = val.astype(BF16).reshape(ch, n, c1)

        @pl.when((t == 0) & has_fwd)
        def _():
            y_copy(y1, PAIRS, ch, SEM_Y1, True, c, NCH).start()

        @pl.when((t == 3) & has_bwd)
        def _():
            y_copy(y1, PAIRS, ch, SEM_Y1, False, c, NCH).start()
    phase(PAIRS, NCH, y1_item)
    row_messages("y1", "send")
    for copy in w1c_loads:
        copy.wait()

    def wait_halo(ref, width, rows_per, sem0, forward, c, nch):
        exists = has_bwd if forward else has_fwd

        @pl.when(exists & (c == 0))
        def _():
            y_recv(ref, width, rows_per, sem0, forward, 0, nch).wait_recv()

        @pl.when(exists & (c < nch - 1))
        def _():
            y_recv(ref, width, rows_per, sem0, forward, c + 1, nch).wait_recv()

    def z1_item(o, i):
        t = jnp.where(o < 0, o, jnp.where(o == 3, o, lax.rem(o + 1, 3)))
        mid = jnp.where(i < NCH - 2, i + 1, jnp.where(i == NCH - 2, 0, NCH - 1))
        c = jnp.where(o < 2, mid, i)
        k = own_col(t, 4)

        @pl.when((o == t_first) & (i == NCH - 2))
        def _():
            row_messages("y1", "recv")

        @pl.when(t == 0)
        def _():
            wait_halo(y1, PAIRS, ch, SEM_Y1, False, c, NCH)

        @pl.when(t == 3)
        def _():
            wait_halo(y1, PAIRS, ch, SEM_Y1, True, c, NCH)

        at = 1 + c * ch
        taps = []
        for first, sub in ((at - 1, 1), (at, 0), (at, 1), (at + 1, 0)):
            for side in (1, 2, 3):
                taps.append(flat(y1[k + side, pl.ds(first, ch), sub]))
        for sub in (0, 2):
            taps.append(flat(xs[k + 2, pl.ds(at, ch), sub]))
        acc = dot(jnp.concatenate(taps, axis=1), w1c[...])
        for p in range(2):
            val = jnp.maximum(acc[:, p * c1:(p + 1) * c1] + b1c[...], 0.0)
            z1[k + 3 - s, pl.ds(at, ch), p] = val.astype(BF16).reshape(ch, n, c1)

        @pl.when((t == 0) & has_fwd)
        def _():
            z_copy(z1, PAIRS, ch, SEM_Z1, c).start()
    phase(PAIRS, NCH, z1_item)
    row_messages("z1", "send")
    for copy in w2d_loads + w3d_loads:
        copy.wait()

    def turn_weight(i, carry):
        turned = lax.dot_general(eye[0:c2, 0:c2], w3r[i], NT, preferred_element_type=F32)
        w3d[i] = turned.astype(BF16)
        return carry
    loop(9, turn_weight)
    wp3[...] = lax.dot_general(eye[0:c2, 0:c2], wp3r[...], NT, preferred_element_type=F32).astype(BF16)

    def y2_item(t, i):
        c = jnp.where(t < 1, lax.rem(i + 1, NCH), i)
        k = own_col(t, 2)

        @pl.when((t == t_first) & (i == NCH - 1))
        def _():
            row_messages("z1", "recv")

        @pl.when((t == 1) & has_bwd)
        def _():
            z_recv(z1, PAIRS, ch, SEM_Z1, c).wait_recv()

        at = 1 + c * ch
        taps = []
        for first, sub in ((at - 1, 1), (at, 0), (at, 1)):
            for side in range(3):
                taps.append(flat(z1[2 * k + 2 + side, pl.ds(first, ch), sub]))
        acc = dot(jnp.concatenate(taps, axis=1), w2d[...])
        val = jnp.maximum(acc + b2d[...], 0.0)
        val = jnp.where(last_void & (t == 1), 0.0, val)
        y2[k + 2, pl.ds(at, ch)] = val.astype(BF16).reshape(ch, n, c2)

        @pl.when((t == 0) & has_fwd)
        def _():
            y_copy(y2, 2, ch, SEM_Y2, True, c, NCH).start()

        @pl.when((t == 1) & has_bwd)
        def _():
            y_copy(y2, 2, ch, SEM_Y2, False, c, NCH).start()
    phase(2, NCH, y2_item)
    row_messages("y2", "send")
    for copy in w2c_loads:
        copy.wait()

    def z2_item(t, c):
        k = own_col(t, 2)

        @pl.when((t == t_first) & (c == 0))
        def _():
            row_messages("y2", "recv")

        @pl.when(t == 0)
        def _():
            wait_halo(y2, 2, ch, SEM_Y2, False, c, NCH)

        @pl.when(t == 1)
        def _():
            wait_halo(y2, 2, ch, SEM_Y2, True, c, NCH)

        at = 1 + c * ch
        taps = []
        for first in (at - 1, at, at + 1):
            for side in (1, 2, 3):
                taps.append(flat(y2[k + side, pl.ds(first, ch)]))
        taps.append(flat(z1[2 * k + 3, pl.ds(at, ch), 0]))
        acc = dot(jnp.concatenate(taps, axis=1), w2c[...])
        val = jnp.maximum(acc + b2c[...], 0.0).astype(BF16).reshape(ch // 2, 2, n, c2)
        z2[k + 3 - s, pl.ds(1 + c * (ch // 2), ch // 2)] = val

        @pl.when((t == 0) & has_fwd)
        def _():
            z_copy(z2, 2, ch // 2, SEM_Z2, c).start()
    phase(2, NCH, z2_item)
    row_messages("z2", "send")

    def y3_item(t, c):
        k = t

        @pl.when((t == t_first) & (c == 0))
        def _():
            row_messages("z2", "recv")

        @pl.when((t == 0) & has_bwd)
        def _():
            for j in range(NCH // NCH3):
                z_recv(z2, 2, ch // 2, SEM_Z2, c * (NCH // NCH3) + j).wait_recv()

        at = 1 + c * ch3
        acc = jnp.zeros((ch3 * n, c3), F32)
        tap = 0
        for first, sub in ((at - 1, 1), (at, 0), (at, 1)):
            for side in range(3):
                acc = acc + dot(flat(z2[2 * k + 2 + side, pl.ds(first, ch3), sub]), w3d[tap])
                tap += 1
        val = jnp.maximum(acc + b3d[...], 0.0)
        val = jnp.where(last_void & (t == 0), 0.0, val)
        y3[k + 2, pl.ds(at, ch3)] = val.astype(BF16).reshape(ch3, n, c3)

        @pl.when((t == 0) & has_fwd)
        def _():
            y_copy(y3, 1, ch3, SEM_Y3, True, c, NCH3).start()

        @pl.when((t == 0) & has_bwd)
        def _():
            y_copy(y3, 1, ch3, SEM_Y3, False, c, NCH3).start()
    phase(1, NCH3, y3_item)
    row_messages("y3", "send")
    for copy in w3c_loads:
        copy.wait()

    ships = (s == 1) & has_bwd

    def ship(c):
        part = pl.ds(c * ch3, ch3)
        return remote(zo.at[1, part], out_hbm.at[part], out_sem.at[c], out_sem.at[NCH3 + c], row, bwd_col)

    def ship_recv(c):
        part = pl.ds(c * ch3, ch3)
        return remote(zo.at[1, part], out_hbm.at[part], out_sem.at[c], out_sem.at[NCH3 + c], row, fwd_col)

    keep = jnp.where(is0, 1, 0)

    def put(c):
        part = pl.ds(c * ch3, ch3)
        return pltpu.make_async_copy(zo.at[keep, part], out_hbm.at[part], out_sem.at[2 * NCH3 + c])

    def z3_item(t, c):
        k = t

        @pl.when((t == t_first) & (c == 0))
        def _():
            row_messages("y3", "recv")

        @pl.when(t == 0)
        def _():
            wait_halo(y3, 1, ch3, SEM_Y3, False, c, NCH3)
            wait_halo(y3, 1, ch3, SEM_Y3, True, c, NCH3)

        at = 1 + c * ch3
        acc = dot(flat(z2[2 * k + 3, pl.ds(at, ch3), 0]), wp3[...])
        tap = 0
        for first in (at - 1, at, at + 1):
            for side in (1, 2, 3):
                acc = acc + dot(flat(y3[k + side, pl.ds(first, ch3)]), w3c[tap])
                tap += 1
        val = jnp.maximum(acc + b3c[...], 0.0)
        zo[k + 1, pl.ds(c * ch3, ch3)] = val.astype(BF16).reshape(ch3, n, c3)

        @pl.when((t == 0) & ships)
        def _():
            ship(c).start()

        @pl.when(((t == 0) & is0) | (t == -1))
        def _():
            put(c).start()
    phase(1, NCH3, z3_item)

    for shift in SHIFTS:
        @pl.when(has_fwd & (s == shift))
        def _():
            for half in range(2):
                x_copy(shift, half).wait_send()

    def drain(c, carry):
        @pl.when(has_fwd)
        def _():
            y_copy(y1, PAIRS, ch, SEM_Y1, True, c, NCH).wait_send()
            z_copy(z1, PAIRS, ch, SEM_Z1, c).wait_send()
            y_copy(y2, 2, ch, SEM_Y2, True, c, NCH).wait_send()
            z_copy(z2, 2, ch // 2, SEM_Z2, c).wait_send()

        @pl.when(has_bwd)
        def _():
            y_copy(y1, PAIRS, ch, SEM_Y1, False, c, NCH).wait_send()
            y_copy(y2, 2, ch, SEM_Y2, False, c, NCH).wait_send()
        return carry
    loop(NCH, drain)

    def drain3(c, carry):
        @pl.when(has_fwd)
        def _():
            y_copy(y3, 1, ch3, SEM_Y3, True, c, NCH3).wait_send()

        @pl.when(has_bwd)
        def _():
            y_copy(y3, 1, ch3, SEM_Y3, False, c, NCH3).wait_send()

        @pl.when(ships)
        def _():
            ship(c).wait_send()

        @pl.when((s == 1) & has_fwd)
        def _():
            ship_recv(c).wait_recv()

        @pl.when(is0 | first_extra)
        def _():
            put(c).wait()
        return carry
    loop(NCH3, drain3)
    for name in ROW_SEM:
        row_messages(name, "sent")


def solution(mesh):
    rows = mesh.shape["row"]
    cols = mesh.shape["col"]
    tile_spec = P("batch", "row", "col")

    def local_blocks(x, w1d, b1d, w1c, b1c, wp1, w2d, b2d, w2c, b2c, wp2, w3d, b3d, w3c, b3c, wp3):
        n, h, w, c0 = x.shape
        c1, c2, c3 = w1d.shape[3], w2d.shape[3], w3d.shape[3]
        h4, h8 = h // 4, h // 8
        dims = (n, h, c0, c1, c2, c3, rows, cols)
        pair = 2 * c0
        xt = jnp.moveaxis(x, 1, 3).reshape(n, PAIRS, pair, h)
        args = (xt, w1d.reshape(3, 3 * c0, c1), w1c.reshape(9 * c1, c1), wp1, w2d.reshape(9 * c1, c2), w2c.reshape(9 * c2, c2), wp2,
                jnp.swapaxes(w3d.reshape(9, c2, c3), 1, 2), w3c.reshape(9, c3, c3), wp3.T,
                *(bias.reshape(1, -1) for bias in (b1d, b1c, b2d, b2c, b3d, b3c)))
        vm = pltpu.VMEM
        dma = pltpu.SemaphoreType.DMA
        flops = 2 * n * h * w * c1 * 7 * (c0 + c1)
        out = pl.pallas_call(
            functools.partial(kernel, dims),
            out_shape=jax.ShapeDtypeStruct((h8, n, c3), BF16),
            in_specs=[pl.BlockSpec(memory_space=pl.ANY)] * len(args),
            out_specs=pl.BlockSpec(memory_space=pl.ANY),
            scratch_shapes=[
                vm((PAIRS, n, pair, h), BF16), vm((2, n, pair, h // 2), BF16), vm((h * n, pair), F32), vm((h, h), BF16),
                vm((6, h4 + 1, 4, n, pair), BF16), vm((7, h4 + 2, 2, n, c1), BF16), vm((7, h4 + 1, 2, n, c1), BF16),
                vm((5, h4 + 2, n, c2), BF16), vm((5, h8 + 1, 2, n, c2), BF16), vm((4, h8 + 2, n, c3), BF16), vm((2, h8, n, c3), BF16),
                vm((10 * pair, 2 * c1), BF16), vm((12 * c1 + 2 * pair, 2 * c1), BF16), vm((9 * c1, c2), BF16), vm((9 * c2 + c1, c2), BF16),
                vm((9, c3, c2), BF16), vm((9, c2, c3), BF16), vm((9, c3, c3), BF16), vm((c3, c2), BF16), vm((c2, c3), BF16),
            ] + [vm((1, width), F32) for width in (c1, c1, c2, c2, c3, c3)] + [
                dma((count,)) for count in (32, 4, 10 * NCH, 10 * NCH, 12 * MAX_PLAN, 12 * MAX_PLAN, 3 * NCH3)],
            compiler_params=pltpu.CompilerParams(collective_id=0, has_side_effects=True, vmem_limit_bytes=63 * 1024 * 1024),
            cost_estimate=pl.CostEstimate(flops=flops, bytes_accessed=16 * 1024 * 1024, transcendentals=0),
        )(*args)
        return jnp.swapaxes(out, 0, 1).reshape(n, h8, 1, c3)

    return jax.shard_map(local_blocks, mesh=mesh, in_specs=(tile_spec,) + (P(),) * 15, out_specs=tile_spec, check_vma=False)
```

```python
import functools

import jax
import jax.numpy as jnp
from jax import lax
from jax.experimental import pallas as pl
from jax.experimental.pallas import tpu as pltpu
from jax.sharding import PartitionSpec as P

BF16 = jnp.bfloat16
F32 = jnp.float32
SHIFTS = (0, 1)
NCH = 4
NCH3 = 2
PAIRS = 4
MAX_PLAN = 5
BLOCK = 16
UNROLL = 4
OWN, HALO = range(2)
NT = (((1,), (1,)), ((), ()))


def loop(count, body):
    lax.fori_loop(0, count, body, 0)


def row_plan(kind, width, s_send, s_recv):
    if kind == "x":
        own = (0, width - 1)
        need = (-1, width - 1) if s_recv == 0 else (0, width)
        src_at, dst_at = 2 - s_send, 2 - s_recv
    elif kind == "y":
        own = (s_send, width - 1 + s_send)
        need = (s_recv - 1, s_recv + width)
        src_at, dst_at = 2 - s_send, 2 - s_recv
    else:
        own = (s_send, width - 1 + s_send)
        need = (-1, width - 1) if s_recv == 0 else (0, width + 1)
        src_at, dst_at = 3 - 2 * s_send, 3 - 2 * s_recv
    plan = []
    for dist in range(-2, 3):
        lo = max(own[0], width * dist + need[0])
        hi = min(own[1], width * dist + need[1])
        if lo <= hi:
            plan.append((dist, lo + src_at, lo - width * dist + dst_at, hi - lo + 1, False))
        if kind != "x" and s_send == 1 and s_recv == 0 and dist >= 0 and need[0] + width * dist <= 0 <= need[1] + width * dist:
            plan.append((dist, src_at, dst_at - width * dist, 1, True))
    return plan


def kernel(dims, x_hbm, w1d_h, w1c_h, wp1_h, w2d_h, w2c_h, wp2_h, w3d_h, w3c_h, wp3_h, b1d_h, b1c_h, b2d_h, b2c_h, b3d_h, b3c_h, out_hbm,
           raw, xh, turned, eye, mix, xs, y1, z1, y2, z2, y3, zo, w1d, w1c, w2d, w2c, w3r, w3d, w3c, wp3r, wp3,
           b1d, b1c, b2d, b2c, b3d, b3c, load_sem, x_sem, col_send, col_recv, row_send, row_recv, out_sem):
    n, h, c0, c1, c2, c3, rows, cols = dims
    h4, h8 = h // 4, h // 8
    ch, ch3 = h4 // NCH, h8 // NCH3
    hh = h // 2
    row = lax.axis_index("row")
    col = lax.axis_index("col")
    s = lax.rem(row, 2)
    is0 = s == 0
    first_extra = (s == 1) & (col == 0)
    last_void = (s == 1) & (col == cols - 1)
    t_first = jnp.where(first_extra, -1, 0)
    fwd_col = jnp.where(is0, col + 1, col - 1)
    bwd_col = jnp.where(is0, col - 1, col + 1)
    has_fwd = (fwd_col >= 0) & (fwd_col < cols)
    has_bwd = (bwd_col >= 0) & (bwd_col < cols)

    load_count = []

    def load(src, dst):
        load_count.append(dst)
        return pltpu.make_async_copy(src, dst, load_sem.at[len(load_count) - 1])

    k1, k2 = 9 * c1, 9 * c2
    pair = 2 * c0
    x_loads = [load(x_hbm.at[:, q], raw.at[q]) for q in range(PAIRS)]
    w1d_loads = [load(b1d_h, b1d.at[0]), load(b1c_h, b1c.at[0])]
    w1c_loads = []
    for p in range(2):
        lanes = pl.ds(p * c1, c1)
        for kh in range(3):
            w1d_loads.append(load(w1d_h.at[kh], w1d.at[pl.ds((kh + 2 * p) * 2 * pair + c0, 3 * c0), lanes]))
        w1c_loads.append(load(w1c_h, w1c.at[pl.ds(p * 3 * c1, k1), lanes]))
        w1c_loads.append(load(wp1_h, w1c.at[pl.ds(12 * c1 + p * pair, c0), lanes]))
    w2d_loads = [load(w2d_h, w2d), load(b2d_h, b2d.at[0])]
    w2c_loads = [load(w2c_h, w2c.at[pl.ds(0, k2)]), load(wp2_h, w2c.at[pl.ds(k2, c1)]), load(b2c_h, b2c.at[0])]
    w3d_loads = [load(w3d_h, w3r), load(b3d_h, b3d.at[0]), load(wp3_h, wp3r)]
    w3c_loads = [load(w3c_h, w3c), load(b3c_h, b3c.at[0])]
    for copy in x_loads + w1d_loads + w1c_loads + w2d_loads + w2c_loads + w3d_loads + w3c_loads:
        copy.start()

    def row_refs(name, slots, down, side):
        ref = refs[name]
        last = ref.shape[1] - (2 if ROW_SEM[name][0] == "y" else 1)
        own_at, halo_at = (last, 0) if down else (1, last + 1)
        at = own_at if side == OWN else halo_at
        subs = 1 if len(ref.shape) == 4 else ref.shape[2]
        if subs == 1:
            return ref.at[slots, at]
        return ref.at[slots, at, subs - 1 if down else 0]

    refs = dict(x=xs, y1=y1, z1=z1, y2=y2, z2=z2, y3=y3)
    ROW_SEM = {}
    for name, kind, width in (("x", "x", PAIRS), ("y1", "y", PAIRS), ("z1", "z", PAIRS), ("y2", "y", 2), ("z2", "z", 2), ("y3", "y", 1)):
        ROW_SEM[name] = (kind, width, 2 * MAX_PLAN * len(ROW_SEM))

    def directions(name):
        return (True, False) if ROW_SEM[name][0] == "y" else (True,)

    def dot(lhs, rhs):
        return jnp.dot(lhs, rhs, preferred_element_type=F32)

    def zero_slot(ref, idx):
        def body(i, carry):
            ref[idx, i] = jnp.zeros(ref.shape[2:], ref.dtype)
            return carry
        loop(ref.shape[1], body)

    for name in ROW_SEM:
        for down in directions(name):
            edge = row_refs(name, slice(None), down, HALO)
            edge[...] = jnp.zeros(edge.shape, BF16)

    @pl.when(col == 0)
    def _():
        for slots, group in enumerate(((xs, y1, z1, y2, z2, y3), (y1, z1, y2, z2, y3), (z1, z2))):
            for ref in group:
                zero_slot(ref, slots)

    @pl.when(col == cols - 1)
    def _():
        for ref in (y1, z1, y2, z2, y3):
            zero_slot(ref, ref.shape[0] - 1)

    @pl.when(is0 | jnp.logical_not(has_bwd))
    def _():
        def body(i, carry):
            xh[0, i] = jnp.zeros((2 * c0, hh), BF16)
            xh[1, i] = jnp.zeros((2 * c0, hh), BF16)
            return carry
        loop(n, body)

    barrier = pltpu.get_barrier_semaphore()
    for rr in range(rows):
        for cc in range(cols):
            pl.semaphore_signal(barrier, inc=1, device_id={"row": jnp.int32(rr), "col": jnp.int32(cc)}, device_id_type=pl.DeviceIdType.MESH)
    pl.semaphore_wait(barrier, rows * cols)

    def remote(src, dst, send_sem, recv_sem, to_row, to_col):
        return pltpu.make_async_remote_copy(src_ref=src, dst_ref=dst, send_sem=send_sem, recv_sem=recv_sem,
                                            device_id={"row": to_row, "col": to_col}, device_id_type=pl.DeviceIdType.MESH)

    def x_copy(shift, half):
        lanes = pl.ds(half * hh, hh)
        if shift == 0:
            src, dst = x_hbm.at[:, 3, pl.ds(c0, c0), lanes], xh.at[half, :, pl.ds(c0, c0)]
        else:
            src, dst = x_hbm.at[:, 0, :, lanes], xh.at[half]
        return remote(src, dst, x_sem.at[half], x_sem.at[2 + half], row, fwd_col)

    for shift in SHIFTS:
        @pl.when(has_fwd & (s == shift))
        def _():
            for half in range(2):
                x_copy(shift, half).start()

    def y_copy(ref, width, rows_per, sem0, forward, chunk, nch):
        to_right = is0 if forward else jnp.logical_not(is0)
        src_slot = jnp.where(to_right, width + 1, 2)
        dst_slot = jnp.where(to_right, 1, width + 2)
        part = pl.ds(1 + chunk * rows_per, rows_per)
        sem = sem0 + (0 if forward else nch) + chunk
        return remote(ref.at[src_slot, part], ref.at[dst_slot, part], col_send.at[sem], col_recv.at[sem], row, fwd_col if forward else bwd_col)

    def y_recv(ref, width, rows_per, sem0, forward, chunk, nch):
        to_right = is0 if forward else jnp.logical_not(is0)
        dst_slot = jnp.where(to_right, 1, width + 2)
        part = pl.ds(1 + chunk * rows_per, rows_per)
        sem = sem0 + (0 if forward else nch) + chunk
        return remote(ref.at[dst_slot, part], ref.at[dst_slot, part], col_send.at[sem], col_recv.at[sem], row, bwd_col if forward else fwd_col)

    def z_copy(ref, width, rows_per, sem0, chunk):
        src_slot = jnp.where(is0, width + 2, 2)
        dst_slot = jnp.where(is0, 2, width + 2)
        part = pl.ds(1 + chunk * rows_per, rows_per)
        sem = sem0 + chunk
        return remote(ref.at[src_slot, part], ref.at[dst_slot, part], col_send.at[sem], col_recv.at[sem], row, fwd_col)

    def z_recv(ref, width, rows_per, sem0, chunk):
        dst_slot = jnp.where(is0, 2, width + 2)
        part = pl.ds(1 + chunk * rows_per, rows_per)
        sem = sem0 + chunk
        return remote(ref.at[dst_slot, part], ref.at[dst_slot, part], col_send.at[sem], col_recv.at[sem], row, bwd_col)

    SEM_Y1, SEM_Z1, SEM_Y2, SEM_Z2, SEM_Y3 = (i * 2 * NCH for i in range(5))

    def row_messages(name, act):
        kind, width, sem0 = ROW_SEM[name]
        for down in directions(name):
            for s_send, s_recv in zip(SHIFTS, reversed(SHIFTS)):
                step = 1 if down else -1
                for i, (dist, src, dst, count, extra) in enumerate(row_plan(kind, width, s_send, s_recv)):
                    sem = sem0 + i + (0 if down else MAX_PLAN)
                    if act == "recv":
                        from_row, from_col = row - step, col - dist
                        ok = (s == s_recv) & (from_row >= 0) & (from_row < rows) & (from_col >= 0) & (from_col < cols)
                        if extra:
                            ok = ok & (from_col == 0)

                        @pl.when(ok)
                        def _():
                            ref = row_refs(name, pl.ds(dst, count), down, HALO)
                            remote(ref, ref, row_send.at[sem], row_recv.at[sem], from_row, from_col).wait_recv()
                    else:
                        to_row, to_col = row + step, col + dist
                        ok = (s == s_send) & (to_row >= 0) & (to_row < rows) & (to_col >= 0) & (to_col < cols)
                        if extra:
                            ok = ok & (col == 0)

                        @pl.when(ok)
                        def _():
                            copy = remote(row_refs(name, pl.ds(src, count), down, OWN), row_refs(name, pl.ds(dst, count), down, HALO),
                                          row_send.at[sem], row_recv.at[sem], to_row, to_col)
                            if act == "send":
                                copy.start()
                            else:
                                copy.wait_send()

    def unit_where(size, source):
        at = lax.broadcasted_iota(jnp.int32, (size, size), 0)
        return (at == source(lax.broadcasted_iota(jnp.int32, (size, size), 1))).astype(F32).astype(BF16)

    eye[...] = unit_where(h, lambda at: at)
    mix[...] = unit_where(n * BLOCK, lambda at: (at & (BLOCK - 1)) * n + (at >> BLOCK.bit_length() - 1))

    def to_rows(value):
        return value.astype(BF16).reshape(BLOCK // 4, 4, n, pair)

    def turn_group(q):
        def turn(i, carry):
            for j in range(UNROLL):
                at = i * UNROLL + j
                block = raw[pl.ds(q, 2), at].reshape(2 * pair, h)
                turned[at] = lax.dot_general(eye[...], block, NT, preferred_element_type=F32).astype(BF16)
            return carry
        loop(n // UNROLL, turn)

        def place(i, carry):
            for j in range(UNROLL):
                at = i * UNROLL + j
                block = turned[:, pl.ds(at * BLOCK, BLOCK), :].reshape(n * BLOCK, 2 * pair)
                moved = dot(mix[...], block)
                for side in range(2):
                    xs[q + 2 - s + side, pl.ds(1 + at * (BLOCK // 4), BLOCK // 4)] = to_rows(moved[:, side * pair:(side + 1) * pair])
            return carry
        loop(h // BLOCK // UNROLL, place)

    def turn_halo(half):
        slot = jnp.where(is0, 1, PAIRS + 1)
        unit = eye[:hh, :hh]

        def turn(i, carry):
            for j in range(UNROLL):
                at = 2 * (i * UNROLL + j)
                block = xh[half, pl.ds(at, 2)].reshape(2 * pair, hh)
                both = lax.dot_general(unit, block, NT, preferred_element_type=F32).astype(BF16)
                for side in range(2):
                    turned[at + side, :hh, :pair] = both[:, side * pair:(side + 1) * pair]
            return carry
        loop(n // 2 // UNROLL, turn)

        def place(i, carry):
            blocks = [turned[:, pl.ds((2 * i + j) * BLOCK, BLOCK), :pair].reshape(n * BLOCK, pair) for j in range(2)]
            moved = dot(mix[...], jnp.concatenate(blocks, axis=1))
            for j in range(2):
                first = 1 + half * (h4 // 2) + (2 * i + j) * (BLOCK // 4)
                xs[slot, pl.ds(first, BLOCK // 4)] = to_rows(moved[:, j * pair:(j + 1) * pair])
            return carry
        loop(hh // BLOCK // 2, place)

    def zero_part(ref, first, size, p):
        ref[pl.ds(first, size), pl.ds(p * c1, c1)] = jnp.zeros((size, c1), BF16)

    def zero_weights():
        for p in range(2):
            for kh in range(5):
                tap_at = kh * 2 * pair
                used = 2 * p <= kh < 2 * p + 3
                zero_part(w1d, tap_at, c0 if used else 2 * pair, p)
            zero_part(w1c, (1 - p) * k1, 3 * c1, p)
            proj_at = 12 * c1
            zero_part(w1c, proj_at + (1 - p) * pair, pair, p)
            zero_part(w1c, proj_at + p * pair + c0, c0, p)

    zero_weights()
    for copy in x_loads + w1d_loads:
        copy.wait()

    def flat(value):
        return value.reshape(value.shape[0] * n, value.shape[-1])

    def own_col(t, width):
        return jnp.where(is0, width - 1 - t, t)

    def phase(width, nch, item):
        def body(at, carry):
            item(lax.div(at, nch) - 1, lax.rem(at, nch))
            return carry
        lax.fori_loop((t_first + 1) * nch, (width + 1) * nch, body, 0)

    def y1_item(at, carry):
        early = 3 - t_first
        t = jnp.where(at < 3 * early, lax.div(at, 3) + t_first, at - 3 * early + t_first)
        t = jnp.where(at < NCH * early, t, 3)
        c = jnp.where(at < 3 * early, lax.rem(at, 3) + 1, jnp.where(t < 3, 0, at - NCH * early))
        k = own_col(t, PAIRS)

        @pl.when((at == 0) | (t == 1) & (c == 1))
        def _():
            turn_group(2 * jnp.where(is0 == (t < 1), 1, 0))

        @pl.when((t == 1) & (c == 1))
        def _():
            row_messages("x", "send")

        @pl.when(at == 3 * early)
        def _():
            row_messages("x", "recv")

        @pl.when((t == 3) & (lax.rem(c, NCH // 2) == 0))
        def _():
            half = lax.div(c, NCH // 2)
            for shift in SHIFTS:
                @pl.when(has_bwd & (s == shift))
                def _():
                    ref = xh.at[half, :, pl.ds(c0, c0)] if shift == 0 else xh.at[half]
                    remote(ref, ref, x_sem.at[half], x_sem.at[2 + half], row, bwd_col).wait_recv()
            turn_halo(half)

        at = 1 + c * ch
        taps = []
        for kh in range(5):
            first, sub = (at - 1, 3) if kh == 0 else (at, kh - 1)
            for side in (1, 2):
                taps.append(flat(xs[k + side, pl.ds(first, ch), sub]))
        acc = dot(jnp.concatenate(taps, axis=1), w1d[...])
        void = last_void & (t == 3)
        for p in range(2):
            val = jnp.maximum(acc[:, p * c1:(p + 1) * c1] + b1d[...], 0.0)
            val = jnp.where(void, 0.0, val)
            y1[k + 2, pl.ds(at, ch), p] = val.astype(BF16).reshape(ch, n, c1)

        @pl.when((t == 0) & has_fwd)
        def _():
            y_copy(y1, PAIRS, ch, SEM_Y1, True, c, NCH).start()

        @pl.when((t == 3) & has_bwd)
        def _():
            y_copy(y1, PAIRS, ch, SEM_Y1, False, c, NCH).start()
        return carry
    lax.fori_loop(0, NCH * (PAIRS - t_first), y1_item, 0)
    row_messages("y1", "send")
    for copy in w1c_loads:
        copy.wait()

    def wait_halo(ref, width, rows_per, sem0, forward, c, nch):
        exists = has_bwd if forward else has_fwd

        @pl.when(exists & (c == 0))
        def _():
            y_recv(ref, width, rows_per, sem0, forward, 0, nch).wait_recv()

        @pl.when(exists & (c < nch - 1))
        def _():
            y_recv(ref, width, rows_per, sem0, forward, c + 1, nch).wait_recv()

    def z1_item(o, i):
        t = jnp.where(o < 0, o, jnp.where(o == 3, o, lax.rem(o + 1, 3)))
        mid = jnp.where(i < NCH - 2, i + 1, jnp.where(i == NCH - 2, 0, NCH - 1))
        c = jnp.where(o < 2, mid, i)
        k = own_col(t, 4)

        @pl.when((o == t_first) & (i == NCH - 2))
        def _():
            row_messages("y1", "recv")

        @pl.when(t == 0)
        def _():
            wait_halo(y1, PAIRS, ch, SEM_Y1, False, c, NCH)

        @pl.when(t == 3)
        def _():
            wait_halo(y1, PAIRS, ch, SEM_Y1, True, c, NCH)

        at = 1 + c * ch
        taps = []
        for first, sub in ((at - 1, 1), (at, 0), (at, 1), (at + 1, 0)):
            for side in (1, 2, 3):
                taps.append(flat(y1[k + side, pl.ds(first, ch), sub]))
        for sub in (0, 2):
            taps.append(flat(xs[k + 2, pl.ds(at, ch), sub]))
        acc = dot(jnp.concatenate(taps, axis=1), w1c[...])
        for p in range(2):
            val = jnp.maximum(acc[:, p * c1:(p + 1) * c1] + b1c[...], 0.0)
            z1[k + 3 - s, pl.ds(at, ch), p] = val.astype(BF16).reshape(ch, n, c1)

        @pl.when((t == 0) & has_fwd)
        def _():
            z_copy(z1, PAIRS, ch, SEM_Z1, c).start()
    phase(PAIRS, NCH, z1_item)
    row_messages("z1", "send")
    for copy in w2d_loads + w3d_loads:
        copy.wait()

    def turn_weight(i, carry):
        turned = lax.dot_general(eye[0:c2, 0:c2], w3r[i], NT, preferred_element_type=F32)
        w3d[i] = turned.astype(BF16)
        return carry
    loop(9, turn_weight)
    wp3[...] = lax.dot_general(eye[0:c2, 0:c2], wp3r[...], NT, preferred_element_type=F32).astype(BF16)

    def y2_item(t, i):
        c = jnp.where(t < 1, lax.rem(i + 1, NCH), i)
        k = own_col(t, 2)

        @pl.when((t == t_first) & (i == NCH - 1))
        def _():
            row_messages("z1", "recv")

        @pl.when((t == 1) & has_bwd)
        def _():
            z_recv(z1, PAIRS, ch, SEM_Z1, c).wait_recv()

        at = 1 + c * ch
        taps = []
        for first, sub in ((at - 1, 1), (at, 0), (at, 1)):
            for side in range(3):
                taps.append(flat(z1[2 * k + 2 + side, pl.ds(first, ch), sub]))
        acc = dot(jnp.concatenate(taps, axis=1), w2d[...])
        val = jnp.maximum(acc + b2d[...], 0.0)
        val = jnp.where(last_void & (t == 1), 0.0, val)
        y2[k + 2, pl.ds(at, ch)] = val.astype(BF16).reshape(ch, n, c2)

        @pl.when((t == 0) & has_fwd)
        def _():
            y_copy(y2, 2, ch, SEM_Y2, True, c, NCH).start()

        @pl.when((t == 1) & has_bwd)
        def _():
            y_copy(y2, 2, ch, SEM_Y2, False, c, NCH).start()
    phase(2, NCH, y2_item)
    row_messages("y2", "send")
    for copy in w2c_loads:
        copy.wait()

    def z2_item(t, c):
        k = own_col(t, 2)

        @pl.when((t == t_first) & (c == 0))
        def _():
            row_messages("y2", "recv")

        @pl.when(t == 0)
        def _():
            wait_halo(y2, 2, ch, SEM_Y2, False, c, NCH)

        @pl.when(t == 1)
        def _():
            wait_halo(y2, 2, ch, SEM_Y2, True, c, NCH)

        at = 1 + c * ch
        taps = []
        for first in (at - 1, at, at + 1):
            for side in (1, 2, 3):
                taps.append(flat(y2[k + side, pl.ds(first, ch)]))
        taps.append(flat(z1[2 * k + 3, pl.ds(at, ch), 0]))
        acc = dot(jnp.concatenate(taps, axis=1), w2c[...])
        val = jnp.maximum(acc + b2c[...], 0.0).astype(BF16).reshape(ch // 2, 2, n, c2)
        z2[k + 3 - s, pl.ds(1 + c * (ch // 2), ch // 2)] = val

        @pl.when((t == 0) & has_fwd)
        def _():
            z_copy(z2, 2, ch // 2, SEM_Z2, c).start()
    phase(2, NCH, z2_item)
    row_messages("z2", "send")

    def y3_item(t, c):
        k = t

        @pl.when((t == t_first) & (c == 0))
        def _():
            row_messages("z2", "recv")

        @pl.when((t == 0) & has_bwd)
        def _():
            for j in range(NCH // NCH3):
                z_recv(z2, 2, ch // 2, SEM_Z2, c * (NCH // NCH3) + j).wait_recv()

        at = 1 + c * ch3
        acc = jnp.zeros((ch3 * n, c3), F32)
        tap = 0
        for first, sub in ((at - 1, 1), (at, 0), (at, 1)):
            for side in range(3):
                acc = acc + dot(flat(z2[2 * k + 2 + side, pl.ds(first, ch3), sub]), w3d[tap])
                tap += 1
        val = jnp.maximum(acc + b3d[...], 0.0)
        val = jnp.where(last_void & (t == 0), 0.0, val)
        y3[k + 2, pl.ds(at, ch3)] = val.astype(BF16).reshape(ch3, n, c3)

        @pl.when((t == 0) & has_fwd)
        def _():
            y_copy(y3, 1, ch3, SEM_Y3, True, c, NCH3).start()

        @pl.when((t == 0) & has_bwd)
        def _():
            y_copy(y3, 1, ch3, SEM_Y3, False, c, NCH3).start()
    phase(1, NCH3, y3_item)
    row_messages("y3", "send")
    for copy in w3c_loads:
        copy.wait()

    ships = (s == 1) & has_bwd

    def ship(c):
        part = pl.ds(c * ch3, ch3)
        return remote(zo.at[1, part], out_hbm.at[part], out_sem.at[c], out_sem.at[NCH3 + c], row, bwd_col)

    def ship_recv(c):
        part = pl.ds(c * ch3, ch3)
        return remote(zo.at[1, part], out_hbm.at[part], out_sem.at[c], out_sem.at[NCH3 + c], row, fwd_col)

    keep = jnp.where(is0, 1, 0)

    def put(c):
        part = pl.ds(c * ch3, ch3)
        return pltpu.make_async_copy(zo.at[keep, part], out_hbm.at[part], out_sem.at[2 * NCH3 + c])

    def z3_item(t, c):
        k = t

        @pl.when((t == t_first) & (c == 0))
        def _():
            row_messages("y3", "recv")

        @pl.when(t == 0)
        def _():
            wait_halo(y3, 1, ch3, SEM_Y3, False, c, NCH3)
            wait_halo(y3, 1, ch3, SEM_Y3, True, c, NCH3)

        at = 1 + c * ch3
        acc = dot(flat(z2[2 * k + 3, pl.ds(at, ch3), 0]), wp3[...])
        tap = 0
        for first in (at - 1, at, at + 1):
            for side in (1, 2, 3):
                acc = acc + dot(flat(y3[k + side, pl.ds(first, ch3)]), w3c[tap])
                tap += 1
        val = jnp.maximum(acc + b3c[...], 0.0)
        zo[k + 1, pl.ds(c * ch3, ch3)] = val.astype(BF16).reshape(ch3, n, c3)

        @pl.when((t == 0) & ships)
        def _():
            ship(c).start()

        @pl.when(((t == 0) & is0) | (t == -1))
        def _():
            put(c).start()
    phase(1, NCH3, z3_item)

    for shift in SHIFTS:
        @pl.when(has_fwd & (s == shift))
        def _():
            for half in range(2):
                x_copy(shift, half).wait_send()

    def drain(c, carry):
        @pl.when(has_fwd)
        def _():
            y_copy(y1, PAIRS, ch, SEM_Y1, True, c, NCH).wait_send()
            z_copy(z1, PAIRS, ch, SEM_Z1, c).wait_send()
            y_copy(y2, 2, ch, SEM_Y2, True, c, NCH).wait_send()
            z_copy(z2, 2, ch // 2, SEM_Z2, c).wait_send()

        @pl.when(has_bwd)
        def _():
            y_copy(y1, PAIRS, ch, SEM_Y1, False, c, NCH).wait_send()
            y_copy(y2, 2, ch, SEM_Y2, False, c, NCH).wait_send()
        return carry
    loop(NCH, drain)

    def drain3(c, carry):
        @pl.when(has_fwd)
        def _():
            y_copy(y3, 1, ch3, SEM_Y3, True, c, NCH3).wait_send()

        @pl.when(has_bwd)
        def _():
            y_copy(y3, 1, ch3, SEM_Y3, False, c, NCH3).wait_send()

        @pl.when(ships)
        def _():
            ship(c).wait_send()

        @pl.when((s == 1) & has_fwd)
        def _():
            ship_recv(c).wait_recv()

        @pl.when(is0 | first_extra)
        def _():
            put(c).wait()
        return carry
    loop(NCH3, drain3)
    for name in ROW_SEM:
        row_messages(name, "sent")


def solution(mesh):
    rows = mesh.shape["row"]
    cols = mesh.shape["col"]
    tile_spec = P("batch", "row", "col")

    def local_blocks(x, w1d, b1d, w1c, b1c, wp1, w2d, b2d, w2c, b2c, wp2, w3d, b3d, w3c, b3c, wp3):
        n, h, w, c0 = x.shape
        c1, c2, c3 = w1d.shape[3], w2d.shape[3], w3d.shape[3]
        h4, h8 = h // 4, h // 8
        dims = (n, h, c0, c1, c2, c3, rows, cols)
        pair = 2 * c0
        xt = jnp.moveaxis(x, 1, 3).reshape(n, PAIRS, pair, h)
        args = (xt, w1d.reshape(3, 3 * c0, c1), w1c.reshape(9 * c1, c1), wp1, w2d.reshape(9 * c1, c2), w2c.reshape(9 * c2, c2), wp2,
                jnp.swapaxes(w3d.reshape(9, c2, c3), 1, 2), w3c.reshape(9, c3, c3), wp3.T,
                b1d, b1c, b2d, b2c, b3d, b3c)
        vm = pltpu.VMEM
        dma = pltpu.SemaphoreType.DMA
        flops = 2 * n * h * w * c1 * 7 * (c0 + c1)
        out = pl.pallas_call(
            functools.partial(kernel, dims),
            out_shape=jax.ShapeDtypeStruct((h8, n, c3), BF16),
            in_specs=[pl.BlockSpec(memory_space=pl.ANY)] * len(args),
            out_specs=pl.BlockSpec(memory_space=pl.ANY),
            scratch_shapes=[
                vm((PAIRS, n, pair, h), BF16), vm((2, n, pair, h // 2), BF16), vm((n, h, 2 * pair), BF16), vm((h, h), BF16), vm((n * BLOCK, n * BLOCK), BF16),
                vm((6, h4 + 1, 4, n, pair), BF16), vm((7, h4 + 2, 2, n, c1), BF16), vm((7, h4 + 1, 2, n, c1), BF16),
                vm((5, h4 + 2, n, c2), BF16), vm((5, h8 + 1, 2, n, c2), BF16), vm((4, h8 + 2, n, c3), BF16), vm((2, h8, n, c3), BF16),
                vm((10 * pair, 2 * c1), BF16), vm((12 * c1 + 2 * pair, 2 * c1), BF16), vm((9 * c1, c2), BF16), vm((9 * c2 + c1, c2), BF16),
                vm((9, c3, c2), BF16), vm((9, c2, c3), BF16), vm((9, c3, c3), BF16), vm((c3, c2), BF16), vm((c2, c3), BF16),
            ] + [vm((1, width), F32) for width in (c1, c1, c2, c2, c3, c3)] + [
                dma((count,)) for count in (32, 4, 10 * NCH, 10 * NCH, 12 * MAX_PLAN, 12 * MAX_PLAN, 3 * NCH3)],
            compiler_params=pltpu.CompilerParams(collective_id=0, has_side_effects=True, vmem_limit_bytes=63 * 1024 * 1024),
            cost_estimate=pl.CostEstimate(flops=flops, bytes_accessed=16 * 1024 * 1024, transcendentals=0),
        )(*args)
        return jnp.swapaxes(out, 0, 1).reshape(n, h8, 1, c3)

    return jax.shard_map(local_blocks, mesh=mesh, in_specs=(tile_spec,) + (P(),) * 15, out_specs=tile_spec, check_vma=False)
```

```python
import functools

import jax
import jax.numpy as jnp
from jax import lax
from jax.experimental import pallas as pl
from jax.experimental.pallas import tpu as pltpu
from jax.sharding import PartitionSpec as P

BF16 = jnp.bfloat16
F32 = jnp.float32
SHIFTS = (0, 1)
NCH = 4
NCH3 = 2
PAIRS = 4
MAX_PLAN = 5
BLOCK = 16
UNROLL = 4
OWN, HALO = range(2)
NT = (((1,), (1,)), ((), ()))


def relu(value):
    return jnp.maximum(value, 0.0)


def loop(count, body):
    lax.fori_loop(0, count, body, 0)


def row_plan(kind, width, s_send, s_recv):
    if kind == "x":
        own = (0, width - 1)
        need = (-1, width - 1) if s_recv == 0 else (0, width)
        src_at, dst_at = 2 - s_send, 2 - s_recv
    elif kind == "y":
        own = (s_send, width - 1 + s_send)
        need = (s_recv - 1, s_recv + width)
        src_at, dst_at = 2 - s_send, 2 - s_recv
    else:
        own = (s_send, width - 1 + s_send)
        need = (-1, width - 1) if s_recv == 0 else (0, width + 1)
        src_at, dst_at = 3 - 2 * s_send, 3 - 2 * s_recv
    plan = []
    for dist in range(-2, 3):
        lo = max(own[0], width * dist + need[0])
        hi = min(own[1], width * dist + need[1])
        if lo <= hi:
            plan.append((dist, lo + src_at, lo - width * dist + dst_at, hi - lo + 1, False))
        if kind != "x" and s_send == 1 and s_recv == 0 and dist >= 0 and need[0] + width * dist <= 0 <= need[1] + width * dist:
            plan.append((dist, src_at, dst_at - width * dist, 1, True))
    return plan


def kernel(dims, x_hbm, w1d_h, w1c_h, wp1_h, w2d_h, w2c_h, wp2_h, w3d_h, w3c_h, wp3_h, b1d_h, b1c_h, b2d_h, b2c_h, b3d_h, b3c_h, out_hbm,
           raw, xh, turned, eye, mix, xs, y1, z1, y2, z2, y3, zo, w1d, w1c, w2d, w2c, w3r, w3c, wp3r,
           b1d, b1c, b2d, b2c, b3d, b3c, load_sem, x_sem, col_send, col_recv, row_send, row_recv, out_sem):
    n, h, c0, c1, c2, c3, rows, cols = dims
    h4, h8 = h // 4, h // 8
    ch, ch3 = h4 // NCH, h8 // NCH3
    hh = h // 2
    row = lax.axis_index("row")
    col = lax.axis_index("col")
    s = lax.rem(row, 2)
    is0 = s == 0
    first_extra = (s == 1) & (col == 0)
    last_void = (s == 1) & (col == cols - 1)
    t_first = jnp.where(first_extra, -1, 0)
    fwd_col = jnp.where(is0, col + 1, col - 1)
    bwd_col = jnp.where(is0, col - 1, col + 1)
    has_fwd = (fwd_col >= 0) & (fwd_col < cols)
    has_bwd = (bwd_col >= 0) & (bwd_col < cols)

    load_count = []

    def load(src, dst):
        load_count.append(dst)
        return pltpu.make_async_copy(src, dst, load_sem.at[len(load_count) - 1])

    k1, k2 = 9 * c1, 9 * c2
    pair = 2 * c0
    x_loads = [load(x_hbm.at[:, q], raw.at[q]) for q in range(PAIRS)]
    w1d_loads = [load(b1d_h, b1d.at[0]), load(b1c_h, b1c.at[0])]
    w1c_loads = []
    for p in range(2):
        lanes = pl.ds(p * c1, c1)
        for kh in range(3):
            w1d_loads.append(load(w1d_h.at[kh], w1d.at[pl.ds((kh + 2 * p) * 2 * pair + c0, 3 * c0), lanes]))
        w1c_loads.append(load(w1c_h, w1c.at[pl.ds(p * 3 * c1, k1), lanes]))
        w1c_loads.append(load(wp1_h, w1c.at[pl.ds(12 * c1 + p * pair, c0), lanes]))
    w2d_loads = [load(w2d_h, w2d), load(b2d_h, b2d.at[0])]
    w2c_loads = [load(w2c_h, w2c.at[pl.ds(0, k2)]), load(wp2_h, w2c.at[pl.ds(k2, c1)]), load(b2c_h, b2c.at[0])]
    w3d_loads = [load(w3d_h, w3r), load(b3d_h, b3d.at[0]), load(wp3_h, wp3r)]
    w3c_loads = [load(w3c_h, w3c), load(b3c_h, b3c.at[0])]
    for copy in x_loads + w1d_loads + w1c_loads + w2d_loads + w2c_loads + w3d_loads + w3c_loads:
        copy.start()

    def row_refs(name, slots, down, side):
        ref = refs[name]
        last = ref.shape[1] - (2 if ROW_SEM[name][0] == "y" else 1)
        own_at, halo_at = (last, 0) if down else (1, last + 1)
        at = own_at if side == OWN else halo_at
        subs = 1 if len(ref.shape) == 4 else ref.shape[2]
        if subs == 1:
            return ref.at[slots, at]
        return ref.at[slots, at, subs - 1 if down else 0]

    refs = dict(x=xs, y1=y1, z1=z1, y2=y2, z2=z2, y3=y3)
    ROW_SEM = {}
    for name, kind, width in (("x", "x", PAIRS), ("y1", "y", PAIRS), ("z1", "z", PAIRS), ("y2", "y", 2), ("z2", "z", 2), ("y3", "y", 1)):
        ROW_SEM[name] = (kind, width, 2 * MAX_PLAN * len(ROW_SEM))

    def directions(name):
        return (True, False) if ROW_SEM[name][0] == "y" else (True,)

    def dot(lhs, rhs):
        return jnp.dot(lhs, rhs, preferred_element_type=F32)

    def zero_slot(ref, idx):
        def body(i, carry):
            ref[idx, i] = jnp.zeros(ref.shape[2:], ref.dtype)
            return carry
        loop(ref.shape[1], body)

    for name in ROW_SEM:
        for down in directions(name):
            edge = row_refs(name, slice(None), down, HALO)
            edge[...] = jnp.zeros(edge.shape, BF16)

    @pl.when(col == 0)
    def _():
        for slots, group in enumerate(((xs, y1, z1, y2, z2, y3), (y1, z1, y2, z2, y3), (z1, z2))):
            for ref in group:
                zero_slot(ref, slots)

    @pl.when(col == cols - 1)
    def _():
        for ref in (y1, z1, y2, z2, y3):
            zero_slot(ref, ref.shape[0] - 1)

    @pl.when(is0 | jnp.logical_not(has_bwd))
    def _():
        def body(i, carry):
            xh[0, i] = jnp.zeros((2 * c0, hh), BF16)
            xh[1, i] = jnp.zeros((2 * c0, hh), BF16)
            return carry
        loop(n, body)

    barrier = pltpu.get_barrier_semaphore()
    for rr in range(rows):
        for cc in range(cols):
            pl.semaphore_signal(barrier, inc=1, device_id={"row": jnp.int32(rr), "col": jnp.int32(cc)}, device_id_type=pl.DeviceIdType.MESH)
    pl.semaphore_wait(barrier, rows * cols)

    def remote(src, dst, send_sem, recv_sem, to_row, to_col):
        return pltpu.make_async_remote_copy(src_ref=src, dst_ref=dst, send_sem=send_sem, recv_sem=recv_sem,
                                            device_id={"row": to_row, "col": to_col}, device_id_type=pl.DeviceIdType.MESH)

    def x_copy(shift, half):
        lanes = pl.ds(half * hh, hh)
        if shift == 0:
            src, dst = x_hbm.at[:, 3, pl.ds(c0, c0), lanes], xh.at[half, :, pl.ds(c0, c0)]
        else:
            src, dst = x_hbm.at[:, 0, :, lanes], xh.at[half]
        return remote(src, dst, x_sem.at[half], x_sem.at[2 + half], row, fwd_col)

    for shift in SHIFTS:
        @pl.when(has_fwd & (s == shift))
        def _():
            for half in range(2):
                x_copy(shift, half).start()

    def y_copy(ref, width, rows_per, sem0, forward, chunk, nch):
        to_right = is0 if forward else jnp.logical_not(is0)
        src_slot = jnp.where(to_right, width + 1, 2)
        dst_slot = jnp.where(to_right, 1, width + 2)
        part = pl.ds(1 + chunk * rows_per, rows_per)
        sem = sem0 + (0 if forward else nch) + chunk
        return remote(ref.at[src_slot, part], ref.at[dst_slot, part], col_send.at[sem], col_recv.at[sem], row, fwd_col if forward else bwd_col)

    def y_recv(ref, width, rows_per, sem0, forward, chunk, nch):
        to_right = is0 if forward else jnp.logical_not(is0)
        dst_slot = jnp.where(to_right, 1, width + 2)
        part = pl.ds(1 + chunk * rows_per, rows_per)
        sem = sem0 + (0 if forward else nch) + chunk
        return remote(ref.at[dst_slot, part], ref.at[dst_slot, part], col_send.at[sem], col_recv.at[sem], row, bwd_col if forward else fwd_col)

    def z_copy(ref, width, rows_per, sem0, chunk):
        src_slot = jnp.where(is0, width + 2, 2)
        dst_slot = jnp.where(is0, 2, width + 2)
        part = pl.ds(1 + chunk * rows_per, rows_per)
        sem = sem0 + chunk
        return remote(ref.at[src_slot, part], ref.at[dst_slot, part], col_send.at[sem], col_recv.at[sem], row, fwd_col)

    def z_recv(ref, width, rows_per, sem0, chunk):
        dst_slot = jnp.where(is0, 2, width + 2)
        part = pl.ds(1 + chunk * rows_per, rows_per)
        sem = sem0 + chunk
        return remote(ref.at[dst_slot, part], ref.at[dst_slot, part], col_send.at[sem], col_recv.at[sem], row, bwd_col)

    SEM_Y1, SEM_Z1, SEM_Y2, SEM_Z2, SEM_Y3 = (i * 2 * NCH for i in range(5))

    def row_messages(name, act):
        kind, width, sem0 = ROW_SEM[name]
        for down in directions(name):
            for s_send, s_recv in zip(SHIFTS, reversed(SHIFTS)):
                step = 1 if down else -1
                for i, (dist, src, dst, count, extra) in enumerate(row_plan(kind, width, s_send, s_recv)):
                    sem = sem0 + i + (0 if down else MAX_PLAN)
                    if act == "recv":
                        from_row, from_col = row - step, col - dist
                        ok = (s == s_recv) & (from_row >= 0) & (from_row < rows) & (from_col >= 0) & (from_col < cols)
                        if extra:
                            ok = ok & (from_col == 0)

                        @pl.when(ok)
                        def _():
                            ref = row_refs(name, pl.ds(dst, count), down, HALO)
                            remote(ref, ref, row_send.at[sem], row_recv.at[sem], from_row, from_col).wait_recv()
                    else:
                        to_row, to_col = row + step, col + dist
                        ok = (s == s_send) & (to_row >= 0) & (to_row < rows) & (to_col >= 0) & (to_col < cols)
                        if extra:
                            ok = ok & (col == 0)

                        @pl.when(ok)
                        def _():
                            copy = remote(row_refs(name, pl.ds(src, count), down, OWN), row_refs(name, pl.ds(dst, count), down, HALO),
                                          row_send.at[sem], row_recv.at[sem], to_row, to_col)
                            if act == "send":
                                copy.start()
                            else:
                                copy.wait_send()

    def unit_where(size, source):
        at = lax.broadcasted_iota(jnp.int32, (size, size), 0)
        return (at == source(lax.broadcasted_iota(jnp.int32, (size, size), 1))).astype(F32).astype(BF16)

    eye[...] = unit_where(h, lambda at: at)
    mix[...] = unit_where(n * BLOCK, lambda at: (at & (BLOCK - 1)) * n + (at >> BLOCK.bit_length() - 1))

    def to_rows(value):
        return value.astype(BF16).reshape(BLOCK // 4, 4, n, pair)

    def turn_group(q):
        def turn(i, carry):
            for j in range(UNROLL):
                at = i * UNROLL + j
                block = raw[pl.ds(q, 2), at].reshape(2 * pair, h)
                turned[at] = lax.dot_general(eye[...], block, NT, preferred_element_type=F32).astype(BF16)
            return carry
        loop(n // UNROLL, turn)

        def place(i, carry):
            for j in range(UNROLL):
                at = i * UNROLL + j
                block = turned[:, pl.ds(at * BLOCK, BLOCK), :].reshape(n * BLOCK, 2 * pair)
                moved = dot(mix[...], block)
                for side in range(2):
                    xs[q + 2 - s + side, pl.ds(1 + at * (BLOCK // 4), BLOCK // 4)] = to_rows(moved[:, side * pair:(side + 1) * pair])
            return carry
        loop(h // BLOCK // UNROLL, place)

    def turn_halo(half):
        slot = jnp.where(is0, 1, PAIRS + 1)
        unit = eye[:hh, :hh]

        def turn(i, carry):
            for j in range(UNROLL):
                at = 2 * (i * UNROLL + j)
                block = xh[half, pl.ds(at, 2)].reshape(2 * pair, hh)
                both = lax.dot_general(unit, block, NT, preferred_element_type=F32).astype(BF16)
                for side in range(2):
                    turned[at + side, :hh, :pair] = both[:, side * pair:(side + 1) * pair]
            return carry
        loop(n // 2 // UNROLL, turn)

        def place(i, carry):
            blocks = [turned[:, pl.ds((2 * i + j) * BLOCK, BLOCK), :pair].reshape(n * BLOCK, pair) for j in range(2)]
            moved = dot(mix[...], jnp.concatenate(blocks, axis=1))
            for j in range(2):
                first = 1 + half * (h4 // 2) + (2 * i + j) * (BLOCK // 4)
                xs[slot, pl.ds(first, BLOCK // 4)] = to_rows(moved[:, j * pair:(j + 1) * pair])
            return carry
        loop(hh // BLOCK // 2, place)

    def zero_part(ref, first, size, p):
        ref[pl.ds(first, size), pl.ds(p * c1, c1)] = jnp.zeros((size, c1), BF16)

    def zero_weights():
        for p in range(2):
            for kh in range(5):
                tap_at = kh * 2 * pair
                used = 2 * p <= kh < 2 * p + 3
                zero_part(w1d, tap_at, c0 if used else 2 * pair, p)
            zero_part(w1c, (1 - p) * k1, 3 * c1, p)
            proj_at = 12 * c1
            zero_part(w1c, proj_at + (1 - p) * pair, pair, p)
            zero_part(w1c, proj_at + p * pair + c0, c0, p)

    zero_weights()
    for copy in x_loads + w1d_loads:
        copy.wait()

    def flat(value):
        return value.reshape(value.shape[0] * n, value.shape[-1])

    def parts(first, count):
        size = count // 2
        return tuple((first + i * size, size) for i in range(2))

    def dot_nt(lhs, rhs):
        return lax.dot_general(lhs, rhs, NT, preferred_element_type=F32)

    def own_col(t, width):
        return jnp.where(is0, width - 1 - t, t)

    def phase(width, nch, item):
        def body(at, carry):
            item(lax.div(at, nch) - 1, lax.rem(at, nch))
            return carry
        lax.fori_loop((t_first + 1) * nch, (width + 1) * nch, body, 0)

    def y1_job(t, c):
        k = own_col(t, PAIRS)
        at = 1 + c * ch
        taps = []
        for kh in range(5):
            first, sub = (at - 1, 3) if kh == 0 else (at, kh - 1)
            for side in (1, 2):
                taps.append(flat(xs[k + side, pl.ds(first, ch), sub]))
        acc = dot(jnp.concatenate(taps, axis=1), w1d[...])
        void = last_void & (t == 3)
        for p in range(2):
            val = relu(acc[:, p * c1:(p + 1) * c1] + b1d[...])
            val = jnp.where(void, 0.0, val)
            y1[k + 2, pl.ds(at, ch), p] = val.astype(BF16).reshape(ch, n, c1)

    def own_group(group, carry):
        turn_group(2 * group)
        return carry
    loop(PAIRS // 2, own_group)
    row_messages("x", "send")
    early = 3 - t_first

    def y1_item(item, carry):
        @pl.when(item == lax.div(3 * early, 2))
        def _():
            row_messages("x", "recv")

        half = item - 2 * early

        @pl.when(half >= 0)
        def _():
            for shift in SHIFTS:
                @pl.when(has_bwd & (s == shift))
                def _():
                    ref = xh.at[half, :, pl.ds(c0, c0)] if shift == 0 else xh.at[half]
                    remote(ref, ref, x_sem.at[half], x_sem.at[2 + half], row, bwd_col).wait_recv()
            turn_halo(half)

        jobs = []
        for j in range(2):
            at = 2 * item + j
            t = jnp.where(at < 3 * early, lax.div(at, 3) + t_first, jnp.where(half >= 0, 3, at - 3 * early + t_first))
            c = jnp.where(at < 3 * early, lax.rem(at, 3) + 1, jnp.where(half >= 0, at - NCH * early, 0))
            jobs.append((t, c))
        for t, c in jobs:
            y1_job(t, c)
        for t, c in jobs:
            @pl.when((t == 0) & has_fwd)
            def _():
                y_copy(y1, PAIRS, ch, SEM_Y1, True, c, NCH).start()

            @pl.when((t == 3) & has_bwd)
            def _():
                y_copy(y1, PAIRS, ch, SEM_Y1, False, c, NCH).start()
        return carry
    loop(2 * (PAIRS - t_first), y1_item)
    row_messages("y1", "send")
    for copy in w1c_loads:
        copy.wait()

    def wait_halo(ref, width, rows_per, sem0, forward, c, nch):
        exists = has_bwd if forward else has_fwd

        @pl.when(exists & (c == 0))
        def _():
            y_recv(ref, width, rows_per, sem0, forward, 0, nch).wait_recv()

        @pl.when(exists & (c < nch - 1))
        def _():
            y_recv(ref, width, rows_per, sem0, forward, c + 1, nch).wait_recv()

    def z1_job(t, c):
        k = own_col(t, PAIRS)
        at = 1 + c * ch
        taps = []
        for first, sub in ((at - 1, 1), (at, 0), (at, 1), (at + 1, 0)):
            for side in (1, 2, 3):
                taps.append(flat(y1[k + side, pl.ds(first, ch), sub]))
        for sub in (0, 2):
            taps.append(flat(xs[k + 2, pl.ds(at, ch), sub]))
        acc = dot(jnp.concatenate(taps, axis=1), w1c[...])
        for p in range(2):
            val = relu(acc[:, p * c1:(p + 1) * c1] + b1c[...])
            z1[k + 3 - s, pl.ds(at, ch), p] = val.astype(BF16).reshape(ch, n, c1)

    extra = -t_first

    def z1_item(item, carry):
        inner = item - extra
        edge = inner - NCH - extra
        more = (inner < 0) | (extra == 1) & (inner == NCH)

        @pl.when(inner == 2)
        def _():
            row_messages("y1", "recv")

        @pl.when(edge >= 0)
        def _():
            wait_halo(y1, PAIRS, ch, SEM_Y1, False, edge, NCH)
            wait_halo(y1, PAIRS, ch, SEM_Y1, True, edge, NCH)

        mid = jnp.where(inner < 2, inner + 1, jnp.where(inner == 2, 0, inner))
        for j in range(2):
            t = jnp.where(more, -1, jnp.where(edge >= 0, 3 * j, j + 1))
            c = jnp.where(more, jnp.where(inner < 0, j + 1, 3 * j), jnp.where(edge >= 0, edge, mid))
            z1_job(t, c)

        @pl.when((edge >= 0) & has_fwd)
        def _():
            z_copy(z1, PAIRS, ch, SEM_Z1, edge).start()
        return carry
    loop(2 * (NCH + extra), z1_item)
    row_messages("z1", "send")
    for copy in w2d_loads:
        copy.wait()

    def y2_job(t, at, size):
        k = own_col(t, 2)
        taps = []
        for first, sub in ((at - 1, 1), (at, 0), (at, 1)):
            for side in range(3):
                taps.append(flat(z1[2 * k + 2 + side, pl.ds(first, size), sub]))
        acc = dot(jnp.concatenate(taps, axis=1), w2d[...])
        val = relu(acc + b2d[...])
        val = jnp.where(last_void & (t == 1), 0.0, val)
        y2[k + 2, pl.ds(at, size)] = val.astype(BF16).reshape(size, n, c2)

    def y2_inner(item, carry):
        t = t_first + lax.div(item, 2)
        late = lax.rem(item, 2)

        @pl.when(item == 1)
        def _():
            row_messages("z1", "recv")

        chunks = (1 + 2 * late, 2 - 2 * late)
        for c in chunks:
            y2_job(t, 1 + c * ch, ch)

        @pl.when((t == 0) & has_fwd)
        def _():
            for c in chunks:
                y_copy(y2, 2, ch, SEM_Y2, True, c, NCH).start()
        return carry
    loop(2 + 2 * extra, y2_inner)

    def y2_edge(c, carry):
        @pl.when(has_bwd)
        def _():
            z_recv(z1, PAIRS, ch, SEM_Z1, c).wait_recv()

        for at, size in parts(1 + c * ch, ch):
            y2_job(jnp.int32(1), at, size)

        @pl.when(has_bwd)
        def _():
            y_copy(y2, 2, ch, SEM_Y2, False, c, NCH).start()
        return carry
    loop(NCH, y2_edge)
    row_messages("y2", "send")
    for copy in w2c_loads:
        copy.wait()

    def z2_job(t, c):
        k = own_col(t, 2)
        at = 1 + c * ch
        taps = []
        for first in (at - 1, at, at + 1):
            for side in (1, 2, 3):
                taps.append(flat(y2[k + side, pl.ds(first, ch)]))
        taps.append(flat(z1[2 * k + 3, pl.ds(at, ch), 0]))
        acc = dot(jnp.concatenate(taps, axis=1), w2c[...])
        val = relu(acc + b2c[...]).astype(BF16).reshape(ch // 2, 2, n, c2)
        z2[k + 3 - s, pl.ds(1 + c * (ch // 2), ch // 2)] = val

    row_messages("y2", "recv")

    def z2_item(item, carry):
        c = item - 2 * extra

        @pl.when(c >= 0)
        def _():
            wait_halo(y2, 2, ch, SEM_Y2, False, c, NCH)
            wait_halo(y2, 2, ch, SEM_Y2, True, c, NCH)

        for j in range(2):
            z2_job(jnp.where(c < 0, -1, j), jnp.where(c < 0, 2 * item + j, c))

        @pl.when((c >= 0) & has_fwd)
        def _():
            z_copy(z2, 2, ch // 2, SEM_Z2, c).start()
        return carry
    loop(NCH + 2 * extra, z2_item)
    row_messages("z2", "send")

    for copy in w3d_loads:
        copy.wait()

    def y3_item(t, c):
        k = t

        @pl.when((t == t_first) & (c == 0))
        def _():
            row_messages("z2", "recv")

        @pl.when((t == 0) & has_bwd)
        def _():
            for j in range(NCH // NCH3):
                z_recv(z2, 2, ch // 2, SEM_Z2, c * (NCH // NCH3) + j).wait_recv()

        for at, size in parts(1 + c * ch3, ch3):
            acc = b3d[...]
            tap = 0
            for first, sub in ((at - 1, 1), (at, 0), (at, 1)):
                for side in range(3):
                    acc = acc + dot_nt(flat(z2[2 * k + 2 + side, pl.ds(first, size), sub]), w3r[tap])
                    tap += 1
            val = jnp.where(last_void & (t == 0), 0.0, relu(acc))
            y3[k + 2, pl.ds(at, size)] = val.astype(BF16).reshape(size, n, c3)

        @pl.when((t == 0) & has_fwd)
        def _():
            y_copy(y3, 1, ch3, SEM_Y3, True, c, NCH3).start()

        @pl.when((t == 0) & has_bwd)
        def _():
            y_copy(y3, 1, ch3, SEM_Y3, False, c, NCH3).start()
    phase(1, NCH3, y3_item)
    row_messages("y3", "send")
    for copy in w3c_loads:
        copy.wait()

    ships = (s == 1) & has_bwd

    def ship(c):
        part = pl.ds(c * ch3, ch3)
        return remote(zo.at[1, part], out_hbm.at[part], out_sem.at[c], out_sem.at[NCH3 + c], row, bwd_col)

    def ship_recv(c):
        part = pl.ds(c * ch3, ch3)
        return remote(zo.at[1, part], out_hbm.at[part], out_sem.at[c], out_sem.at[NCH3 + c], row, fwd_col)

    keep = jnp.where(is0, 1, 0)

    def put(c):
        part = pl.ds(c * ch3, ch3)
        return pltpu.make_async_copy(zo.at[keep, part], out_hbm.at[part], out_sem.at[2 * NCH3 + c])

    def z3_item(t, c):
        k = t

        @pl.when((t == t_first) & (c == 0))
        def _():
            row_messages("y3", "recv")

        @pl.when(t == 0)
        def _():
            wait_halo(y3, 1, ch3, SEM_Y3, False, c, NCH3)
            wait_halo(y3, 1, ch3, SEM_Y3, True, c, NCH3)

        for at, size in parts(1 + c * ch3, ch3):
            acc = dot_nt(flat(z2[2 * k + 3, pl.ds(at, size), 0]), wp3r[...]) + b3c[...]
            tap = 0
            for first in (at - 1, at, at + 1):
                for side in (1, 2, 3):
                    acc = acc + dot(flat(y3[k + side, pl.ds(first, size)]), w3c[tap])
                    tap += 1
            zo[k + 1, pl.ds(at - 1, size)] = relu(acc).astype(BF16).reshape(size, n, c3)

        @pl.when((t == 0) & ships)
        def _():
            ship(c).start()

        @pl.when(((t == 0) & is0) | (t == -1))
        def _():
            put(c).start()
    phase(1, NCH3, z3_item)

    for shift in SHIFTS:
        @pl.when(has_fwd & (s == shift))
        def _():
            for half in range(2):
                x_copy(shift, half).wait_send()

    def drain(c, carry):
        @pl.when(has_fwd)
        def _():
            y_copy(y1, PAIRS, ch, SEM_Y1, True, c, NCH).wait_send()
            z_copy(z1, PAIRS, ch, SEM_Z1, c).wait_send()
            y_copy(y2, 2, ch, SEM_Y2, True, c, NCH).wait_send()
            z_copy(z2, 2, ch // 2, SEM_Z2, c).wait_send()

        @pl.when(has_bwd)
        def _():
            y_copy(y1, PAIRS, ch, SEM_Y1, False, c, NCH).wait_send()
            y_copy(y2, 2, ch, SEM_Y2, False, c, NCH).wait_send()
        return carry
    loop(NCH, drain)

    def drain3(c, carry):
        @pl.when(has_fwd)
        def _():
            y_copy(y3, 1, ch3, SEM_Y3, True, c, NCH3).wait_send()

        @pl.when(has_bwd)
        def _():
            y_copy(y3, 1, ch3, SEM_Y3, False, c, NCH3).wait_send()

        @pl.when(ships)
        def _():
            ship(c).wait_send()

        @pl.when((s == 1) & has_fwd)
        def _():
            ship_recv(c).wait_recv()

        @pl.when(is0 | first_extra)
        def _():
            put(c).wait()
        return carry
    loop(NCH3, drain3)
    for name in ROW_SEM:
        row_messages(name, "sent")


def solution(mesh):
    rows = mesh.shape["row"]
    cols = mesh.shape["col"]
    tile_spec = P("batch", "row", "col")

    def local_blocks(x, w1d, b1d, w1c, b1c, wp1, w2d, b2d, w2c, b2c, wp2, w3d, b3d, w3c, b3c, wp3):
        n, h, w, c0 = x.shape
        c1, c2, c3 = w1d.shape[3], w2d.shape[3], w3d.shape[3]
        h4, h8 = h // 4, h // 8
        dims = (n, h, c0, c1, c2, c3, rows, cols)
        pair = 2 * c0
        xt = jnp.moveaxis(x, 1, 3).reshape(n, PAIRS, pair, h)
        args = (xt, w1d.reshape(3, 3 * c0, c1), w1c.reshape(9 * c1, c1), wp1, w2d.reshape(9 * c1, c2), w2c.reshape(9 * c2, c2), wp2,
                jnp.swapaxes(w3d.reshape(9, c2, c3), 1, 2), w3c.reshape(9, c3, c3), wp3.T,
                b1d, b1c, b2d, b2c, b3d, b3c)
        vm = pltpu.VMEM
        dma = pltpu.SemaphoreType.DMA
        flops = 2 * n * h * w * c1 * 7 * (c0 + c1)
        out = pl.pallas_call(
            functools.partial(kernel, dims),
            out_shape=jax.ShapeDtypeStruct((h8, n, c3), BF16),
            in_specs=[pl.BlockSpec(memory_space=pl.ANY)] * len(args),
            out_specs=pl.BlockSpec(memory_space=pl.ANY),
            scratch_shapes=[
                vm((PAIRS, n, pair, h), BF16), vm((2, n, pair, h // 2), BF16), vm((n, h, 2 * pair), BF16), vm((h, h), BF16), vm((n * BLOCK, n * BLOCK), BF16),
                vm((6, h4 + 1, 4, n, pair), BF16), vm((7, h4 + 2, 2, n, c1), BF16), vm((7, h4 + 1, 2, n, c1), BF16),
                vm((5, h4 + 2, n, c2), BF16), vm((5, h8 + 1, 2, n, c2), BF16), vm((4, h8 + 2, n, c3), BF16), vm((2, h8, n, c3), BF16),
                vm((10 * pair, 2 * c1), BF16), vm((12 * c1 + 2 * pair, 2 * c1), BF16), vm((9 * c1, c2), BF16), vm((9 * c2 + c1, c2), BF16),
                vm((9, c3, c2), BF16), vm((9, c3, c3), BF16), vm((c3, c2), BF16),
            ] + [vm((1, width), F32) for width in (c1, c1, c2, c2, c3, c3)] + [
                dma((count,)) for count in (32, 4, 10 * NCH, 10 * NCH, 12 * MAX_PLAN, 12 * MAX_PLAN, 3 * NCH3)],
            compiler_params=pltpu.CompilerParams(collective_id=0, has_side_effects=True, vmem_limit_bytes=63 * 1024 * 1024),
            cost_estimate=pl.CostEstimate(flops=flops, bytes_accessed=16 * 1024 * 1024, transcendentals=0),
        )(*args)
        return jnp.swapaxes(out, 0, 1).reshape(n, h8, 1, c3)

    return jax.shard_map(local_blocks, mesh=mesh, in_specs=(tile_spec,) + (P(),) * 15, out_specs=tile_spec, check_vma=False)
```

```python
import functools

import jax
import jax.numpy as jnp
from jax import lax
from jax.experimental import pallas as pl
from jax.experimental.pallas import tpu as pltpu
from jax.sharding import PartitionSpec as P

BF16 = jnp.bfloat16
F32 = jnp.float32
SHIFTS = (0, 1)
NCH = 4
NCH3 = 2
PAIRS = 4
MAX_PLAN = 5
BLOCK = 16
UNROLL = 4
OWN, HALO = BOTH = range(2)
AROUND = (1, 2, 3)
UP, DOWN = (False,), (True,)
NT = (((1,), (1,)), ((), ()))


def relu(value):
    return jnp.maximum(value, 0.0)


def loop(count, body):
    lax.fori_loop(0, count, body, 0)


def row_plan(kind, width, s_send, s_recv):
    if kind == "x":
        own = (0, width - 1)
        need = (-1, width - 1) if s_recv == 0 else (0, width)
        src_at, dst_at = 2 - s_send, 2 - s_recv
    elif kind == "y":
        own = (s_send, width - 1 + s_send)
        need = (s_recv - 1, s_recv + width)
        src_at, dst_at = 2 - s_send, 2 - s_recv
    else:
        own = (s_send, width - 1 + s_send)
        need = (-1, width - 1) if s_recv == 0 else (0, width + 1)
        src_at, dst_at = 3 - 2 * s_send, 3 - 2 * s_recv
    plan = []
    for dist in range(-2, 3):
        lo = max(own[0], width * dist + need[0])
        hi = min(own[1], width * dist + need[1])
        if lo <= hi:
            plan.append((dist, lo + src_at, lo - width * dist + dst_at, hi - lo + 1, False))
        if kind != "x" and s_send == 1 and s_recv == 0 and dist >= 0 and need[0] + width * dist <= 0 <= need[1] + width * dist:
            plan.append((dist, src_at, dst_at - width * dist, 1, True))
    return plan


def kernel(dims, x_hbm, w1d_h, w1c_h, wp1_h, w2d_h, w2c_h, wp2_h, w3d_h, w3c_h, wp3_h, b1d_h, b1c_h, b2d_h, b2c_h, b3d_h, b3c_h, out_hbm,
           raw, xh, turned, eye, mix, xs, y1, z1, y2, z2, y3, zo, w1d, w1c, w2d, w2c, w3r, w3c, wp3r,
           b1d, b1c, b2d, b2c, b3d, b3c, load_sem, x_sem, col_send, col_recv, row_send, row_recv, out_sem):
    n, h, c0, c1, c2, c3, rows, cols = dims
    h4, h8 = h // 4, h // 8
    ch, ch3 = h4 // NCH, h8 // NCH3
    hh = h // 2
    row = lax.axis_index("row")
    col = lax.axis_index("col")
    s = lax.rem(row, 2)
    is0 = s == 0
    first_extra = (s == 1) & (col == 0)
    last_void = (s == 1) & (col == cols - 1)
    t_first = jnp.where(first_extra, -1, 0)
    fwd_col = jnp.where(is0, col + 1, col - 1)
    bwd_col = jnp.where(is0, col - 1, col + 1)
    has_fwd = (fwd_col >= 0) & (fwd_col < cols)
    has_bwd = (bwd_col >= 0) & (bwd_col < cols)

    load_count = []

    def load(src, dst):
        load_count.append(dst)
        return pltpu.make_async_copy(src, dst, load_sem.at[len(load_count) - 1])

    k1, k2 = 9 * c1, 9 * c2
    pair = 2 * c0
    x_loads = [load(x_hbm.at[:, q], raw.at[q]) for q in range(PAIRS)]
    w1d_loads = [load(b1d_h, b1d.at[0]), load(b1c_h, b1c.at[0])]
    w1c_loads = []
    for p in BOTH:
        lanes = pl.ds(p * c1, c1)
        for kh in range(3):
            w1d_loads.append(load(w1d_h.at[kh], w1d.at[pl.ds((kh + 2 * p) * 2 * pair + c0, 3 * c0), lanes]))
        w1c_loads.append(load(w1c_h, w1c.at[pl.ds(p * 3 * c1, k1), lanes]))
        w1c_loads.append(load(wp1_h, w1c.at[pl.ds(12 * c1 + p * pair, c0), lanes]))
    w2d_loads = [load(w2d_h, w2d), load(b2d_h, b2d.at[0])]
    w2c_loads = [load(w2c_h, w2c.at[pl.ds(0, k2)]), load(wp2_h, w2c.at[pl.ds(k2, c1)]), load(b2c_h, b2c.at[0])]
    w3d_loads = [load(w3d_h, w3r), load(b3d_h, b3d.at[0]), load(wp3_h, wp3r)]
    w3c_loads = [load(w3c_h, w3c), load(b3c_h, b3c.at[0])]
    for copy in x_loads + w1d_loads + w1c_loads + w2d_loads + w2c_loads + w3d_loads + w3c_loads:
        copy.start()

    def row_refs(name, slots, down, side):
        ref = refs[name]
        last = ref.shape[1] - (2 if ROW_SEM[name][0] == "y" else 1)
        own_at, halo_at = (last, 0) if down else (1, last + 1)
        at = own_at if side == OWN else halo_at
        subs = 1 if len(ref.shape) == 4 else ref.shape[2]
        if subs == 1:
            return ref.at[slots, at]
        return ref.at[slots, at, subs - 1 if down else 0]

    refs = dict(x=xs, y1=y1, z1=z1, y2=y2, z2=z2, y3=y3)
    ROW_SEM = {}
    for name, kind, width in (("x", "x", PAIRS), ("y1", "y", PAIRS), ("z1", "z", PAIRS), ("y2", "y", 2), ("z2", "z", 2), ("y3", "y", 1)):
        ROW_SEM[name] = (kind, width, 2 * MAX_PLAN * len(ROW_SEM))

    def directions(name):
        return (True, False) if ROW_SEM[name][0] == "y" else (True,)

    def dot(lhs, rhs):
        return jnp.dot(lhs, rhs, preferred_element_type=F32)

    def zero_slot(ref, idx):
        ref[idx] = jnp.zeros(ref.shape[1:], ref.dtype)

    def dot(lhs, rhs):
        return jnp.dot(lhs, rhs, preferred_element_type=F32)

    def zero_slot(ref, idx):
        def body(i, carry):
            ref[idx, i] = jnp.zeros(ref.shape[2:], ref.dtype)
            return carry
        loop(ref.shape[1], body)

    for name in ROW_SEM:
        for down in directions(name):
            edge = row_refs(name, slice(None), down, HALO)
            edge[...] = jnp.zeros(edge.shape, BF16)

    @pl.when(col == 0)
    def _():
        for ref in (y1, y2, y3):
            zero_slot(ref, 1 - s)
        for ref in (z1, z2):
            zero_slot(ref, 2 - 2 * s)

    @pl.when(first_extra)
    def _():
        zero_slot(xs, 0)

    @pl.when(col == cols - 1)
    def _():
        for ref in (y1, y2, y3):
            zero_slot(ref, ref.shape[0] - 1)

    @pl.when(is0 | jnp.logical_not(has_bwd))
    def _():
        def body(i, carry):
            xh[0, i] = jnp.zeros((2 * c0, hh), BF16)
            xh[1, i] = jnp.zeros((2 * c0, hh), BF16)
            return carry
        loop(n, body)

    barrier = pltpu.get_barrier_semaphore()
    for rr in range(rows):
        for cc in range(cols):
            pl.semaphore_signal(barrier, inc=1, device_id={"row": jnp.int32(rr), "col": jnp.int32(cc)}, device_id_type=pl.DeviceIdType.MESH)
    pl.semaphore_wait(barrier, rows * cols)

    def remote(src, dst, send_sem, recv_sem, to_row, to_col):
        return pltpu.make_async_remote_copy(src_ref=src, dst_ref=dst, send_sem=send_sem, recv_sem=recv_sem,
                                            device_id={"row": to_row, "col": to_col}, device_id_type=pl.DeviceIdType.MESH)

    def x_copy(shift, half):
        lanes = pl.ds(half * hh, hh)
        if shift == 0:
            src, dst = x_hbm.at[:, 3, pl.ds(c0, c0), lanes], xh.at[half, :, pl.ds(c0, c0)]
        else:
            src, dst = x_hbm.at[:, 0, :, lanes], xh.at[half]
        return remote(src, dst, x_sem.at[half], x_sem.at[2 + half], row, fwd_col)

    for shift in SHIFTS:
        @pl.when(has_fwd & (s == shift))
        def _():
            for half in BOTH:
                x_copy(shift, half).start()

    def y_copy(ref, width, rows_per, sem0, forward, chunk, nch):
        to_right = is0 if forward else jnp.logical_not(is0)
        src_slot = jnp.where(to_right, width + 1, 2)
        dst_slot = jnp.where(to_right, 1, width + 2)
        part = pl.ds(1 + chunk * rows_per, rows_per)
        sem = sem0 + (0 if forward else nch) + chunk
        return remote(ref.at[src_slot, part], ref.at[dst_slot, part], col_send.at[sem], col_recv.at[sem], row, fwd_col if forward else bwd_col)

    def y_recv(ref, width, rows_per, sem0, forward, chunk, nch):
        to_right = is0 if forward else jnp.logical_not(is0)
        dst_slot = jnp.where(to_right, 1, width + 2)
        part = pl.ds(1 + chunk * rows_per, rows_per)
        sem = sem0 + (0 if forward else nch) + chunk
        return remote(ref.at[dst_slot, part], ref.at[dst_slot, part], col_send.at[sem], col_recv.at[sem], row, bwd_col if forward else fwd_col)

    def z_copy(ref, width, rows_per, sem0, chunk):
        src_slot = jnp.where(is0, width + 2, 2)
        dst_slot = jnp.where(is0, 2, width + 2)
        part = pl.ds(1 + chunk * rows_per, rows_per)
        sem = sem0 + chunk
        return remote(ref.at[src_slot, part], ref.at[dst_slot, part], col_send.at[sem], col_recv.at[sem], row, fwd_col)

    def z_recv(ref, width, rows_per, sem0, chunk):
        dst_slot = jnp.where(is0, 2, width + 2)
        part = pl.ds(1 + chunk * rows_per, rows_per)
        sem = sem0 + chunk
        return remote(ref.at[dst_slot, part], ref.at[dst_slot, part], col_send.at[sem], col_recv.at[sem], row, bwd_col)

    SEM_Y1, SEM_Z1, SEM_Y2, SEM_Z2, SEM_Y3 = (i * 2 * NCH for i in range(5))

    def row_messages(name, act, ways=None):
        kind, width, sem0 = ROW_SEM[name]
        for down in ways or directions(name):
            for s_send, s_recv in zip(SHIFTS, reversed(SHIFTS)):
                step = 1 if down else -1
                for i, (dist, src, dst, count, extra) in enumerate(row_plan(kind, width, s_send, s_recv)):
                    sem = sem0 + i + (0 if down else MAX_PLAN)
                    if act == "recv":
                        from_row, from_col = row - step, col - dist
                        ok = (s == s_recv) & (from_row >= 0) & (from_row < rows) & (from_col >= 0) & (from_col < cols)
                        if extra:
                            ok = ok & (from_col == 0)

                        @pl.when(ok)
                        def _():
                            ref = row_refs(name, pl.ds(dst, count), down, HALO)
                            remote(ref, ref, row_send.at[sem], row_recv.at[sem], from_row, from_col).wait_recv()
                    else:
                        to_row, to_col = row + step, col + dist
                        ok = (s == s_send) & (to_row >= 0) & (to_row < rows) & (to_col >= 0) & (to_col < cols)
                        if extra:
                            ok = ok & (col == 0)

                        @pl.when(ok)
                        def _():
                            copy = remote(row_refs(name, pl.ds(src, count), down, OWN), row_refs(name, pl.ds(dst, count), down, HALO),
                                          row_send.at[sem], row_recv.at[sem], to_row, to_col)
                            if act == "send":
                                copy.start()
                            else:
                                copy.wait_send()

    def send_edges(name, chunk, nch):
        @pl.when(chunk == 0)
        def _():
            row_messages(name, "send", UP)

        @pl.when(chunk == nch - 1)
        def _():
            row_messages(name, "send", DOWN)

    def unit_where(size, source):
        at = lax.broadcasted_iota(jnp.int32, (size, size), 0)
        return (at == source(lax.broadcasted_iota(jnp.int32, (size, size), 1))).astype(F32).astype(BF16)

    eye[...] = unit_where(h, lambda at: at)
    mix[...] = unit_where(n * BLOCK, lambda at: (at & (BLOCK - 1)) * n + (at >> BLOCK.bit_length() - 1))

    def to_rows(value):
        return value.astype(BF16).reshape(BLOCK // 4, 4, n, pair)

    def turn_group(q):
        def turn(i, carry):
            for j in range(UNROLL):
                at = i * UNROLL + j
                block = raw[pl.ds(q, 2), at].reshape(2 * pair, h)
                turned[at] = lax.dot_general(eye[...], block, NT, preferred_element_type=F32).astype(BF16)
            return carry
        loop(n // UNROLL, turn)

        def place(i, carry):
            for j in range(UNROLL):
                at = i * UNROLL + j
                block = turned[:, pl.ds(at * BLOCK, BLOCK), :].reshape(n * BLOCK, 2 * pair)
                moved = dot(mix[...], block)
                for side in BOTH:
                    xs[q + 2 - s + side, pl.ds(1 + at * (BLOCK // 4), BLOCK // 4)] = to_rows(moved[:, side * pair:(side + 1) * pair])
            return carry
        loop(h // BLOCK // UNROLL, place)

    def turn_halo(half):
        slot = jnp.where(is0, 1, PAIRS + 1)
        unit = eye[:hh, :hh]

        def turn(i, carry):
            for j in range(UNROLL):
                at = 2 * (i * UNROLL + j)
                block = xh[half, pl.ds(at, 2)].reshape(2 * pair, hh)
                both = lax.dot_general(unit, block, NT, preferred_element_type=F32).astype(BF16)
                for side in BOTH:
                    turned[at + side, :hh, :pair] = both[:, side * pair:(side + 1) * pair]
            return carry
        loop(n // 2 // UNROLL, turn)

        def place(i, carry):
            blocks = [turned[:, pl.ds((2 * i + j) * BLOCK, BLOCK), :pair].reshape(n * BLOCK, pair) for j in BOTH]
            moved = dot(mix[...], jnp.concatenate(blocks, axis=1))
            for j in BOTH:
                first = 1 + half * (h4 // 2) + (2 * i + j) * (BLOCK // 4)
                xs[slot, pl.ds(first, BLOCK // 4)] = to_rows(moved[:, j * pair:(j + 1) * pair])
            return carry
        loop(hh // BLOCK // 2, place)

    def zero_part(ref, first, size, p):
        ref[pl.ds(first, size), pl.ds(p * c1, c1)] = jnp.zeros((size, c1), BF16)

    def zero_weights():
        for p in BOTH:
            for kh in range(5):
                tap_at = kh * 2 * pair
                used = 2 * p <= kh < 2 * p + 3
                zero_part(w1d, tap_at, c0 if used else 2 * pair, p)
            zero_part(w1c, (1 - p) * k1, 3 * c1, p)
            proj_at = 12 * c1
            zero_part(w1c, proj_at + (1 - p) * pair, pair, p)
            zero_part(w1c, proj_at + p * pair + c0, c0, p)

    zero_weights()
    for copy in x_loads + w1d_loads:
        copy.wait()

    def flat(value):
        return value.reshape(value.shape[0] * n, value.shape[-1])

    def parts(first, count):
        size = count // 2
        return tuple((first + i * size, size) for i in BOTH)

    def dot_nt(lhs, rhs):
        return lax.dot_general(lhs, rhs, NT, preferred_element_type=F32)

    def rows_down(at):
        return (at - 1, 1), (at, 0), (at, 1)

    def own_col(t, width):
        return jnp.where(is0, width - 1 - t, t)

    def phase(width, nch, item):
        def body(at, carry):
            item(lax.div(at, nch) - 1, lax.rem(at, nch))
            return carry
        lax.fori_loop((t_first + 1) * nch, (width + 1) * nch, body, 0)

    def y1_job(t, c):
        k = own_col(t, PAIRS)
        at = 1 + c * ch
        taps = []
        for kh in range(5):
            first, sub = (at - 1, 3) if kh == 0 else (at, kh - 1)
            for side in (1, 2):
                taps.append(flat(xs[k + side, pl.ds(first, ch), sub]))
        acc = dot(jnp.concatenate(taps, axis=1), w1d[...])
        void = last_void & (t == 3)
        for p in BOTH:
            val = relu(acc[:, p * c1:(p + 1) * c1] + b1d[...])
            val = jnp.where(void, 0.0, val)
            y1[k + 2, pl.ds(at, ch), p] = val.astype(BF16).reshape(ch, n, c1)

    def own_group(group, carry):
        turn_group(2 * group)
        return carry
    loop(PAIRS // 2, own_group)
    row_messages("x", "send")
    early = 3 - t_first

    def y1_item(item, carry):
        @pl.when(item == lax.div(3 * early, 2))
        def _():
            row_messages("x", "recv")

        half = item - 2 * early

        @pl.when(half >= 0)
        def _():
            for shift in SHIFTS:
                @pl.when(has_bwd & (s == shift))
                def _():
                    ref = xh.at[half, :, pl.ds(c0, c0)] if shift == 0 else xh.at[half]
                    remote(ref, ref, x_sem.at[half], x_sem.at[2 + half], row, bwd_col).wait_recv()
            turn_halo(half)

        jobs = []
        for j in BOTH:
            at = 2 * item + j
            t = jnp.where(at < 3 * early, lax.div(at, 3) + t_first, jnp.where(half >= 0, 3, at - 3 * early + t_first))
            c = jnp.where(at < 3 * early, lax.rem(at, 3) + 1, jnp.where(half >= 0, at - NCH * early, 0))
            jobs.append((t, c))
        for t, c in jobs:
            y1_job(t, c)
        send_edges("y1", half, 2)

        for t, c in jobs:
            @pl.when((t == 0) & has_fwd)
            def _():
                y_copy(y1, PAIRS, ch, SEM_Y1, True, c, NCH).start()

            @pl.when((t == 3) & has_bwd)
            def _():
                y_copy(y1, PAIRS, ch, SEM_Y1, False, c, NCH).start()
        return carry
    loop(2 * (PAIRS - t_first), y1_item)
    for copy in w1c_loads:
        copy.wait()

    def wait_halo(ref, width, rows_per, sem0, forward, c, nch):
        exists = has_bwd if forward else has_fwd

        @pl.when(exists & (c == 0))
        def _():
            y_recv(ref, width, rows_per, sem0, forward, 0, nch).wait_recv()

        @pl.when(exists & (c < nch - 1))
        def _():
            y_recv(ref, width, rows_per, sem0, forward, c + 1, nch).wait_recv()

    def z1_job(t, c):
        k = own_col(t, PAIRS)
        at = 1 + c * ch
        taps = []
        for first, sub in ((at - 1, 1), (at, 0), (at, 1), (at + 1, 0)):
            for side in AROUND:
                taps.append(flat(y1[k + side, pl.ds(first, ch), sub]))
        for sub in (0, 2):
            taps.append(flat(xs[k + 2, pl.ds(at, ch), sub]))
        acc = dot(jnp.concatenate(taps, axis=1), w1c[...])
        for p in BOTH:
            val = relu(acc[:, p * c1:(p + 1) * c1] + b1c[...])
            z1[k + 3 - s, pl.ds(at, ch), p] = val.astype(BF16).reshape(ch, n, c1)

    extra = -t_first

    def z1_item(item, carry):
        inner = item - extra
        edge = inner - NCH - extra
        more = (inner < 0) | (extra == 1) & (inner == NCH)

        @pl.when(inner == 2)
        def _():
            row_messages("y1", "recv")

        @pl.when(edge >= 0)
        def _():
            wait_halo(y1, PAIRS, ch, SEM_Y1, False, edge, NCH)
            wait_halo(y1, PAIRS, ch, SEM_Y1, True, edge, NCH)

        mid = jnp.where(inner < 2, inner + 1, jnp.where(inner == 2, 0, inner))
        for j in BOTH:
            t = jnp.where(more, -1, jnp.where(edge >= 0, 3 * j, j + 1))
            c = jnp.where(more, jnp.where(inner < 0, j + 1, 3 * j), jnp.where(edge >= 0, edge, mid))
            z1_job(t, c)

        @pl.when((edge >= 0) & has_fwd)
        def _():
            z_copy(z1, PAIRS, ch, SEM_Z1, edge).start()
        return carry
    loop(2 * (NCH + extra), z1_item)
    row_messages("z1", "send")
    for copy in w2d_loads:
        copy.wait()

    def y2_job(t, at, size):
        k = own_col(t, 2)
        taps = []
        for first, sub in rows_down(at):
            for side in range(3):
                taps.append(flat(z1[2 * k + 2 + side, pl.ds(first, size), sub]))
        acc = dot(jnp.concatenate(taps, axis=1), w2d[...])
        val = relu(acc + b2d[...])
        val = jnp.where(last_void & (t == 1), 0.0, val)
        y2[k + 2, pl.ds(at, size)] = val.astype(BF16).reshape(size, n, c2)

    def y2_inner(item, carry):
        t = t_first + lax.div(item, 2)
        late = lax.rem(item, 2)

        @pl.when(item == 1)
        def _():
            row_messages("z1", "recv")

        chunks = (1 + 2 * late, 2 - 2 * late)
        for c in chunks:
            y2_job(t, 1 + c * ch, ch)

        @pl.when((t == 0) & has_fwd)
        def _():
            for c in chunks:
                y_copy(y2, 2, ch, SEM_Y2, True, c, NCH).start()
        return carry
    loop(2 + 2 * extra, y2_inner)

    def y2_edge(c, carry):
        @pl.when(has_bwd)
        def _():
            z_recv(z1, PAIRS, ch, SEM_Z1, c).wait_recv()

        for at, size in parts(1 + c * ch, ch):
            y2_job(jnp.int32(1), at, size)

        send_edges("y2", c, NCH)

        @pl.when(has_bwd)
        def _():
            y_copy(y2, 2, ch, SEM_Y2, False, c, NCH).start()
        return carry
    loop(NCH, y2_edge)
    for copy in w2c_loads:
        copy.wait()

    def z2_job(t, c):
        k = own_col(t, 2)
        at = 1 + c * ch
        taps = []
        for first in (at - 1, at, at + 1):
            for side in AROUND:
                taps.append(flat(y2[k + side, pl.ds(first, ch)]))
        taps.append(flat(z1[2 * k + 3, pl.ds(at, ch), 0]))
        acc = dot(jnp.concatenate(taps, axis=1), w2c[...])
        val = relu(acc + b2c[...]).astype(BF16).reshape(ch // 2, 2, n, c2)
        z2[k + 3 - s, pl.ds(1 + c * (ch // 2), ch // 2)] = val

    row_messages("y2", "recv")

    def z2_item(item, carry):
        c = item - 2 * extra

        @pl.when(c >= 0)
        def _():
            wait_halo(y2, 2, ch, SEM_Y2, False, c, NCH)
            wait_halo(y2, 2, ch, SEM_Y2, True, c, NCH)

        for j in BOTH:
            z2_job(jnp.where(c < 0, -1, j), jnp.where(c < 0, 2 * item + j, c))

        @pl.when((c >= 0) & has_fwd)
        def _():
            z_copy(z2, 2, ch // 2, SEM_Z2, c).start()
        return carry
    loop(NCH + 2 * extra, z2_item)
    row_messages("z2", "send")

    for copy in w3d_loads:
        copy.wait()

    def y3_item(t, c):
        k = t

        @pl.when((t == t_first) & (c == 0))
        def _():
            row_messages("z2", "recv")

        @pl.when((t == 0) & has_bwd)
        def _():
            for j in range(NCH // NCH3):
                z_recv(z2, 2, ch // 2, SEM_Z2, c * (NCH // NCH3) + j).wait_recv()

        for at, size in parts(1 + c * ch3, ch3):
            acc = b3d[...]
            tap = 0
            for first, sub in rows_down(at):
                for side in range(3):
                    acc = acc + dot_nt(flat(z2[2 * k + 2 + side, pl.ds(first, size), sub]), w3r[tap])
                    tap += 1
            val = jnp.where(last_void & (t == 0), 0.0, relu(acc))
            y3[k + 2, pl.ds(at, size)] = val.astype(BF16).reshape(size, n, c3)

        @pl.when(t == 0)
        def _():
            send_edges("y3", c, NCH3)

        @pl.when((t == 0) & has_fwd)
        def _():
            y_copy(y3, 1, ch3, SEM_Y3, True, c, NCH3).start()

        @pl.when((t == 0) & has_bwd)
        def _():
            y_copy(y3, 1, ch3, SEM_Y3, False, c, NCH3).start()
    phase(1, NCH3, y3_item)
    for copy in w3c_loads:
        copy.wait()

    ships = (s == 1) & has_bwd

    def ship(c):
        part = pl.ds(c * ch3, ch3)
        return remote(zo.at[1, part], out_hbm.at[part], out_sem.at[c], out_sem.at[NCH3 + c], row, bwd_col)

    def ship_recv(c):
        part = pl.ds(c * ch3, ch3)
        return remote(zo.at[1, part], out_hbm.at[part], out_sem.at[c], out_sem.at[NCH3 + c], row, fwd_col)

    keep = jnp.where(is0, 1, 0)

    def put(c):
        part = pl.ds(c * ch3, ch3)
        return pltpu.make_async_copy(zo.at[keep, part], out_hbm.at[part], out_sem.at[2 * NCH3 + c])

    def z3_item(t, c):
        k = t

        @pl.when((t == t_first) & (c == 0))
        def _():
            row_messages("y3", "recv")

        @pl.when(t == 0)
        def _():
            wait_halo(y3, 1, ch3, SEM_Y3, False, c, NCH3)
            wait_halo(y3, 1, ch3, SEM_Y3, True, c, NCH3)

        for at, size in parts(1 + c * ch3, ch3):
            acc = dot_nt(flat(z2[2 * k + 3, pl.ds(at, size), 0]), wp3r[...]) + b3c[...]
            tap = 0
            for first in (at - 1, at, at + 1):
                for side in AROUND:
                    acc = acc + dot(flat(y3[k + side, pl.ds(first, size)]), w3c[tap])
                    tap += 1
            zo[k + 1, pl.ds(at - 1, size)] = relu(acc).astype(BF16).reshape(size, n, c3)

        @pl.when((t == 0) & ships)
        def _():
            ship(c).start()

        @pl.when(((t == 0) & is0) | (t == -1))
        def _():
            put(c).start()
    phase(1, NCH3, z3_item)

    for shift in SHIFTS:
        @pl.when(has_fwd & (s == shift))
        def _():
            for half in BOTH:
                x_copy(shift, half).wait_send()

    def drain(c, carry):
        @pl.when(has_fwd)
        def _():
            y_copy(y1, PAIRS, ch, SEM_Y1, True, c, NCH).wait_send()
            z_copy(z1, PAIRS, ch, SEM_Z1, c).wait_send()
            y_copy(y2, 2, ch, SEM_Y2, True, c, NCH).wait_send()
            z_copy(z2, 2, ch // 2, SEM_Z2, c).wait_send()

        @pl.when(has_bwd)
        def _():
            y_copy(y1, PAIRS, ch, SEM_Y1, False, c, NCH).wait_send()
            y_copy(y2, 2, ch, SEM_Y2, False, c, NCH).wait_send()
        return carry
    loop(NCH, drain)

    def drain3(c, carry):
        @pl.when(has_fwd)
        def _():
            y_copy(y3, 1, ch3, SEM_Y3, True, c, NCH3).wait_send()

        @pl.when(has_bwd)
        def _():
            y_copy(y3, 1, ch3, SEM_Y3, False, c, NCH3).wait_send()

        @pl.when(ships)
        def _():
            ship(c).wait_send()

        @pl.when((s == 1) & has_fwd)
        def _():
            ship_recv(c).wait_recv()

        @pl.when(is0 | first_extra)
        def _():
            put(c).wait()
        return carry
    loop(NCH3, drain3)
    for name in ROW_SEM:
        row_messages(name, "sent")


def solution(mesh):
    rows = mesh.shape["row"]
    cols = mesh.shape["col"]
    tile_spec = P("batch", "row", "col")

    def local_blocks(x, w1d, b1d, w1c, b1c, wp1, w2d, b2d, w2c, b2c, wp2, w3d, b3d, w3c, b3c, wp3):
        n, h, w, c0 = x.shape
        c1, c2, c3 = w1d.shape[3], w2d.shape[3], w3d.shape[3]
        h4, h8 = h // 4, h // 8
        dims = (n, h, c0, c1, c2, c3, rows, cols)
        pair = 2 * c0
        xt = jnp.moveaxis(x, 1, 3).reshape(n, PAIRS, pair, h)
        args = (xt, w1d.reshape(3, 3 * c0, c1), w1c.reshape(9 * c1, c1), wp1, w2d.reshape(9 * c1, c2), w2c.reshape(9 * c2, c2), wp2,
                jnp.swapaxes(w3d.reshape(9, c2, c3), 1, 2), w3c.reshape(9, c3, c3), wp3.T,
                b1d, b1c, b2d, b2c, b3d, b3c)
        vm = pltpu.VMEM
        dma = pltpu.SemaphoreType.DMA
        flops = 2 * n * h * w * c1 * 7 * (c0 + c1)
        out = pl.pallas_call(
            functools.partial(kernel, dims),
            out_shape=jax.ShapeDtypeStruct((h8, n, c3), BF16),
            in_specs=[pl.BlockSpec(memory_space=pl.ANY)] * len(args),
            out_specs=pl.BlockSpec(memory_space=pl.ANY),
            scratch_shapes=[
                vm(shape, BF16) for shape in (
                    (PAIRS, n, pair, h), (2, n, pair, h // 2), (n, h, 2 * pair), (h, h), (n * BLOCK, n * BLOCK),
                    (6, h4 + 1, 4, n, pair), (7, h4 + 2, 2, n, c1), (7, h4 + 1, 2, n, c1),
                    (5, h4 + 2, n, c2), (5, h8 + 1, 2, n, c2), (4, h8 + 2, n, c3), (2, h8, n, c3),
                    (10 * pair, 2 * c1), (12 * c1 + 2 * pair, 2 * c1), (9 * c1, c2), (9 * c2 + c1, c2),
                    (9, c3, c2), (9, c3, c3), (c3, c2))
            ] + [vm((1, width), F32) for width in (c1, c1, c2, c2, c3, c3)] + [
                dma((count,)) for count in (32, 4, 10 * NCH, 10 * NCH, 12 * MAX_PLAN, 12 * MAX_PLAN, 3 * NCH3)],
            compiler_params=pltpu.CompilerParams(collective_id=0, has_side_effects=True, vmem_limit_bytes=63 * 1024 * 1024),
            cost_estimate=pl.CostEstimate(flops=flops, bytes_accessed=16 * 1024 * 1024, transcendentals=0),
        )(*args)
        return jnp.swapaxes(out, 0, 1).reshape(n, h8, 1, c3)

    return jax.shard_map(local_blocks, mesh=mesh, in_specs=(tile_spec,) + (P(),) * 15, out_specs=tile_spec, check_vma=False)
```

```python
import functools

import jax
import jax.numpy as jnp
from jax import lax
from jax.experimental import pallas as pl
from jax.experimental.pallas import tpu as pltpu
from jax.sharding import PartitionSpec as P

BF16 = jnp.bfloat16
F32 = jnp.float32
SHIFTS = (0, 1)
NCH = 4
NCH3 = 2
PAIRS = 4
MAX_PLAN = 5
BLOCK = 16
UNROLL = 4
OWN, HALO = BOTH = range(2)
AROUND = (1, 2, 3)
UP, DOWN = (False,), (True,)
NT = (((1,), (1,)), ((), ()))


def relu(value):
    return jnp.maximum(value, 0.0)


def loop(count, body):
    lax.fori_loop(0, count, body, 0)


def row_plan(kind, width, s_send, s_recv):
    if kind == "x":
        own = (0, width - 1)
        need = (-1, width - 1) if s_recv == 0 else (0, width)
        src_at, dst_at = 2 - s_send, 2 - s_recv
    elif kind == "y":
        own = (s_send, width - 1 + s_send)
        need = (s_recv - 1, s_recv + width)
        src_at, dst_at = 2 - s_send, 2 - s_recv
    else:
        own = (s_send, width - 1 + s_send)
        need = (-1, width - 1) if s_recv == 0 else (0, width + 1)
        src_at, dst_at = 3 - 2 * s_send, 3 - 2 * s_recv
    plan = []
    for dist in range(-2, 3):
        lo = max(own[0], width * dist + need[0])
        hi = min(own[1], width * dist + need[1])
        if lo <= hi:
            plan.append((dist, lo + src_at, lo - width * dist + dst_at, hi - lo + 1, False))
        if kind != "x" and s_send == 1 and s_recv == 0 and dist >= 0 and need[0] + width * dist <= 0 <= need[1] + width * dist:
            plan.append((dist, src_at, dst_at - width * dist, 1, True))
    return plan


def kernel(dims, x_hbm, w1d_h, w1c_h, wp1_h, w2d_h, w2c_h, wp2_h, w3d_h, w3c_h, wp3_h, b1d_h, b1c_h, b2d_h, b2c_h, b3d_h, b3c_h, out_hbm,
           raw, xh, turned, eye, mix, xs, y1, z1, y2, z2, y3, zo, w1d, w1c, w2d, w2c, w3r, w3c, wp3r,
           b1d, b1c, b2d, b2c, b3d, b3c, load_sem, x_sem, col_send, col_recv, row_send, row_recv, out_sem):
    n, h, c0, c1, c2, c3, rows, cols = dims
    h4, h8 = h // 4, h // 8
    ch, ch3 = h4 // NCH, h8 // NCH3
    hh = h // 2
    row = lax.axis_index("row")
    col = lax.axis_index("col")
    s = lax.rem(row, 2)
    is0 = s == 0
    first_extra = (s == 1) & (col == 0)
    last_void = (s == 1) & (col == cols - 1)
    t_first = jnp.where(first_extra, -1, 0)
    fwd_col = jnp.where(is0, col + 1, col - 1)
    bwd_col = jnp.where(is0, col - 1, col + 1)
    has_fwd = (fwd_col >= 0) & (fwd_col < cols)
    has_bwd = (bwd_col >= 0) & (bwd_col < cols)

    load_count = []

    def load(src, dst):
        load_count.append(dst)
        return pltpu.make_async_copy(src, dst, load_sem.at[len(load_count) - 1])

    k1, k2 = 9 * c1, 9 * c2
    pair = 2 * c0
    x_loads = [load(x_hbm.at[:, q], raw.at[q]) for q in range(PAIRS)]
    w1d_loads = [load(b1d_h, b1d.at[0]), load(b1c_h, b1c.at[0])]
    w1c_loads = []
    for p in BOTH:
        lanes = pl.ds(p * c1, c1)
        for kh in range(3):
            w1d_loads.append(load(w1d_h.at[kh], w1d.at[pl.ds((kh + 2 * p) * 2 * pair + c0, 3 * c0), lanes]))
        w1c_loads.append(load(w1c_h, w1c.at[pl.ds(p * 3 * c1, k1), lanes]))
        w1c_loads.append(load(wp1_h, w1c.at[pl.ds(12 * c1 + p * pair, c0), lanes]))
    w2d_loads = [load(w2d_h, w2d), load(b2d_h, b2d.at[0])]
    w2c_loads = [load(w2c_h, w2c.at[pl.ds(0, k2)]), load(wp2_h, w2c.at[pl.ds(k2, c1)]), load(b2c_h, b2c.at[0])]
    w3d_loads = [load(w3d_h, w3r), load(b3d_h, b3d.at[0]), load(wp3_h, wp3r)]
    w3c_loads = [load(w3c_h, w3c), load(b3c_h, b3c.at[0])]
    for copy in x_loads:
        copy.start()

    def row_refs(name, slots, down, side):
        ref = refs[name]
        last = ref.shape[1] - (2 if ROW_SEM[name][0] == "y" else 1)
        own_at, halo_at = (last, 0) if down else (1, last + 1)
        at = own_at if side == OWN else halo_at
        subs = 1 if len(ref.shape) == 4 else ref.shape[2]
        if subs == 1:
            return ref.at[slots, at]
        return ref.at[slots, at, subs - 1 if down else 0]

    refs = dict(x=xs, y1=y1, z1=z1, y2=y2, z2=z2, y3=y3)
    ROW_SEM = {}
    for name, kind, width in (("x", "x", PAIRS), ("y1", "y", PAIRS), ("z1", "z", PAIRS), ("y2", "y", 2), ("z2", "z", 2), ("y3", "y", 1)):
        ROW_SEM[name] = (kind, width, 2 * MAX_PLAN * len(ROW_SEM))

    def directions(name):
        return (True, False) if ROW_SEM[name][0] == "y" else (True,)

    def dot(lhs, rhs):
        return jnp.dot(lhs, rhs, preferred_element_type=F32)

    def zero_slot(ref, idx):
        ref[idx] = jnp.zeros(ref.shape[1:], ref.dtype)

    def dot(lhs, rhs):
        return jnp.dot(lhs, rhs, preferred_element_type=F32)

    def zero_slot(ref, idx):
        def body(i, carry):
            ref[idx, i] = jnp.zeros(ref.shape[2:], ref.dtype)
            return carry
        loop(ref.shape[1], body)

    for name in ROW_SEM:
        for down in directions(name):
            edge = row_refs(name, slice(None), down, HALO)
            edge[...] = jnp.zeros(edge.shape, BF16)

    @pl.when(col == 0)
    def _():
        for ref in (y1, y2, y3):
            zero_slot(ref, 1 - s)
        for ref in (z1, z2):
            zero_slot(ref, 2 - 2 * s)

    @pl.when(first_extra)
    def _():
        zero_slot(xs, 0)

    @pl.when(col == cols - 1)
    def _():
        for ref in (y1, y2, y3):
            zero_slot(ref, ref.shape[0] - 1)

    @pl.when(is0 | jnp.logical_not(has_bwd))
    def _():
        def body(i, carry):
            xh[0, i] = jnp.zeros((2 * c0, hh), BF16)
            xh[1, i] = jnp.zeros((2 * c0, hh), BF16)
            return carry
        loop(n, body)

    barrier = pltpu.get_barrier_semaphore()
    around = 0
    for step in range(-1, 2):
        for dist in range(-2, 3):
            near_row, near_col = row + step, col + dist
            ok = (near_row >= 0) & (near_row < rows) & (near_col >= 0) & (near_col < cols)
            around = around + ok.astype(jnp.int32)

            @pl.when(ok)
            def _():
                pl.semaphore_signal(barrier, inc=1, device_id={"row": near_row, "col": near_col}, device_id_type=pl.DeviceIdType.MESH)

    def unit_where(size, source):
        at = lax.broadcasted_iota(jnp.int32, (size, size), 0)
        return (at == source(lax.broadcasted_iota(jnp.int32, (size, size), 1))).astype(F32).astype(BF16)

    eye[...] = unit_where(h, lambda at: at)
    mix[...] = unit_where(n * BLOCK, lambda at: (at & (BLOCK - 1)) * n + (at >> BLOCK.bit_length() - 1))

    def zero_part(ref, first, size, p):
        ref[pl.ds(first, size), pl.ds(p * c1, c1)] = jnp.zeros((size, c1), BF16)

    for p in BOTH:
        for kh in range(5):
            tap_at = kh * 2 * pair
            used = 2 * p <= kh < 2 * p + 3
            zero_part(w1d, tap_at, c0 if used else 2 * pair, p)
        zero_part(w1c, (1 - p) * k1, 3 * c1, p)
        proj_at = 12 * c1
        zero_part(w1c, proj_at + (1 - p) * pair, pair, p)
        zero_part(w1c, proj_at + p * pair + c0, c0, p)
    pl.semaphore_wait(barrier, around)

    def remote(src, dst, send_sem, recv_sem, to_row, to_col):
        return pltpu.make_async_remote_copy(src_ref=src, dst_ref=dst, send_sem=send_sem, recv_sem=recv_sem,
                                            device_id={"row": to_row, "col": to_col}, device_id_type=pl.DeviceIdType.MESH)

    def x_copy(shift, half):
        lanes = pl.ds(half * hh, hh)
        if shift == 0:
            src, dst = x_hbm.at[:, 3, pl.ds(c0, c0), lanes], xh.at[half, :, pl.ds(c0, c0)]
        else:
            src, dst = x_hbm.at[:, 0, :, lanes], xh.at[half]
        return remote(src, dst, x_sem.at[half], x_sem.at[2 + half], row, fwd_col)

    for shift in SHIFTS:
        @pl.when(has_fwd & (s == shift))
        def _():
            for half in BOTH:
                x_copy(shift, half).start()

    def y_copy(ref, width, rows_per, sem0, forward, chunk, nch):
        to_right = is0 if forward else jnp.logical_not(is0)
        src_slot = jnp.where(to_right, width + 1, 2)
        dst_slot = jnp.where(to_right, 1, width + 2)
        part = pl.ds(1 + chunk * rows_per, rows_per)
        sem = sem0 + (0 if forward else nch) + chunk
        return remote(ref.at[src_slot, part], ref.at[dst_slot, part], col_send.at[sem], col_recv.at[sem], row, fwd_col if forward else bwd_col)

    def y_recv(ref, width, rows_per, sem0, forward, chunk, nch):
        to_right = is0 if forward else jnp.logical_not(is0)
        dst_slot = jnp.where(to_right, 1, width + 2)
        part = pl.ds(1 + chunk * rows_per, rows_per)
        sem = sem0 + (0 if forward else nch) + chunk
        return remote(ref.at[dst_slot, part], ref.at[dst_slot, part], col_send.at[sem], col_recv.at[sem], row, bwd_col if forward else fwd_col)

    def z_copy(ref, width, rows_per, sem0, chunk):
        src_slot = jnp.where(is0, width + 2, 2)
        dst_slot = jnp.where(is0, 2, width + 2)
        part = pl.ds(1 + chunk * rows_per, rows_per)
        sem = sem0 + chunk
        return remote(ref.at[src_slot, part], ref.at[dst_slot, part], col_send.at[sem], col_recv.at[sem], row, fwd_col)

    def z_recv(ref, width, rows_per, sem0, chunk):
        dst_slot = jnp.where(is0, 2, width + 2)
        part = pl.ds(1 + chunk * rows_per, rows_per)
        sem = sem0 + chunk
        return remote(ref.at[dst_slot, part], ref.at[dst_slot, part], col_send.at[sem], col_recv.at[sem], row, bwd_col)

    SEM_Y1, SEM_Z1, SEM_Y2, SEM_Z2, SEM_Y3 = (i * 2 * NCH for i in range(5))

    def row_messages(name, act, ways=None):
        kind, width, sem0 = ROW_SEM[name]
        for down in ways or directions(name):
            for s_send, s_recv in zip(SHIFTS, reversed(SHIFTS)):
                step = 1 if down else -1
                for i, (dist, src, dst, count, extra) in enumerate(row_plan(kind, width, s_send, s_recv)):
                    sem = sem0 + i + (0 if down else MAX_PLAN)
                    if act == "recv":
                        from_row, from_col = row - step, col - dist
                        ok = (s == s_recv) & (from_row >= 0) & (from_row < rows) & (from_col >= 0) & (from_col < cols)
                        if extra:
                            ok = ok & (from_col == 0)

                        @pl.when(ok)
                        def _():
                            ref = row_refs(name, pl.ds(dst, count), down, HALO)
                            remote(ref, ref, row_send.at[sem], row_recv.at[sem], from_row, from_col).wait_recv()
                    else:
                        to_row, to_col = row + step, col + dist
                        ok = (s == s_send) & (to_row >= 0) & (to_row < rows) & (to_col >= 0) & (to_col < cols)
                        if extra:
                            ok = ok & (col == 0)

                        @pl.when(ok)
                        def _():
                            copy = remote(row_refs(name, pl.ds(src, count), down, OWN), row_refs(name, pl.ds(dst, count), down, HALO),
                                          row_send.at[sem], row_recv.at[sem], to_row, to_col)
                            if act == "send":
                                copy.start()
                            else:
                                copy.wait_send()

    def send_edges(name, chunk, nch):
        @pl.when(chunk == 0)
        def _():
            row_messages(name, "send", UP)

        @pl.when(chunk == nch - 1)
        def _():
            row_messages(name, "send", DOWN)

    def to_rows(value):
        return value.astype(BF16).reshape(BLOCK // 4, 4, n, pair)

    def turn_group(q):
        def turn(i, carry):
            for j in range(UNROLL):
                at = i * UNROLL + j
                block = raw[pl.ds(q, 2), at].reshape(2 * pair, h)
                turned[at] = lax.dot_general(eye[...], block, NT, preferred_element_type=F32).astype(BF16)
            return carry
        loop(n // UNROLL, turn)

        def place(i, carry):
            for j in range(UNROLL):
                at = i * UNROLL + j
                block = turned[:, pl.ds(at * BLOCK, BLOCK), :].reshape(n * BLOCK, 2 * pair)
                moved = dot(mix[...], block)
                for side in BOTH:
                    xs[q + 2 - s + side, pl.ds(1 + at * (BLOCK // 4), BLOCK // 4)] = to_rows(moved[:, side * pair:(side + 1) * pair])
            return carry
        loop(h // BLOCK // UNROLL, place)

    def turn_halo(half):
        slot = jnp.where(is0, 1, PAIRS + 1)
        unit = eye[:hh, :hh]

        def turn(i, carry):
            for j in range(UNROLL):
                at = 2 * (i * UNROLL + j)
                block = xh[half, pl.ds(at, 2)].reshape(2 * pair, hh)
                both = lax.dot_general(unit, block, NT, preferred_element_type=F32).astype(BF16)
                for side in BOTH:
                    turned[at + side, :hh, :pair] = both[:, side * pair:(side + 1) * pair]
            return carry
        loop(n // 2 // UNROLL, turn)

        def place(i, carry):
            blocks = [turned[:, pl.ds((2 * i + j) * BLOCK, BLOCK), :pair].reshape(n * BLOCK, pair) for j in BOTH]
            moved = dot(mix[...], jnp.concatenate(blocks, axis=1))
            for j in BOTH:
                first = 1 + half * (h4 // 2) + (2 * i + j) * (BLOCK // 4)
                xs[slot, pl.ds(first, BLOCK // 4)] = to_rows(moved[:, j * pair:(j + 1) * pair])
            return carry
        loop(hh // BLOCK // 2, place)

    for copy in w1d_loads + w1c_loads + w2d_loads + w2c_loads + w3d_loads + w3c_loads:
        copy.start()
    for copy in x_loads:
        copy.wait()

    def flat(value):
        return value.reshape(value.shape[0] * n, value.shape[-1])

    def parts(first, count):
        size = count // 2
        return tuple((first + i * size, size) for i in BOTH)

    def dot_nt(lhs, rhs):
        return lax.dot_general(lhs, rhs, NT, preferred_element_type=F32)

    def rows_down(at):
        return (at - 1, 1), (at, 0), (at, 1)

    def own_col(t, width):
        return jnp.where(is0, width - 1 - t, t)

    def phase(width, nch, item):
        def body(at, carry):
            item(lax.div(at, nch) - 1, lax.rem(at, nch))
            return carry
        lax.fori_loop((t_first + 1) * nch, (width + 1) * nch, body, 0)

    def y1_job(t, c):
        k = own_col(t, PAIRS)
        at = 1 + c * ch
        taps = []
        for kh in range(5):
            first, sub = (at - 1, 3) if kh == 0 else (at, kh - 1)
            for side in (1, 2):
                taps.append(flat(xs[k + side, pl.ds(first, ch), sub]))
        acc = dot(jnp.concatenate(taps, axis=1), w1d[...])
        void = last_void & (t == 3)
        for p in BOTH:
            val = relu(acc[:, p * c1:(p + 1) * c1] + b1d[...])
            val = jnp.where(void, 0.0, val)
            y1[k + 2, pl.ds(at, ch), p] = val.astype(BF16).reshape(ch, n, c1)

    def own_group(group, carry):
        turn_group(2 * group)
        return carry
    loop(PAIRS // 2, own_group)
    row_messages("x", "send")
    for copy in w1d_loads:
        copy.wait()
    early = 3 - t_first

    def y1_item(item, carry):
        @pl.when(item == lax.div(3 * early, 2))
        def _():
            row_messages("x", "recv")

        half = item - 2 * early

        @pl.when(half >= 0)
        def _():
            for shift in SHIFTS:
                @pl.when(has_bwd & (s == shift))
                def _():
                    ref = xh.at[half, :, pl.ds(c0, c0)] if shift == 0 else xh.at[half]
                    remote(ref, ref, x_sem.at[half], x_sem.at[2 + half], row, bwd_col).wait_recv()
            turn_halo(half)

        jobs = []
        for j in BOTH:
            at = 2 * item + j
            t = jnp.where(at < 3 * early, lax.div(at, 3) + t_first, jnp.where(half >= 0, 3, at - 3 * early + t_first))
            c = jnp.where(at < 3 * early, lax.rem(at, 3) + 1, jnp.where(half >= 0, at - NCH * early, 0))
            jobs.append((t, c))
        for t, c in jobs:
            y1_job(t, c)
        send_edges("y1", half, 2)

        for t, c in jobs:
            @pl.when((t == 0) & has_fwd)
            def _():
                y_copy(y1, PAIRS, ch, SEM_Y1, True, c, NCH).start()

            @pl.when((t == 3) & has_bwd)
            def _():
                y_copy(y1, PAIRS, ch, SEM_Y1, False, c, NCH).start()
        return carry
    loop(2 * (PAIRS - t_first), y1_item)
    for copy in w1c_loads:
        copy.wait()

    def wait_halo(ref, width, rows_per, sem0, forward, half, nch):
        exists = has_bwd if forward else has_fwd

        @pl.when(exists & (half == 0))
        def _():
            for c in range(nch - nch // 4):
                y_recv(ref, width, rows_per, sem0, forward, c, nch).wait_recv()

        @pl.when(exists & (half == 1))
        def _():
            for c in range(nch - nch // 4, nch):
                y_recv(ref, width, rows_per, sem0, forward, c, nch).wait_recv()

    def z1_job(t, c):
        k = own_col(t, PAIRS)
        at = 1 + c * ch
        taps = []
        for first, sub in ((at - 1, 1), (at, 0), (at, 1), (at + 1, 0)):
            for side in AROUND:
                taps.append(flat(y1[k + side, pl.ds(first, ch), sub]))
        for sub in (0, 2):
            taps.append(flat(xs[k + 2, pl.ds(at, ch), sub]))
        acc = dot(jnp.concatenate(taps, axis=1), w1c[...])
        for p in BOTH:
            val = relu(acc[:, p * c1:(p + 1) * c1] + b1c[...])
            z1[k + 3 - s, pl.ds(at, ch), p] = val.astype(BF16).reshape(ch, n, c1)

    extra = -t_first

    def z1_item(item, carry):
        inner = item - extra
        edge = inner - NCH - extra
        more = (inner < 0) | (extra == 1) & (inner == NCH)

        @pl.when(inner == 2)
        def _():
            row_messages("y1", "recv")

        half = lax.rem(edge, 2)
        far = edge >= 2

        @pl.when((edge >= 0) & (edge < 2))
        def _():
            wait_halo(y1, PAIRS, ch, SEM_Y1, False, half, NCH)

        @pl.when(far)
        def _():
            wait_halo(y1, PAIRS, ch, SEM_Y1, True, half, NCH)

        mid = jnp.where(inner < 2, inner + 1, jnp.where(inner == 2, 0, inner))
        edge_col = jnp.where(far, 3, 0)
        for j in BOTH:
            t = jnp.where(more, -1, jnp.where(edge >= 0, edge_col, j + 1))
            c = jnp.where(more, jnp.where(inner < 0, j + 1, 3 * j), jnp.where(edge >= 0, 2 * half + j, mid))
            z1_job(t, c)

        @pl.when((edge >= 0) & (edge < 2) & has_fwd)
        def _():
            for j in BOTH:
                z_copy(z1, PAIRS, ch, SEM_Z1, 2 * half + j).start()
        return carry
    loop(2 * (NCH + extra), z1_item)
    row_messages("z1", "send")
    for copy in w2d_loads:
        copy.wait()

    def y2_job(t, at, size):
        k = own_col(t, 2)
        taps = []
        for first, sub in rows_down(at):
            for side in range(3):
                taps.append(flat(z1[2 * k + 2 + side, pl.ds(first, size), sub]))
        acc = dot(jnp.concatenate(taps, axis=1), w2d[...])
        val = relu(acc + b2d[...])
        val = jnp.where(last_void & (t == 1), 0.0, val)
        y2[k + 2, pl.ds(at, size)] = val.astype(BF16).reshape(size, n, c2)

    def y2_inner(item, carry):
        t = t_first + lax.div(item, 2)
        late = lax.rem(item, 2)

        @pl.when(item == 1)
        def _():
            row_messages("z1", "recv")

        chunks = (1 + 2 * late, 2 - 2 * late)
        for c in chunks:
            y2_job(t, 1 + c * ch, ch)

        @pl.when((t == 0) & has_fwd)
        def _():
            for c in chunks:
                y_copy(y2, 2, ch, SEM_Y2, True, c, NCH).start()
        return carry
    loop(2 + 2 * extra, y2_inner)

    def y2_edge(c, carry):
        @pl.when(has_bwd)
        def _():
            z_recv(z1, PAIRS, ch, SEM_Z1, c).wait_recv()

        for at, size in parts(1 + c * ch, ch):
            y2_job(jnp.int32(1), at, size)

        send_edges("y2", c, NCH)

        @pl.when(has_bwd)
        def _():
            y_copy(y2, 2, ch, SEM_Y2, False, c, NCH).start()
        return carry
    loop(NCH, y2_edge)
    for copy in w2c_loads:
        copy.wait()

    def z2_job(t, c):
        k = own_col(t, 2)
        at = 1 + c * ch
        taps = []
        for first in (at - 1, at, at + 1):
            for side in AROUND:
                taps.append(flat(y2[k + side, pl.ds(first, ch)]))
        taps.append(flat(z1[2 * k + 3, pl.ds(at, ch), 0]))
        acc = dot(jnp.concatenate(taps, axis=1), w2c[...])
        val = relu(acc + b2c[...]).astype(BF16).reshape(ch // 2, 2, n, c2)
        z2[k + 3 - s, pl.ds(1 + c * (ch // 2), ch // 2)] = val

    row_messages("y2", "recv")

    def z2_item(item, carry):
        edge = item - 2 * extra
        half = lax.rem(item, 2)
        near = (edge >= 0) & (edge < 2)

        @pl.when(near)
        def _():
            wait_halo(y2, 2, ch, SEM_Y2, False, half, NCH)

        @pl.when(edge >= 2)
        def _():
            wait_halo(y2, 2, ch, SEM_Y2, True, half, NCH)

        for j in BOTH:
            z2_job(lax.div(edge + 2, 2) - 1, 2 * half + j)

        @pl.when(near & has_fwd)
        def _():
            for j in BOTH:
                z_copy(z2, 2, ch // 2, SEM_Z2, 2 * half + j).start()
        return carry
    loop(NCH + 2 * extra, z2_item)
    row_messages("z2", "send")

    for copy in w3d_loads:
        copy.wait()

    def y3_item(t, c):
        k = t

        @pl.when((t == t_first) & (c == 0))
        def _():
            row_messages("z2", "recv")

        @pl.when((t == 0) & has_bwd)
        def _():
            for j in range(NCH // NCH3):
                z_recv(z2, 2, ch // 2, SEM_Z2, c * (NCH // NCH3) + j).wait_recv()

        for at, size in parts(1 + c * ch3, ch3):
            acc = b3d[...]
            tap = 0
            for first, sub in rows_down(at):
                for side in range(3):
                    acc = acc + dot_nt(flat(z2[2 * k + 2 + side, pl.ds(first, size), sub]), w3r[tap])
                    tap += 1
            val = jnp.where(last_void & (t == 0), 0.0, relu(acc))
            y3[k + 2, pl.ds(at, size)] = val.astype(BF16).reshape(size, n, c3)

        @pl.when(t == 0)
        def _():
            send_edges("y3", c, NCH3)

        @pl.when((t == 0) & has_fwd)
        def _():
            y_copy(y3, 1, ch3, SEM_Y3, True, c, NCH3).start()

        @pl.when((t == 0) & has_bwd)
        def _():
            y_copy(y3, 1, ch3, SEM_Y3, False, c, NCH3).start()
    phase(1, NCH3, y3_item)
    for copy in w3c_loads:
        copy.wait()

    ships = (s == 1) & has_bwd

    def ship(c):
        part = pl.ds(c * ch3, ch3)
        return remote(zo.at[1, part], out_hbm.at[part], out_sem.at[c], out_sem.at[NCH3 + c], row, bwd_col)

    def ship_recv(c):
        part = pl.ds(c * ch3, ch3)
        return remote(zo.at[1, part], out_hbm.at[part], out_sem.at[c], out_sem.at[NCH3 + c], row, fwd_col)

    keep = jnp.where(is0, 1, 0)

    def put(c):
        part = pl.ds(c * ch3, ch3)
        return pltpu.make_async_copy(zo.at[keep, part], out_hbm.at[part], out_sem.at[2 * NCH3 + c])

    def z3_item(t, c):
        k = t

        @pl.when((t == t_first) & (c == 0))
        def _():
            row_messages("y3", "recv")

        @pl.when((t == 0) & (c == 0))
        def _():
            for forward, exists in ((False, has_fwd), (True, has_bwd)):
                @pl.when(exists)
                def _():
                    for chunk in range(NCH3):
                        y_recv(y3, 1, ch3, SEM_Y3, forward, chunk, NCH3).wait_recv()

        for at, size in parts(1 + c * ch3, ch3):
            acc = dot_nt(flat(z2[2 * k + 3, pl.ds(at, size), 0]), wp3r[...]) + b3c[...]
            tap = 0
            for first in (at - 1, at, at + 1):
                for side in AROUND:
                    acc = acc + dot(flat(y3[k + side, pl.ds(first, size)]), w3c[tap])
                    tap += 1
            zo[k + 1, pl.ds(at - 1, size)] = relu(acc).astype(BF16).reshape(size, n, c3)

        @pl.when((t == 0) & ships)
        def _():
            ship(c).start()

        @pl.when(((t == 0) & is0) | (t == -1))
        def _():
            put(c).start()
    phase(1, NCH3, z3_item)

    for shift in SHIFTS:
        @pl.when(has_fwd & (s == shift))
        def _():
            for half in BOTH:
                x_copy(shift, half).wait_send()

    def drain(c, carry):
        @pl.when(has_fwd)
        def _():
            y_copy(y1, PAIRS, ch, SEM_Y1, True, c, NCH).wait_send()
            z_copy(z1, PAIRS, ch, SEM_Z1, c).wait_send()
            y_copy(y2, 2, ch, SEM_Y2, True, c, NCH).wait_send()
            z_copy(z2, 2, ch // 2, SEM_Z2, c).wait_send()

        @pl.when(has_bwd)
        def _():
            y_copy(y1, PAIRS, ch, SEM_Y1, False, c, NCH).wait_send()
            y_copy(y2, 2, ch, SEM_Y2, False, c, NCH).wait_send()
        return carry
    loop(NCH, drain)

    def drain3(c, carry):
        @pl.when(has_fwd)
        def _():
            y_copy(y3, 1, ch3, SEM_Y3, True, c, NCH3).wait_send()

        @pl.when(has_bwd)
        def _():
            y_copy(y3, 1, ch3, SEM_Y3, False, c, NCH3).wait_send()

        @pl.when(ships)
        def _():
            ship(c).wait_send()

        @pl.when((s == 1) & has_fwd)
        def _():
            ship_recv(c).wait_recv()

        @pl.when(is0 | first_extra)
        def _():
            put(c).wait()
        return carry
    loop(NCH3, drain3)
    for name in ROW_SEM:
        row_messages(name, "sent")


def solution(mesh):
    rows = mesh.shape["row"]
    cols = mesh.shape["col"]
    tile_spec = P("batch", "row", "col")

    def local_blocks(x, w1d, b1d, w1c, b1c, wp1, w2d, b2d, w2c, b2c, wp2, w3d, b3d, w3c, b3c, wp3):
        n, h, w, c0 = x.shape
        c1, c2, c3 = w1d.shape[3], w2d.shape[3], w3d.shape[3]
        h4, h8 = h // 4, h // 8
        dims = (n, h, c0, c1, c2, c3, rows, cols)
        pair = 2 * c0
        xt = jnp.moveaxis(x, 1, 3).reshape(n, PAIRS, pair, h)
        args = (xt, w1d.reshape(3, 3 * c0, c1), w1c.reshape(9 * c1, c1), wp1, w2d.reshape(9 * c1, c2), w2c.reshape(9 * c2, c2), wp2,
                jnp.swapaxes(w3d.reshape(9, c2, c3), 1, 2), w3c.reshape(9, c3, c3), wp3.T,
                b1d, b1c, b2d, b2c, b3d, b3c)
        vm = pltpu.VMEM
        dma = pltpu.SemaphoreType.DMA
        flops = 2 * n * h * w * c1 * 7 * (c0 + c1)
        out = pl.pallas_call(
            functools.partial(kernel, dims),
            out_shape=jax.ShapeDtypeStruct((h8, n, c3), BF16),
            in_specs=[pl.BlockSpec(memory_space=pl.ANY)] * len(args),
            out_specs=pl.BlockSpec(memory_space=pl.ANY),
            scratch_shapes=[
                vm(shape, BF16) for shape in (
                    (PAIRS, n, pair, h), (2, n, pair, h // 2), (n, h, 2 * pair), (h, h), (n * BLOCK, n * BLOCK),
                    (6, h4 + 1, 4, n, pair), (7, h4 + 2, 2, n, c1), (7, h4 + 1, 2, n, c1),
                    (5, h4 + 2, n, c2), (5, h8 + 1, 2, n, c2), (4, h8 + 2, n, c3), (2, h8, n, c3),
                    (10 * pair, 2 * c1), (12 * c1 + 2 * pair, 2 * c1), (9 * c1, c2), (9 * c2 + c1, c2),
                    (9, c3, c2), (9, c3, c3), (c3, c2))
            ] + [vm((1, width), F32) for width in (c1, c1, c2, c2, c3, c3)] + [
                dma((count,)) for count in (32, 4, 10 * NCH, 10 * NCH, 12 * MAX_PLAN, 12 * MAX_PLAN, 3 * NCH3)],
            compiler_params=pltpu.CompilerParams(collective_id=0, has_side_effects=True, vmem_limit_bytes=63 * 1024 * 1024),
            cost_estimate=pl.CostEstimate(flops=flops, bytes_accessed=16 * 1024 * 1024, transcendentals=0),
        )(*args)
        return jnp.swapaxes(out, 0, 1).reshape(n, h8, 1, c3)

    return jax.shard_map(local_blocks, mesh=mesh, in_specs=(tile_spec,) + (P(),) * 15, out_specs=tile_spec, check_vma=False)
```

```python
import functools

import jax
import jax.numpy as jnp
from jax import lax
from jax.experimental import pallas as pl
from jax.experimental.pallas import tpu as pltpu
from jax.sharding import PartitionSpec as P

BF16 = jnp.bfloat16
F32 = jnp.float32
SHIFTS = (0, 1)
NCH = 4
NCH3 = 2
PAIRS = 4
MAX_PLAN = 5
BLOCK = 16
UNROLL = 4
OWN, HALO = BOTH = range(2)
AROUND = (1, 2, 3)
NEAR = range(-2, 3)
UP, DOWN = (False,), (True,)
NT = (((1,), (1,)), ((), ()))


def relu(value):
    return jnp.maximum(value, 0.0)


def loop(count, body):
    lax.fori_loop(0, count, body, 0)


def row_plan(kind, width, s_send, s_recv):
    if kind == "x":
        own = (0, width - 1)
        need = (-1, width - 1) if s_recv == 0 else (0, width)
        src_at, dst_at = 2 - s_send, 2 - s_recv
    elif kind == "y":
        own = (s_send, width - 1 + s_send)
        need = (s_recv - 1, s_recv + width)
        src_at, dst_at = 2 - s_send, 2 - s_recv
    else:
        own = (s_send, width - 1 + s_send)
        need = (-1, width - 1) if s_recv == 0 else (0, width + 1)
        src_at, dst_at = 3 - 2 * s_send, 3 - 2 * s_recv
    plan = []
    for dist in NEAR:
        lo = max(own[0], width * dist + need[0])
        hi = min(own[1], width * dist + need[1])
        if lo <= hi:
            plan.append((dist, lo + src_at, lo - width * dist + dst_at, hi - lo + 1, False))
        if kind != "x" and s_send == 1 and s_recv == 0 and dist >= 0 and need[0] + width * dist <= 0 <= need[1] + width * dist:
            plan.append((dist, src_at, dst_at - width * dist, 1, True))
    return plan


def kernel(dims, x_hbm, w1d_h, w1c_h, wp1_h, w2d_h, w2c_h, wp2_h, w3d_h, w3c_h, wp3_h, b1d_h, b1c_h, b2d_h, b2c_h, b3d_h, b3c_h, out_hbm,
           raw, xh, turned, eye, mix, xs, y1, z1, y2, z2, y3, zo, w1d, w1c, w2d, w2c, w3r, w3d, w3c, w3e, wp3r,
           b1d, b1c, b2d, b2c, b3d, b3c, load_sem, x_sem, col_send, col_recv, row_send, row_recv, out_sem):
    n, h, c0, c1, c2, c3, rows, cols = dims
    h4, h8 = h // 4, h // 8
    ch, ch3 = h4 // NCH, h8 // NCH3
    hh = h // 2
    row = lax.axis_index("row")
    col = lax.axis_index("col")
    s = lax.rem(row, 2)
    is0 = s == 0
    first_extra = (s == 1) & (col == 0)
    last_void = (s == 1) & (col == cols - 1)
    t_first = jnp.where(first_extra, -1, 0)
    fwd_col = jnp.where(is0, col + 1, col - 1)
    bwd_col = jnp.where(is0, col - 1, col + 1)
    has_fwd = (fwd_col >= 0) & (fwd_col < cols)
    has_bwd = (bwd_col >= 0) & (bwd_col < cols)

    load_count = []

    def load(src, dst):
        load_count.append(dst)
        return pltpu.make_async_copy(src, dst, load_sem.at[len(load_count) - 1])

    k1, k2 = 9 * c1, 9 * c2
    pair = 2 * c0
    x_loads = [load(x_hbm.at[:, q], raw.at[q]) for q in range(PAIRS)]
    w1d_loads = [load(b1d_h, b1d.at[0]), load(b1c_h, b1c.at[0])]
    w1c_loads = []
    for p in BOTH:
        lanes = pl.ds(p * c1, c1)
        for kh in range(3):
            w1d_loads.append(load(w1d_h.at[kh], w1d.at[pl.ds((kh + 2 * p) * 2 * pair + c0, 3 * c0), lanes]))
        w1c_loads.append(load(w1c_h, w1c.at[pl.ds(p * 3 * c1, k1), lanes]))
        w1c_loads.append(load(wp1_h, w1c.at[pl.ds(12 * c1 + p * pair, c0), lanes]))
    w2d_loads = [load(w2d_h, w2d), load(b2d_h, b2d.at[0])]
    w2c_loads = [load(w2c_h, w2c.at[pl.ds(0, k2)]), load(wp2_h, w2c.at[pl.ds(k2, c1)]), load(b2c_h, b2c.at[0])]
    w3d_loads = [load(w3d_h, w3r), load(b3d_h, b3d.at[0]), load(wp3_h, wp3r)]
    w3c_loads = [load(w3c_h.at[:, pl.ds(0, c2)], w3c), load(w3c_h.at[:, pl.ds(c2, c3 - c2)], w3e), load(b3c_h, b3c.at[0])]
    for copy in x_loads:
        copy.start()

    def row_refs(name, slots, down, side):
        ref = refs[name]
        last = ref.shape[1] - (2 if ROW_SEM[name][0] == "y" else 1)
        own_at, halo_at = (last, 0) if down else (1, last + 1)
        at = own_at if side == OWN else halo_at
        subs = 1 if len(ref.shape) == 4 else ref.shape[2]
        if subs == 1:
            return ref.at[slots, at]
        return ref.at[slots, at, subs - 1 if down else 0]

    refs = dict(x=xs, y1=y1, z1=z1, y2=y2, z2=z2, y3=y3)
    ROW_SEM = {}
    for name, kind, width in (("x", "x", PAIRS), ("y1", "y", PAIRS), ("z1", "z", PAIRS), ("y2", "y", 2), ("z2", "z", 2), ("y3", "y", 1)):
        ROW_SEM[name] = (kind, width, 2 * MAX_PLAN * len(ROW_SEM))

    def directions(name):
        return (True, False) if ROW_SEM[name][0] == "y" else (True,)

    def dot(lhs, rhs):
        return jnp.dot(lhs, rhs, preferred_element_type=F32)

    def zero_slot(ref, idx):
        ref[idx] = jnp.zeros(ref.shape[1:], ref.dtype)

    def dot(lhs, rhs):
        return jnp.dot(lhs, rhs, preferred_element_type=F32)

    def zero_slot(ref, idx):
        def body(i, carry):
            ref[idx, i] = jnp.zeros(ref.shape[2:], ref.dtype)
            return carry
        loop(ref.shape[1], body)

    for name in ROW_SEM:
        for down in directions(name):
            edge = row_refs(name, slice(None), down, HALO)
            edge[...] = jnp.zeros(edge.shape, BF16)

    @pl.when(col == cols - 1)
    def _():
        for ref in (y1, y2, y3):
            zero_slot(ref, ref.shape[0] - 1)

    barrier = pltpu.get_barrier_semaphore()
    around = 0
    for step in range(-1, 2):
        for dist in NEAR:
            near_row, near_col = row + step, col + dist
            ok = (near_row >= 0) & (near_row < rows) & (near_col >= 0) & (near_col < cols)
            around = around + ok.astype(jnp.int32)

            @pl.when(ok)
            def _():
                pl.semaphore_signal(barrier, inc=1, device_id={"row": near_row, "col": near_col}, device_id_type=pl.DeviceIdType.MESH)

    @pl.when(col == 0)
    def _():
        for ref in (y1, y2, y3):
            zero_slot(ref, 1 - s)
        for ref in (z1, z2):
            zero_slot(ref, 2 - 2 * s)

    @pl.when(first_extra)
    def _():
        zero_slot(xs, 0)

    def zero_xh(first, size):
        def body(i, carry):
            for half in BOTH:
                xh[half, i, pl.ds(first, size)] = jnp.zeros((size, hh), BF16)
            return carry
        loop(n, body)

    @pl.when(is0)
    def _():
        zero_xh(0, c0)

    @pl.when(jnp.logical_not(has_bwd))
    def _():
        zero_xh(0, pair)

    def unit_where(size, source):
        at = lax.broadcasted_iota(jnp.int32, (size, size), 0)
        return (at == source(lax.broadcasted_iota(jnp.int32, (size, size), 1))).astype(F32).astype(BF16)

    eye[...] = unit_where(h, lambda at: at)
    mix[...] = unit_where(n * BLOCK, lambda at: (at & (BLOCK - 1)) * n + (at >> BLOCK.bit_length() - 1))

    def zero_part(ref, first, size, p):
        ref[pl.ds(first, size), pl.ds(p * c1, c1)] = jnp.zeros((size, c1), BF16)

    for p in BOTH:
        for kh in range(5):
            tap_at = kh * 2 * pair
            used = 2 * p <= kh < 2 * p + 3
            zero_part(w1d, tap_at, c0 if used else 2 * pair, p)
        zero_part(w1c, (1 - p) * k1, 3 * c1, p)
        proj_at = 12 * c1
        zero_part(w1c, proj_at + (1 - p) * pair, pair, p)
        zero_part(w1c, proj_at + p * pair + c0, c0, p)
    pl.semaphore_wait(barrier, around)

    def remote(src, dst, send_sem, recv_sem, to_row, to_col):
        return pltpu.make_async_remote_copy(src_ref=src, dst_ref=dst, send_sem=send_sem, recv_sem=recv_sem,
                                            device_id={"row": to_row, "col": to_col}, device_id_type=pl.DeviceIdType.MESH)

    def x_copy(shift, half):
        lanes = pl.ds(half * hh, hh)
        if shift == 0:
            src, dst = x_hbm.at[:, 3, pl.ds(c0, c0), lanes], xh.at[half, :, pl.ds(c0, c0)]
        else:
            src, dst = x_hbm.at[:, 0, :, lanes], xh.at[half]
        return remote(src, dst, x_sem.at[half], x_sem.at[2 + half], row, fwd_col)

    for shift in SHIFTS:
        @pl.when(has_fwd & (s == shift))
        def _():
            for half in BOTH:
                x_copy(shift, half).start()

    def y_copy(ref, width, rows_per, sem0, forward, chunk, nch):
        to_right = is0 if forward else jnp.logical_not(is0)
        src_slot = jnp.where(to_right, width + 1, 2)
        dst_slot = jnp.where(to_right, 1, width + 2)
        part = pl.ds(1 + chunk * rows_per, rows_per)
        sem = sem0 + (0 if forward else nch) + chunk
        return remote(ref.at[src_slot, part], ref.at[dst_slot, part], col_send.at[sem], col_recv.at[sem], row, fwd_col if forward else bwd_col)

    def y_recv(ref, width, rows_per, sem0, forward, chunk, nch):
        to_right = is0 if forward else jnp.logical_not(is0)
        dst_slot = jnp.where(to_right, 1, width + 2)
        part = pl.ds(1 + chunk * rows_per, rows_per)
        sem = sem0 + (0 if forward else nch) + chunk
        return remote(ref.at[dst_slot, part], ref.at[dst_slot, part], col_send.at[sem], col_recv.at[sem], row, bwd_col if forward else fwd_col)

    def z_copy(ref, width, rows_per, sem0, chunk):
        src_slot = jnp.where(is0, width + 2, 2)
        dst_slot = jnp.where(is0, 2, width + 2)
        part = pl.ds(1 + chunk * rows_per, rows_per)
        sem = sem0 + chunk
        return remote(ref.at[src_slot, part], ref.at[dst_slot, part], col_send.at[sem], col_recv.at[sem], row, fwd_col)

    def z_recv(ref, width, rows_per, sem0, chunk):
        dst_slot = jnp.where(is0, 2, width + 2)
        part = pl.ds(1 + chunk * rows_per, rows_per)
        sem = sem0 + chunk
        return remote(ref.at[dst_slot, part], ref.at[dst_slot, part], col_send.at[sem], col_recv.at[sem], row, bwd_col)

    SEM_Y1, SEM_Z1, SEM_Y2, SEM_Z2, SEM_Y3 = (i * 2 * NCH for i in range(5))

    def row_messages(name, act, ways=None):
        kind, width, sem0 = ROW_SEM[name]
        for down in ways or directions(name):
            for s_send, s_recv in zip(SHIFTS, reversed(SHIFTS)):
                step = 1 if down else -1
                for i, (dist, src, dst, count, extra) in enumerate(row_plan(kind, width, s_send, s_recv)):
                    sem = sem0 + i + (0 if down else MAX_PLAN)
                    if act == "recv":
                        from_row, from_col = row - step, col - dist
                        ok = (s == s_recv) & (from_row >= 0) & (from_row < rows) & (from_col >= 0) & (from_col < cols)
                        if extra:
                            ok = ok & (from_col == 0)

                        @pl.when(ok)
                        def _():
                            ref = row_refs(name, pl.ds(dst, count), down, HALO)
                            remote(ref, ref, row_send.at[sem], row_recv.at[sem], from_row, from_col).wait_recv()
                    else:
                        to_row, to_col = row + step, col + dist
                        ok = (s == s_send) & (to_row >= 0) & (to_row < rows) & (to_col >= 0) & (to_col < cols)
                        if extra:
                            ok = ok & (col == 0)

                        @pl.when(ok)
                        def _():
                            copy = remote(row_refs(name, pl.ds(src, count), down, OWN), row_refs(name, pl.ds(dst, count), down, HALO),
                                          row_send.at[sem], row_recv.at[sem], to_row, to_col)
                            if act == "send":
                                copy.start()
                            else:
                                copy.wait_send()

    def send_edges(name, chunk, nch):
        @pl.when(chunk == 0)
        def _():
            row_messages(name, "send", UP)

        @pl.when(chunk == nch - 1)
        def _():
            row_messages(name, "send", DOWN)

    def to_rows(value):
        return value.astype(BF16).reshape(BLOCK // 4, 4, n, pair)

    def turn_group(q):
        def turn(i, carry):
            for j in range(UNROLL):
                at = i * UNROLL + j
                block = raw[pl.ds(q, 2), at].reshape(2 * pair, h)
                turned[at] = lax.dot_general(eye[...], block, NT, preferred_element_type=F32).astype(BF16)
            return carry
        loop(n // UNROLL, turn)

        def place(i, carry):
            for j in range(UNROLL):
                at = i * UNROLL + j
                block = turned[:, pl.ds(at * BLOCK, BLOCK), :].reshape(n * BLOCK, 2 * pair)
                moved = dot(mix[...], block)
                for side in BOTH:
                    xs[q + 2 - s + side, pl.ds(1 + at * (BLOCK // 4), BLOCK // 4)] = to_rows(moved[:, side * pair:(side + 1) * pair])
            return carry
        loop(h // BLOCK // UNROLL, place)

    def turn_halo(half):
        slot = jnp.where(is0, 1, PAIRS + 1)
        unit = eye[:hh, :hh]

        def turn(i, carry):
            for j in range(UNROLL):
                at = 2 * (i * UNROLL + j)
                block = xh[half, pl.ds(at, 2)].reshape(2 * pair, hh)
                both = lax.dot_general(unit, block, NT, preferred_element_type=F32).astype(BF16)
                for side in BOTH:
                    turned[at + side, :hh, :pair] = both[:, side * pair:(side + 1) * pair]
            return carry
        loop(n // 2 // UNROLL, turn)

        def place(i, carry):
            blocks = [turned[:, pl.ds((2 * i + j) * BLOCK, BLOCK), :pair].reshape(n * BLOCK, pair) for j in BOTH]
            moved = dot(mix[...], jnp.concatenate(blocks, axis=1))
            for j in BOTH:
                first = 1 + half * (h4 // 2) + (2 * i + j) * (BLOCK // 4)
                xs[slot, pl.ds(first, BLOCK // 4)] = to_rows(moved[:, j * pair:(j + 1) * pair])
            return carry
        loop(hh // BLOCK // 2, place)

    for copy in w1d_loads + w1c_loads + w2d_loads + w2c_loads + w3d_loads + w3c_loads:
        copy.start()
    for copy in x_loads:
        copy.wait()

    def flat(value):
        return value.reshape(value.shape[0] * n, value.shape[-1])

    def parts(first, count):
        size = count // 2
        return tuple((first + i * size, size) for i in BOTH)

    def dot_nt(lhs, rhs):
        return lax.dot_general(lhs, rhs, NT, preferred_element_type=F32)

    def rows_down(at):
        return (at - 1, 1), (at, 0), (at, 1)

    def whole(c):
        return ((1 + c * ch3, ch3),)

    def own_col(t, width):
        return jnp.where(is0, width - 1 - t, t)

    def phase(width, nch, item):
        def body(at, carry):
            item(lax.div(at, nch) - 1, lax.rem(at, nch))
            return carry
        lax.fori_loop((t_first + 1) * nch, (width + 1) * nch, body, 0)

    def y1_job(t, c):
        k = own_col(t, PAIRS)
        at = 1 + c * ch
        taps = []
        for kh in range(5):
            first, sub = (at - 1, 3) if kh == 0 else (at, kh - 1)
            for side in (1, 2):
                taps.append(flat(xs[k + side, pl.ds(first, ch), sub]))
        acc = dot(jnp.concatenate(taps, axis=1), w1d[...])
        void = last_void & (t == 3)
        for p in BOTH:
            val = relu(acc[:, p * c1:(p + 1) * c1] + b1d[...])
            val = jnp.where(void, 0.0, val)
            y1[k + 2, pl.ds(at, ch), p] = val.astype(BF16).reshape(ch, n, c1)

    def own_group(group, carry):
        turn_group(2 * group)
        return carry
    loop(PAIRS // 2, own_group)
    row_messages("x", "send")
    for copy in w1d_loads:
        copy.wait()
    early = 3 - t_first

    def y1_item(item, carry):
        @pl.when(item == lax.div(3 * early, 2))
        def _():
            row_messages("x", "recv")

        half = item - 2 * early

        @pl.when(half >= 0)
        def _():
            for shift in SHIFTS:
                @pl.when(has_bwd & (s == shift))
                def _():
                    ref = xh.at[half, :, pl.ds(c0, c0)] if shift == 0 else xh.at[half]
                    remote(ref, ref, x_sem.at[half], x_sem.at[2 + half], row, bwd_col).wait_recv()
            turn_halo(half)

        jobs = []
        for j in BOTH:
            at = 2 * item + j
            t = jnp.where(at < 3 * early, lax.div(at, 3) + t_first, jnp.where(half >= 0, 3, at - 3 * early + t_first))
            c = jnp.where(at < 3 * early, lax.rem(at, 3) + 1, jnp.where(half >= 0, at - NCH * early, 0))
            jobs.append((t, c))
        for t, c in jobs:
            y1_job(t, c)
        send_edges("y1", half, 2)

        for t, c in jobs:
            @pl.when((t == 0) & has_fwd)
            def _():
                y_copy(y1, PAIRS, ch, SEM_Y1, True, c, NCH).start()

            @pl.when((t == 3) & has_bwd)
            def _():
                y_copy(y1, PAIRS, ch, SEM_Y1, False, c, NCH).start()
        return carry
    loop(2 * (PAIRS - t_first), y1_item)
    for copy in w1c_loads:
        copy.wait()

    def wait_halo(ref, width, rows_per, sem0, forward, half, nch):
        exists = has_bwd if forward else has_fwd

        split = nch - nch // 4
        for part in BOTH:
            @pl.when(exists & (half == part))
            def _():
                for c in range(split, nch) if part else range(split):
                    y_recv(ref, width, rows_per, sem0, forward, c, nch).wait_recv()

    def z1_job(t, c):
        k = own_col(t, PAIRS)
        at = 1 + c * ch
        taps = []
        for first, sub in ((at - 1, 1), (at, 0), (at, 1), (at + 1, 0)):
            for side in AROUND:
                taps.append(flat(y1[k + side, pl.ds(first, ch), sub]))
        for sub in (0, 2):
            taps.append(flat(xs[k + 2, pl.ds(at, ch), sub]))
        acc = dot(jnp.concatenate(taps, axis=1), w1c[...])
        for p in BOTH:
            val = relu(acc[:, p * c1:(p + 1) * c1] + b1c[...])
            z1[k + 3 - s, pl.ds(at, ch), p] = val.astype(BF16).reshape(ch, n, c1)

    extra = -t_first

    def turn_weight(i, carry):
        for j in range(3):
            tap = 3 * i + j
            w3d[tap] = dot_nt(eye[:c2, :c2], w3r[tap]).astype(BF16)
        return carry

    def z1_item(item, carry):
        inner = item - extra
        edge = inner - NCH - extra
        more = (inner < 0) | (extra == 1) & (inner == NCH)

        @pl.when(inner == 2)
        def _():
            row_messages("y1", "recv")

        half = lax.rem(edge, 2)
        far = edge >= 2

        @pl.when(edge == 0)
        def _():
            for copy in w3d_loads:
                copy.wait()
            loop(3, turn_weight)

        @pl.when((edge >= 0) & (edge < 2))
        def _():
            wait_halo(y1, PAIRS, ch, SEM_Y1, False, half, NCH)

        @pl.when(far)
        def _():
            wait_halo(y1, PAIRS, ch, SEM_Y1, True, half, NCH)

        mid = jnp.where(inner < 2, inner + 1, jnp.where(inner == 2, 0, inner))
        edge_col = jnp.where(far, 3, 0)
        for j in BOTH:
            t = jnp.where(more, -1, jnp.where(edge >= 0, edge_col, j + 1))
            c = jnp.where(more, jnp.where(inner < 0, j + 1, 3 * j), jnp.where(edge >= 0, 2 * half + j, mid))
            z1_job(t, c)

        @pl.when((edge >= 0) & (edge < 2) & has_fwd)
        def _():
            for j in BOTH:
                z_copy(z1, PAIRS, ch, SEM_Z1, 2 * half + j).start()
        return carry
    loop(2 * (NCH + extra), z1_item)
    row_messages("z1", "send")
    for copy in w2d_loads:
        copy.wait()

    def y2_job(t, at, size):
        k = own_col(t, 2)
        taps = []
        for first, sub in rows_down(at):
            for side in range(3):
                taps.append(flat(z1[2 * k + 2 + side, pl.ds(first, size), sub]))
        acc = dot(jnp.concatenate(taps, axis=1), w2d[...])
        val = relu(acc + b2d[...])
        val = jnp.where(last_void & (t == 1), 0.0, val)
        y2[k + 2, pl.ds(at, size)] = val.astype(BF16).reshape(size, n, c2)

    def y2_inner(item, carry):
        t = t_first + lax.div(item, 2)
        late = lax.rem(item, 2)

        @pl.when(item == 1)
        def _():
            row_messages("z1", "recv")

        chunks = (1 + 2 * late, 2 - 2 * late)
        for c in chunks:
            y2_job(t, 1 + c * ch, ch)

        @pl.when((t == 0) & has_fwd)
        def _():
            for c in chunks:
                y_copy(y2, 2, ch, SEM_Y2, True, c, NCH).start()
        return carry
    loop(2 + 2 * extra, y2_inner)

    def y2_edge(c, carry):
        @pl.when(has_bwd)
        def _():
            z_recv(z1, PAIRS, ch, SEM_Z1, c).wait_recv()

        for at, size in parts(1 + c * ch, ch):
            y2_job(jnp.int32(1), at, size)

        send_edges("y2", c, NCH)

        @pl.when(has_bwd)
        def _():
            y_copy(y2, 2, ch, SEM_Y2, False, c, NCH).start()
        return carry
    loop(NCH, y2_edge)
    for copy in w2c_loads:
        copy.wait()

    def z2_job(t, c):
        k = own_col(t, 2)
        at = 1 + c * ch
        taps = []
        for first in (at - 1, at, at + 1):
            for side in AROUND:
                taps.append(flat(y2[k + side, pl.ds(first, ch)]))
        taps.append(flat(z1[2 * k + 3, pl.ds(at, ch), 0]))
        acc = dot(jnp.concatenate(taps, axis=1), w2c[...])
        val = relu(acc + b2c[...]).astype(BF16).reshape(ch // 2, 2, n, c2)
        z2[k + 3 - s, pl.ds(1 + c * (ch // 2), ch // 2)] = val

    row_messages("y2", "recv")

    def z2_item(item, carry):
        edge = item - 2 * extra
        half = lax.rem(item, 2)
        near = (edge >= 0) & (edge < 2)

        @pl.when(near)
        def _():
            wait_halo(y2, 2, ch, SEM_Y2, False, half, NCH)

        @pl.when(edge >= 2)
        def _():
            wait_halo(y2, 2, ch, SEM_Y2, True, half, NCH)

        for j in BOTH:
            z2_job(lax.div(edge + 2, 2) - 1, 2 * half + j)

        @pl.when(near & has_fwd)
        def _():
            for j in BOTH:
                z_copy(z2, 2, ch // 2, SEM_Z2, 2 * half + j).start()
        return carry
    loop(NCH + 2 * extra, z2_item)
    row_messages("z2", "send")

    def y3_item(t, c):
        k = t

        @pl.when((t == t_first) & (c == 0))
        def _():
            row_messages("z2", "recv")

        @pl.when((t == 0) & has_bwd)
        def _():
            for j in range(NCH // NCH3):
                z_recv(z2, 2, ch // 2, SEM_Z2, c * (NCH // NCH3) + j).wait_recv()

        for at, size in whole(c):
            taps = [flat(z2[2 * k + 2 + side, pl.ds(first, size), sub]) for first, sub in rows_down(at) for side in range(3)]
            acc = dot(jnp.concatenate(taps, axis=1), w3d[...].reshape(k2, c3)) + b3d[...]
            val = jnp.where(last_void & (t == 0), 0.0, relu(acc))
            y3[k + 2, pl.ds(at, size)] = val.astype(BF16).reshape(size, n, c3)

        @pl.when(t == 0)
        def _():
            send_edges("y3", c, NCH3)

        @pl.when((t == 0) & has_fwd)
        def _():
            y_copy(y3, 1, ch3, SEM_Y3, True, c, NCH3).start()

        @pl.when((t == 0) & has_bwd)
        def _():
            y_copy(y3, 1, ch3, SEM_Y3, False, c, NCH3).start()
    phase(1, NCH3, y3_item)
    for copy in w3c_loads:
        copy.wait()

    ships = (s == 1) & has_bwd

    def ship(c):
        part = pl.ds(c * ch3, ch3)
        return remote(zo.at[1, part], out_hbm.at[part], out_sem.at[c], out_sem.at[NCH3 + c], row, bwd_col)

    def ship_recv(c):
        part = pl.ds(c * ch3, ch3)
        return remote(zo.at[1, part], out_hbm.at[part], out_sem.at[c], out_sem.at[NCH3 + c], row, fwd_col)

    keep = jnp.where(is0, 1, 0)

    def put(c):
        part = pl.ds(c * ch3, ch3)
        return pltpu.make_async_copy(zo.at[keep, part], out_hbm.at[part], out_sem.at[2 * NCH3 + c])

    def z3_item(t, c):
        k = t

        @pl.when((t == t_first) & (c == 0))
        def _():
            row_messages("y3", "recv")

        @pl.when((t == 0) & (c == 0))
        def _():
            for forward, exists in ((False, has_fwd), (True, has_bwd)):
                @pl.when(exists)
                def _():
                    for chunk in range(NCH3):
                        y_recv(y3, 1, ch3, SEM_Y3, forward, chunk, NCH3).wait_recv()

        for at, size in whole(c):
            acc = dot_nt(flat(z2[2 * k + 3, pl.ds(at, size), 0]), wp3r[...]) + b3c[...]
            taps = [flat(y3[k + side, pl.ds(first, size)]) for first in (at - 1, at, at + 1) for side in AROUND]
            acc = acc + dot(jnp.concatenate([tap[:, :c2] for tap in taps], axis=1), w3c[...].reshape(k2, c3))
            acc = acc + dot(jnp.concatenate([tap[:, c2:] for tap in taps], axis=1), w3e[...].reshape(9 * (c3 - c2), c3))
            zo[k + 1, pl.ds(at - 1, size)] = relu(acc).astype(BF16).reshape(size, n, c3)

        @pl.when((t == 0) & ships)
        def _():
            ship(c).start()

        @pl.when(((t == 0) & is0) | (t == -1))
        def _():
            put(c).start()
    phase(1, NCH3, z3_item)

    for shift in SHIFTS:
        @pl.when(has_fwd & (s == shift))
        def _():
            for half in BOTH:
                x_copy(shift, half).wait_send()

    def drain(c, carry):
        @pl.when(has_fwd)
        def _():
            y_copy(y1, PAIRS, ch, SEM_Y1, True, c, NCH).wait_send()
            z_copy(z1, PAIRS, ch, SEM_Z1, c).wait_send()
            y_copy(y2, 2, ch, SEM_Y2, True, c, NCH).wait_send()
            z_copy(z2, 2, ch // 2, SEM_Z2, c).wait_send()

        @pl.when(has_bwd)
        def _():
            y_copy(y1, PAIRS, ch, SEM_Y1, False, c, NCH).wait_send()
            y_copy(y2, 2, ch, SEM_Y2, False, c, NCH).wait_send()
        return carry
    loop(NCH, drain)

    def drain3(c, carry):
        @pl.when(has_fwd)
        def _():
            y_copy(y3, 1, ch3, SEM_Y3, True, c, NCH3).wait_send()

        @pl.when(has_bwd)
        def _():
            y_copy(y3, 1, ch3, SEM_Y3, False, c, NCH3).wait_send()

        @pl.when(ships)
        def _():
            ship(c).wait_send()

        @pl.when((s == 1) & has_fwd)
        def _():
            ship_recv(c).wait_recv()

        @pl.when(is0 | first_extra)
        def _():
            put(c).wait()
        return carry
    loop(NCH3, drain3)
    for name in ROW_SEM:
        row_messages(name, "sent")


def solution(mesh):
    rows = mesh.shape["row"]
    cols = mesh.shape["col"]
    tile_spec = P("batch", "row", "col")

    def local_blocks(x, w1d, b1d, w1c, b1c, wp1, w2d, b2d, w2c, b2c, wp2, w3d, b3d, w3c, b3c, wp3):
        n, h, w, c0 = x.shape
        c1, c2, c3 = w1d.shape[3], w2d.shape[3], w3d.shape[3]
        h4, h8 = h // 4, h // 8
        dims = (n, h, c0, c1, c2, c3, rows, cols)
        pair = 2 * c0
        xt = jnp.moveaxis(x, 1, 3).reshape(n, PAIRS, pair, h)
        args = (xt, w1d.reshape(3, 3 * c0, c1), w1c.reshape(9 * c1, c1), wp1, w2d.reshape(9 * c1, c2), w2c.reshape(9 * c2, c2), wp2,
                jnp.swapaxes(w3d.reshape(9, c2, c3), 1, 2), w3c.reshape(9, c3, c3), wp3.T,
                b1d, b1c, b2d, b2c, b3d, b3c)
        vm = pltpu.VMEM
        dma = pltpu.SemaphoreType.DMA
        flops = 14 * x.size * (c0 + c1)
        out = pl.pallas_call(
            functools.partial(kernel, dims),
            out_shape=jax.ShapeDtypeStruct((h8, n, c3), BF16),
            in_specs=[pl.BlockSpec(memory_space=pl.ANY)] * len(args),
            out_specs=pl.BlockSpec(memory_space=pl.ANY),
            scratch_shapes=[
                vm(shape, BF16) for shape in (
                    (PAIRS, n, pair, h), (2, n, pair, h // 2), (n, h, 2 * pair), (h, h), (n * BLOCK, n * BLOCK),
                    (6, h4 + 1, 4, n, pair), (7, h4 + 2, 2, n, c1), (7, h4 + 1, 2, n, c1),
                    (5, h4 + 2, n, c2), (5, h8 + 1, 2, n, c2), (4, h8 + 2, n, c3), (2, h8, n, c3),
                    (10 * pair, 2 * c1), (12 * c1 + 2 * pair, 2 * c1), (9 * c1, c2), (9 * c2 + c1, c2),
                    (9, c3, c2), (9, c2, c3), (9, c2, c3), (9, c3 - c2, c3), (c3, c2))
            ] + [vm((1, width), F32) for width in (c1, c1, c2, c2, c3, c3)] + [
                dma((count,)) for count in (32, 4, 10 * NCH, 10 * NCH, 12 * MAX_PLAN, 12 * MAX_PLAN, 3 * NCH3)],
            compiler_params=pltpu.CompilerParams(collective_id=0, has_side_effects=True, vmem_limit_bytes=63 << 20),
            cost_estimate=pl.CostEstimate(flops=flops, bytes_accessed=x.size * 4, transcendentals=0),
        )(*args)
        return jnp.swapaxes(out, 0, 1).reshape(n, h8, 1, c3)

    return jax.shard_map(local_blocks, mesh=mesh, in_specs=(tile_spec,) + (P(),) * 15, out_specs=tile_spec, check_vma=False)
```

```python
import functools

import jax
import jax.numpy as jnp
from jax import lax
from jax.experimental import pallas as pl
from jax.experimental.pallas import tpu as pltpu
from jax.sharding import PartitionSpec as P

BF16 = jnp.bfloat16
F32 = jnp.float32
SHIFTS = (0, 1)
NCH = 4
NCH3 = 2
PAIRS = 4
MAX_PLAN = 5
BLOCK = 16
UNROLL = 8
OWN, HALO = BOTH = range(2)
AROUND = (1, 2, 3)
NEAR = range(-2, 3)
UP, DOWN = (False,), (True,)
NT = (((1,), (1,)), ((), ()))


def relu(value):
    return jnp.maximum(value, 0.0)


def loop(count, body):
    lax.fori_loop(0, count, body, 0)


def row_plan(kind, width, s_send, s_recv):
    if kind == "x":
        own = (0, width - 1)
        need = (-1, width - 1) if s_recv == 0 else (0, width)
        src_at, dst_at = 2 - s_send, 2 - s_recv
    elif kind == "y":
        own = (s_send, width - 1 + s_send)
        need = (s_recv - 1, s_recv + width)
        src_at, dst_at = 2 - s_send, 2 - s_recv
    else:
        own = (s_send, width - 1 + s_send)
        need = (-1, width - 1) if s_recv == 0 else (0, width + 1)
        src_at, dst_at = 3 - 2 * s_send, 3 - 2 * s_recv
    plan = []
    for dist in NEAR:
        lo = max(own[0], width * dist + need[0])
        hi = min(own[1], width * dist + need[1])
        if lo <= hi:
            plan.append((dist, lo + src_at, lo - width * dist + dst_at, hi - lo + 1, False))
        if kind != "x" and s_send == 1 and s_recv == 0 and dist >= 0 and need[0] + width * dist <= 0 <= need[1] + width * dist:
            plan.append((dist, src_at, dst_at - width * dist, 1, True))
    return plan


def kernel(dims, x_hbm, w1d_h, w1c_h, wp1_h, w2d_h, w2c_h, wp2_h, w3d_h, w3c_h, wp3_h, b1d_h, b1c_h, b2d_h, b2c_h, b3d_h, b3c_h, out_hbm,
           raw, xh, turned, eye, mix, xs, y1, z1, y2, z2, y3, zo, w1d, w1c, w2d, w2c, w3r, w3d, w3c, w3e, wp3r,
           b1d, b1c, b2d, b2c, b3d, b3c, load_sem, x_sem, col_send, col_recv, row_send, row_recv, out_sem):
    n, h, c0, c1, c2, c3, rows, cols = dims
    h4, h8 = h // 4, h // 8
    ch, ch3 = h4 // NCH, h8 // NCH3
    hh = h // 2
    row = lax.axis_index("row")
    col = lax.axis_index("col")
    s = lax.rem(row, 2)
    is0 = s == 0
    first_extra = (s == 1) & (col == 0)
    last_void = (s == 1) & (col == cols - 1)
    t_first = jnp.where(first_extra, -1, 0)
    fwd_col = jnp.where(is0, col + 1, col - 1)
    bwd_col = jnp.where(is0, col - 1, col + 1)
    has_fwd = (fwd_col >= 0) & (fwd_col < cols)
    has_bwd = (bwd_col >= 0) & (bwd_col < cols)

    load_count = []

    def load(src, dst):
        load_count.append(dst)
        return pltpu.make_async_copy(src, dst, load_sem.at[len(load_count) - 1])

    k1, k2 = 9 * c1, 9 * c2
    pair = 2 * c0
    x_loads = [load(x_hbm.at[:, q], raw.at[q]) for q in range(PAIRS)]
    w1d_loads = [load(b1d_h, b1d.at[0]), load(b1c_h, b1c.at[0])]
    w1c_loads = []
    for p in BOTH:
        lanes = pl.ds(p * c1, c1)
        for kh in range(3):
            w1d_loads.append(load(w1d_h.at[kh], w1d.at[pl.ds((kh + 2 * p) * 2 * pair + c0, 3 * c0), lanes]))
        w1c_loads.append(load(w1c_h, w1c.at[pl.ds(p * 3 * c1, k1), lanes]))
        w1c_loads.append(load(wp1_h, w1c.at[pl.ds(12 * c1 + p * pair, c0), lanes]))
    w2d_loads = [load(w2d_h, w2d), load(b2d_h, b2d.at[0])]
    w2c_loads = [load(w2c_h, w2c.at[pl.ds(0, k2)]), load(wp2_h, w2c.at[pl.ds(k2, c1)]), load(b2c_h, b2c.at[0])]
    w3d_loads = [load(w3d_h, w3r), load(b3d_h, b3d.at[0]), load(wp3_h, wp3r)]
    w3c_loads = [load(w3c_h.at[:, pl.ds(0, c2)], w3c), load(w3c_h.at[:, pl.ds(c2, c3 - c2)], w3e), load(b3c_h, b3c.at[0])]
    for copy in x_loads:
        copy.start()

    def row_refs(name, slots, down, side):
        ref = refs[name]
        last = ref.shape[1] - (2 if ROW_SEM[name][0] == "y" else 1)
        own_at, halo_at = (last, 0) if down else (1, last + 1)
        at = own_at if side == OWN else halo_at
        subs = 1 if len(ref.shape) == 4 else ref.shape[2]
        if subs == 1:
            return ref.at[slots, at]
        return ref.at[slots, at, subs - 1 if down else 0]

    refs = dict(x=xs, y1=y1, z1=z1, y2=y2, z2=z2, y3=y3)
    ROW_SEM = {}
    for name, kind, width in (("x", "x", PAIRS), ("y1", "y", PAIRS), ("z1", "z", PAIRS), ("y2", "y", 2), ("z2", "z", 2), ("y3", "y", 1)):
        ROW_SEM[name] = (kind, width, 2 * MAX_PLAN * len(ROW_SEM))

    def directions(name):
        return (True, False) if ROW_SEM[name][0] == "y" else (True,)

    def dot(lhs, rhs):
        return jnp.dot(lhs, rhs, preferred_element_type=F32)

    def zero_slot(ref, idx):
        ref[idx] = jnp.zeros(ref.shape[1:], ref.dtype)

    def dot(lhs, rhs):
        return jnp.dot(lhs, rhs, preferred_element_type=F32)

    def zero_slot(ref, idx):
        def body(i, carry):
            ref[idx, i] = jnp.zeros(ref.shape[2:], ref.dtype)
            return carry
        loop(ref.shape[1], body)

    for name in ROW_SEM:
        for down in directions(name):
            edge = row_refs(name, slice(None), down, HALO)
            edge[...] = jnp.zeros(edge.shape, BF16)

    @pl.when(col == cols - 1)
    def _():
        for ref in (y1, y2, y3):
            zero_slot(ref, ref.shape[0] - 1)

    barrier = pltpu.get_barrier_semaphore()
    around = 0
    for step in range(-1, 2):
        for dist in NEAR:
            near_row, near_col = row + step, col + dist
            ok = (near_row >= 0) & (near_row < rows) & (near_col >= 0) & (near_col < cols)
            around = around + ok.astype(jnp.int32)

            @pl.when(ok)
            def _():
                pl.semaphore_signal(barrier, inc=1, device_id={"row": near_row, "col": near_col}, device_id_type=pl.DeviceIdType.MESH)

    @pl.when(col == 0)
    def _():
        for ref in (y1, y2, y3):
            zero_slot(ref, 1 - s)
        for ref in (z1, z2):
            zero_slot(ref, 2 - 2 * s)

    @pl.when(first_extra)
    def _():
        zero_slot(xs, 0)

    def zero_xh(first, size):
        def body(i, carry):
            for half in BOTH:
                xh[half, i, pl.ds(first, size)] = jnp.zeros((size, hh), BF16)
            return carry
        loop(n, body)

    @pl.when(is0)
    def _():
        zero_xh(0, c0)

    @pl.when(jnp.logical_not(has_bwd))
    def _():
        zero_xh(0, pair)

    def unit_where(size, source):
        at = lax.broadcasted_iota(jnp.int32, (size, size), 0)
        return (at == source(lax.broadcasted_iota(jnp.int32, (size, size), 1))).astype(F32).astype(BF16)

    eye[...] = unit_where(h, lambda at: at)
    mix[...] = unit_where(n * BLOCK, lambda at: (at & (BLOCK - 1)) * n + (at >> BLOCK.bit_length() - 1))

    def zero_part(ref, first, size, p):
        ref[pl.ds(first, size), pl.ds(p * c1, c1)] = jnp.zeros((size, c1), BF16)

    for p in BOTH:
        for kh in range(5):
            tap_at = kh * 2 * pair
            used = 2 * p <= kh < 2 * p + 3
            zero_part(w1d, tap_at, c0 if used else 2 * pair, p)
        zero_part(w1c, (1 - p) * k1, 3 * c1, p)
        proj_at = 12 * c1
        zero_part(w1c, proj_at + (1 - p) * pair, pair, p)
        zero_part(w1c, proj_at + p * pair + c0, c0, p)
    for copy in x_loads:
        copy.wait()
    pl.semaphore_wait(barrier, around)

    def remote(src, dst, send_sem, recv_sem, to_row, to_col):
        return pltpu.make_async_remote_copy(src_ref=src, dst_ref=dst, send_sem=send_sem, recv_sem=recv_sem,
                                            device_id={"row": to_row, "col": to_col}, device_id_type=pl.DeviceIdType.MESH)

    def x_copy(shift, half):
        lanes = pl.ds(half * hh, hh)
        if shift == 0:
            src, dst = raw.at[PAIRS - 1, :, pl.ds(c0, c0), lanes], xh.at[half, :, pl.ds(c0, c0)]
        else:
            src, dst = raw.at[0, :, :, lanes], xh.at[half]
        return remote(src, dst, x_sem.at[half], x_sem.at[2 + half], row, fwd_col)

    for shift in SHIFTS:
        @pl.when(has_fwd & (s == shift))
        def _():
            for half in BOTH:
                x_copy(shift, half).start()

    def y_copy(ref, width, rows_per, sem0, forward, chunk, nch):
        to_right = is0 if forward else jnp.logical_not(is0)
        src_slot = jnp.where(to_right, width + 1, 2)
        dst_slot = jnp.where(to_right, 1, width + 2)
        part = pl.ds(1 + chunk * rows_per, rows_per)
        sem = sem0 + (0 if forward else nch) + chunk
        return remote(ref.at[src_slot, part], ref.at[dst_slot, part], col_send.at[sem], col_recv.at[sem], row, fwd_col if forward else bwd_col)

    def y_recv(ref, width, rows_per, sem0, forward, chunk, nch):
        to_right = is0 if forward else jnp.logical_not(is0)
        dst_slot = jnp.where(to_right, 1, width + 2)
        part = pl.ds(1 + chunk * rows_per, rows_per)
        sem = sem0 + (0 if forward else nch) + chunk
        return remote(ref.at[dst_slot, part], ref.at[dst_slot, part], col_send.at[sem], col_recv.at[sem], row, bwd_col if forward else fwd_col)

    def z_copy(ref, width, rows_per, sem0, chunk):
        src_slot = jnp.where(is0, width + 2, 2)
        dst_slot = jnp.where(is0, 2, width + 2)
        part = pl.ds(1 + chunk * rows_per, rows_per)
        sem = sem0 + chunk
        return remote(ref.at[src_slot, part], ref.at[dst_slot, part], col_send.at[sem], col_recv.at[sem], row, fwd_col)

    def z_recv(ref, width, rows_per, sem0, chunk):
        dst_slot = jnp.where(is0, 2, width + 2)
        part = pl.ds(1 + chunk * rows_per, rows_per)
        sem = sem0 + chunk
        return remote(ref.at[dst_slot, part], ref.at[dst_slot, part], col_send.at[sem], col_recv.at[sem], row, bwd_col)

    SEM_Y1, SEM_Z1, SEM_Y2, SEM_Z2, SEM_Y3 = (i * 2 * NCH for i in range(5))

    def row_messages(name, act, ways=None):
        kind, width, sem0 = ROW_SEM[name]
        for down in ways or directions(name):
            for s_send, s_recv in zip(SHIFTS, reversed(SHIFTS)):
                step = 1 if down else -1
                for i, (dist, src, dst, count, extra) in enumerate(row_plan(kind, width, s_send, s_recv)):
                    sem = sem0 + i + (0 if down else MAX_PLAN)
                    if act == "recv":
                        from_row, from_col = row - step, col - dist
                        ok = (s == s_recv) & (from_row >= 0) & (from_row < rows) & (from_col >= 0) & (from_col < cols)
                        if extra:
                            ok = ok & (from_col == 0)

                        @pl.when(ok)
                        def _():
                            ref = row_refs(name, pl.ds(dst, count), down, HALO)
                            remote(ref, ref, row_send.at[sem], row_recv.at[sem], from_row, from_col).wait_recv()
                    else:
                        to_row, to_col = row + step, col + dist
                        ok = (s == s_send) & (to_row >= 0) & (to_row < rows) & (to_col >= 0) & (to_col < cols)
                        if extra:
                            ok = ok & (col == 0)

                        @pl.when(ok)
                        def _():
                            copy = remote(row_refs(name, pl.ds(src, count), down, OWN), row_refs(name, pl.ds(dst, count), down, HALO),
                                          row_send.at[sem], row_recv.at[sem], to_row, to_col)
                            if act == "send":
                                copy.start()
                            else:
                                copy.wait_send()

    def send_edges(name, chunk, nch):
        @pl.when(chunk == 0)
        def _():
            row_messages(name, "send", UP)

        @pl.when(chunk == nch - 1)
        def _():
            row_messages(name, "send", DOWN)

    def to_rows(value):
        return value.astype(BF16).reshape(BLOCK // 4, 4, n, pair)

    def turn_group(q):
        def turn(i, carry):
            for j in range(UNROLL):
                at = i * UNROLL + j
                block = raw[pl.ds(q, 2), at].reshape(2 * pair, h)
                turned[at] = lax.dot_general(eye[...], block, NT, preferred_element_type=F32).astype(BF16)
            return carry
        loop(n // UNROLL, turn)

        def place(i, carry):
            for j in range(UNROLL):
                at = i * UNROLL + j
                block = turned[:, pl.ds(at * BLOCK, BLOCK), :].reshape(n * BLOCK, 2 * pair)
                moved = dot(mix[...], block)
                for side in BOTH:
                    xs[q + 2 - s + side, pl.ds(1 + at * (BLOCK // 4), BLOCK // 4)] = to_rows(moved[:, side * pair:(side + 1) * pair])
            return carry
        loop(h // BLOCK // UNROLL, place)

    def turn_halo(half):
        slot = jnp.where(is0, 1, PAIRS + 1)
        unit = eye[:hh, :hh]
        many = min(UNROLL, n // 2)

        def turn(i, carry):
            for j in range(many):
                at = 2 * (i * many + j)
                block = xh[half, pl.ds(at, 2)].reshape(2 * pair, hh)
                both = lax.dot_general(unit, block, NT, preferred_element_type=F32).astype(BF16)
                for side in BOTH:
                    turned[at + side, :hh, :pair] = both[:, side * pair:(side + 1) * pair]
            return carry
        loop(n // 2 // many, turn)

        def place(i):
            blocks = [turned[:, pl.ds((2 * i + j) * BLOCK, BLOCK), :pair].reshape(n * BLOCK, pair) for j in BOTH]
            moved = dot(mix[...], jnp.concatenate(blocks, axis=1))
            for j in BOTH:
                first = 1 + half * (h4 // 2) + (2 * i + j) * (BLOCK // 4)
                xs[slot, pl.ds(first, BLOCK // 4)] = to_rows(moved[:, j * pair:(j + 1) * pair])
        for i in range(hh // BLOCK // 2):
            place(i)

    for copy in w1d_loads + w1c_loads + w2d_loads + w2c_loads + w3d_loads + w3c_loads:
        copy.start()

    def flat(value):
        return value.reshape(value.shape[0] * n, value.shape[-1])

    def parts(first, count):
        size = count // 2
        return tuple((first + i * size, size) for i in BOTH)

    def dot_nt(lhs, rhs):
        return lax.dot_general(lhs, rhs, NT, preferred_element_type=F32)

    def rows_down(at):
        return (at - 1, 1), (at, 0), (at, 1)

    def whole(c):
        return ((1 + c * ch3, ch3),)

    def own_col(t, width):
        return jnp.where(is0, width - 1 - t, t)

    def phase(width, nch, item):
        def body(at, carry):
            item(lax.div(at, nch) - 1, lax.rem(at, nch))
            return carry
        lax.fori_loop((t_first + 1) * nch, (width + 1) * nch, body, 0)

    def y1_job(t, c):
        k = own_col(t, PAIRS)
        at = 1 + c * ch
        taps = []
        for kh in range(5):
            first, sub = (at - 1, 3) if kh == 0 else (at, kh - 1)
            for side in (1, 2):
                taps.append(flat(xs[k + side, pl.ds(first, ch), sub]))
        acc = dot(jnp.concatenate(taps, axis=1), w1d[...])
        void = last_void & (t == 3)
        for p in BOTH:
            val = relu(acc[:, p * c1:(p + 1) * c1] + b1d[...])
            val = jnp.where(void, 0.0, val)
            y1[k + 2, pl.ds(at, ch), p] = val.astype(BF16).reshape(ch, n, c1)

    def own_group(group, carry):
        turn_group(2 * group)
        return carry
    loop(PAIRS // 2, own_group)
    row_messages("x", "send")
    for copy in w1d_loads:
        copy.wait()
    def turn_weight(i, carry):
        for j in range(3):
            tap = 3 * i + j
            w3d[tap] = dot_nt(eye[:c2, :c2], w3r[tap]).astype(BF16)
        return carry

    def turn_weights():
        for copy in w3d_loads:
            copy.wait()
        loop(3, turn_weight)

    early = 3 - t_first

    def y1_item(item, carry):
        @pl.when(item == lax.div(3 * early, 2))
        def _():
            row_messages("x", "recv")

        half = item - 2 * early

        @pl.when((half == 1) & jnp.logical_not(is0))
        def _():
            turn_weights()

        @pl.when(half >= 0)
        def _():
            for shift in SHIFTS:
                @pl.when(has_bwd & (s == shift))
                def _():
                    ref = xh.at[half, :, pl.ds(c0, c0)] if shift == 0 else xh.at[half]
                    remote(ref, ref, x_sem.at[half], x_sem.at[2 + half], row, bwd_col).wait_recv()
            turn_halo(half)

        jobs = []
        for j in BOTH:
            at = 2 * item + j
            t = jnp.where(at < 3 * early, lax.div(at, 3) + t_first, jnp.where(half >= 0, 3, at - 3 * early + t_first))
            c = jnp.where(at < 3 * early, lax.rem(at, 3) + 1, jnp.where(half >= 0, at - NCH * early, 0))
            jobs.append((t, c))
        for t, c in jobs:
            y1_job(t, c)
        send_edges("y1", half, 2)

        for t, c in jobs:
            @pl.when((t == 0) & has_fwd)
            def _():
                y_copy(y1, PAIRS, ch, SEM_Y1, True, c, NCH).start()

            @pl.when((t == 3) & has_bwd)
            def _():
                y_copy(y1, PAIRS, ch, SEM_Y1, False, c, NCH).start()
        return carry
    loop(2 * (PAIRS - t_first), y1_item)
    for copy in w1c_loads:
        copy.wait()

    def wait_halo(ref, width, rows_per, sem0, forward, half, nch):
        exists = has_bwd if forward else has_fwd

        split = nch - nch // 4
        for part in BOTH:
            @pl.when(exists & (half == part))
            def _():
                for c in range(split, nch) if part else range(split):
                    y_recv(ref, width, rows_per, sem0, forward, c, nch).wait_recv()

    def z1_job(t, c):
        k = own_col(t, PAIRS)
        at = 1 + c * ch
        taps = []
        for first, sub in ((at - 1, 1), (at, 0), (at, 1), (at + 1, 0)):
            for side in AROUND:
                taps.append(flat(y1[k + side, pl.ds(first, ch), sub]))
        for sub in (0, 2):
            taps.append(flat(xs[k + 2, pl.ds(at, ch), sub]))
        acc = dot(jnp.concatenate(taps, axis=1), w1c[...])
        for p in BOTH:
            val = relu(acc[:, p * c1:(p + 1) * c1] + b1c[...])
            z1[k + 3 - s, pl.ds(at, ch), p] = val.astype(BF16).reshape(ch, n, c1)

    extra = -t_first

    def z1_item(item, carry):
        inner = item - extra
        edge = inner - NCH - extra
        more = (inner < 0) | (extra == 1) & (inner == NCH)

        @pl.when(inner == 2)
        def _():
            row_messages("y1", "recv")

        half = lax.rem(edge, 2)
        far = edge >= 2

        @pl.when((edge == 0) & is0)
        def _():
            turn_weights()

        @pl.when((edge >= 0) & (edge < 2))
        def _():
            wait_halo(y1, PAIRS, ch, SEM_Y1, False, half, NCH)

        @pl.when(far)
        def _():
            wait_halo(y1, PAIRS, ch, SEM_Y1, True, half, NCH)

        mid = jnp.where(inner < 2, inner + 1, jnp.where(inner == 2, 0, inner))
        edge_col = jnp.where(far, 3, 0)
        for j in BOTH:
            t = jnp.where(more, -1, jnp.where(edge >= 0, edge_col, j + 1))
            c = jnp.where(more, jnp.where(inner < 0, j + 1, 3 * j), jnp.where(edge >= 0, 2 * half + j, mid))
            z1_job(t, c)

        @pl.when((edge >= 0) & (edge < 2) & has_fwd)
        def _():
            for j in BOTH:
                z_copy(z1, PAIRS, ch, SEM_Z1, 2 * half + j).start()
        return carry
    loop(2 * (NCH + extra), z1_item)
    row_messages("z1", "send")
    for copy in w2d_loads:
        copy.wait()

    def y2_job(t, at, size):
        k = own_col(t, 2)
        taps = []
        for first, sub in rows_down(at):
            for side in range(3):
                taps.append(flat(z1[2 * k + 2 + side, pl.ds(first, size), sub]))
        acc = dot(jnp.concatenate(taps, axis=1), w2d[...])
        val = relu(acc + b2d[...])
        val = jnp.where(last_void & (t == 1), 0.0, val)
        y2[k + 2, pl.ds(at, size)] = val.astype(BF16).reshape(size, n, c2)

    def y2_inner(item, carry):
        t = t_first + lax.div(item, 2)
        late = lax.rem(item, 2)

        @pl.when(item == 1)
        def _():
            row_messages("z1", "recv")

        chunks = (1 + 2 * late, 2 - 2 * late)
        for c in chunks:
            y2_job(t, 1 + c * ch, ch)

        @pl.when((t == 0) & has_fwd)
        def _():
            for c in chunks:
                y_copy(y2, 2, ch, SEM_Y2, True, c, NCH).start()
        return carry
    loop(2 + 2 * extra, y2_inner)

    def y2_edge(c, carry):
        @pl.when(has_bwd)
        def _():
            z_recv(z1, PAIRS, ch, SEM_Z1, c).wait_recv()

        for at, size in parts(1 + c * ch, ch):
            y2_job(jnp.int32(1), at, size)

        send_edges("y2", c, NCH)

        @pl.when(has_bwd)
        def _():
            y_copy(y2, 2, ch, SEM_Y2, False, c, NCH).start()
        return carry
    loop(NCH, y2_edge)
    for copy in w2c_loads:
        copy.wait()

    def z2_job(t, c):
        k = own_col(t, 2)
        at = 1 + c * ch
        taps = []
        for first in (at - 1, at, at + 1):
            for side in AROUND:
                taps.append(flat(y2[k + side, pl.ds(first, ch)]))
        taps.append(flat(z1[2 * k + 3, pl.ds(at, ch), 0]))
        acc = dot(jnp.concatenate(taps, axis=1), w2c[...])
        val = relu(acc + b2c[...]).astype(BF16).reshape(ch // 2, 2, n, c2)
        z2[k + 3 - s, pl.ds(1 + c * (ch // 2), ch // 2)] = val

    row_messages("y2", "recv")

    def z2_item(item, carry):
        edge = item - 2 * extra
        half = lax.rem(item, 2)
        near = (edge >= 0) & (edge < 2)

        @pl.when(near)
        def _():
            wait_halo(y2, 2, ch, SEM_Y2, False, half, NCH)

        @pl.when(edge >= 2)
        def _():
            wait_halo(y2, 2, ch, SEM_Y2, True, half, NCH)

        for j in BOTH:
            z2_job(lax.div(edge + 2, 2) - 1, 2 * half + j)

        @pl.when(near & has_fwd)
        def _():
            for j in BOTH:
                z_copy(z2, 2, ch // 2, SEM_Z2, 2 * half + j).start()
        return carry
    loop(NCH + 2 * extra, z2_item)
    row_messages("z2", "send")

    def y3_item(t, c):
        k = t

        @pl.when((t == t_first) & (c == 0))
        def _():
            row_messages("z2", "recv")

        @pl.when((t == 0) & has_bwd)
        def _():
            for j in range(NCH // NCH3):
                z_recv(z2, 2, ch // 2, SEM_Z2, c * (NCH // NCH3) + j).wait_recv()

        for at, size in whole(c):
            taps = [flat(z2[2 * k + 2 + side, pl.ds(first, size), sub]) for first, sub in rows_down(at) for side in range(3)]
            acc = dot(jnp.concatenate(taps, axis=1), w3d[...].reshape(k2, c3)) + b3d[...]
            val = jnp.where(last_void & (t == 0), 0.0, relu(acc))
            y3[k + 2, pl.ds(at, size)] = val.astype(BF16).reshape(size, n, c3)

        @pl.when(t == 0)
        def _():
            send_edges("y3", c, NCH3)

        @pl.when((t == 0) & has_fwd)
        def _():
            y_copy(y3, 1, ch3, SEM_Y3, True, c, NCH3).start()

        @pl.when((t == 0) & has_bwd)
        def _():
            y_copy(y3, 1, ch3, SEM_Y3, False, c, NCH3).start()
    phase(1, NCH3, y3_item)
    for copy in w3c_loads:
        copy.wait()

    ships = (s == 1) & has_bwd

    def ship(c):
        part = pl.ds(c * ch3, ch3)
        return remote(zo.at[1, part], out_hbm.at[part], out_sem.at[c], out_sem.at[NCH3 + c], row, bwd_col)

    def ship_recv(c):
        part = pl.ds(c * ch3, ch3)
        return remote(zo.at[1, part], out_hbm.at[part], out_sem.at[c], out_sem.at[NCH3 + c], row, fwd_col)

    keep = jnp.where(is0, 1, 0)

    def put(c):
        part = pl.ds(c * ch3, ch3)
        return pltpu.make_async_copy(zo.at[keep, part], out_hbm.at[part], out_sem.at[2 * NCH3 + c])

    def z3_item(t, c):
        k = t

        @pl.when((t == t_first) & (c == 0))
        def _():
            row_messages("y3", "recv")

        @pl.when((t == 0) & (c == 0))
        def _():
            for forward, exists in ((False, has_fwd), (True, has_bwd)):
                @pl.when(exists)
                def _():
                    for chunk in range(NCH3):
                        y_recv(y3, 1, ch3, SEM_Y3, forward, chunk, NCH3).wait_recv()

        for at, size in whole(c):
            acc = dot_nt(flat(z2[2 * k + 3, pl.ds(at, size), 0]), wp3r[...]) + b3c[...]
            taps = [flat(y3[k + side, pl.ds(first, size)]) for first in (at - 1, at, at + 1) for side in AROUND]
            acc = acc + dot(jnp.concatenate([tap[:, :c2] for tap in taps], axis=1), w3c[...].reshape(k2, c3))
            acc = acc + dot(jnp.concatenate([tap[:, c2:] for tap in taps], axis=1), w3e[...].reshape(9 * (c3 - c2), c3))
            zo[k + 1, pl.ds(at - 1, size)] = relu(acc).astype(BF16).reshape(size, n, c3)

        @pl.when((t == 0) & ships)
        def _():
            ship(c).start()

        @pl.when(((t == 0) & is0) | (t == -1))
        def _():
            put(c).start()
    phase(1, NCH3, z3_item)

    for shift in SHIFTS:
        @pl.when(has_fwd & (s == shift))
        def _():
            for half in BOTH:
                x_copy(shift, half).wait_send()

    def drain(c, carry):
        @pl.when(has_fwd)
        def _():
            y_copy(y1, PAIRS, ch, SEM_Y1, True, c, NCH).wait_send()
            z_copy(z1, PAIRS, ch, SEM_Z1, c).wait_send()
            y_copy(y2, 2, ch, SEM_Y2, True, c, NCH).wait_send()
            z_copy(z2, 2, ch // 2, SEM_Z2, c).wait_send()

        @pl.when(has_bwd)
        def _():
            y_copy(y1, PAIRS, ch, SEM_Y1, False, c, NCH).wait_send()
            y_copy(y2, 2, ch, SEM_Y2, False, c, NCH).wait_send()
        return carry
    loop(NCH, drain)

    def drain3(c, carry):
        @pl.when(has_fwd)
        def _():
            y_copy(y3, 1, ch3, SEM_Y3, True, c, NCH3).wait_send()

        @pl.when(has_bwd)
        def _():
            y_copy(y3, 1, ch3, SEM_Y3, False, c, NCH3).wait_send()

        @pl.when(ships)
        def _():
            ship(c).wait_send()

        @pl.when((s == 1) & has_fwd)
        def _():
            ship_recv(c).wait_recv()

        @pl.when(is0 | first_extra)
        def _():
            put(c).wait()
        return carry
    loop(NCH3, drain3)
    for name in ROW_SEM:
        row_messages(name, "sent")


def solution(mesh):
    rows = mesh.shape["row"]
    cols = mesh.shape["col"]
    tile_spec = P("batch", "row", "col")

    def local_blocks(x, w1d, b1d, w1c, b1c, wp1, w2d, b2d, w2c, b2c, wp2, w3d, b3d, w3c, b3c, wp3):
        n, h, w, c0 = x.shape
        c1, c2, c3 = w1d.shape[3], w2d.shape[3], w3d.shape[3]
        h4, h8 = h // 4, h // 8
        dims = (n, h, c0, c1, c2, c3, rows, cols)
        pair = 2 * c0
        xt = jnp.moveaxis(x, 1, 3).reshape(n, PAIRS, pair, h)
        args = (xt, w1d.reshape(3, 3 * c0, c1), w1c.reshape(9 * c1, c1), wp1, w2d.reshape(9 * c1, c2), w2c.reshape(9 * c2, c2), wp2,
                jnp.swapaxes(w3d.reshape(9, c2, c3), 1, 2), w3c.reshape(9, c3, c3), wp3.T,
                b1d, b1c, b2d, b2c, b3d, b3c)
        vm = pltpu.VMEM
        dma = pltpu.SemaphoreType.DMA
        flops = 14 * x.size * (c0 + c1)
        out = pl.pallas_call(
            functools.partial(kernel, dims),
            out_shape=jax.ShapeDtypeStruct((h8, n, c3), BF16),
            in_specs=[pl.BlockSpec(memory_space=pl.ANY)] * len(args),
            out_specs=pl.BlockSpec(memory_space=pl.ANY),
            scratch_shapes=[
                vm(shape, BF16) for shape in (
                    (PAIRS, n, pair, h), (2, n, pair, h // 2), (n, h, 2 * pair), (h, h), (n * BLOCK, n * BLOCK),
                    (6, h4 + 1, 4, n, pair), (7, h4 + 2, 2, n, c1), (7, h4 + 1, 2, n, c1),
                    (5, h4 + 2, n, c2), (5, h8 + 1, 2, n, c2), (4, h8 + 2, n, c3), (2, h8, n, c3),
                    (10 * pair, 2 * c1), (12 * c1 + 2 * pair, 2 * c1), (9 * c1, c2), (9 * c2 + c1, c2),
                    (9, c3, c2), (9, c2, c3), (9, c2, c3), (9, c3 - c2, c3), (c3, c2))
            ] + [vm((1, width), F32) for width in (c1, c1, c2, c2, c3, c3)] + [
                dma((count,)) for count in (32, 4, 10 * NCH, 10 * NCH, 12 * MAX_PLAN, 12 * MAX_PLAN, 3 * NCH3)],
            compiler_params=pltpu.CompilerParams(collective_id=0, has_side_effects=True, vmem_limit_bytes=63 << 20),
            cost_estimate=pl.CostEstimate(flops=flops, bytes_accessed=x.size * 4, transcendentals=0),
        )(*args)
        return jnp.swapaxes(out, 0, 1).reshape(n, h8, 1, c3)

    return jax.shard_map(local_blocks, mesh=mesh, in_specs=(tile_spec,) + (P(),) * 15, out_specs=tile_spec, check_vma=False)
```

```python
import functools

import jax
import jax.numpy as jnp
from jax import lax
from jax.experimental import pallas as pl
from jax.experimental.pallas import tpu as pltpu
from jax.sharding import PartitionSpec as P

BF16 = jnp.bfloat16
F32 = jnp.float32
SHIFTS = (0, 1)
NCH = 4
NCH3 = 2
PAIRS = 4
MAX_PLAN = 5
BLOCK = 16
UNROLL = 8
OWN, HALO = BOTH = range(2)
AROUND = (1, 2, 3)
NEAR = range(-2, 3)
UP, DOWN = (False,), (True,)
NT = (((1,), (1,)), ((), ()))


def relu(value):
    return jnp.maximum(value, 0.0)


def loop(count, body):
    lax.fori_loop(0, count, body, 0)


def row_plan(kind, width, s_send, s_recv):
    if kind == "x":
        own = (0, width - 1)
        need = (-1, width - 1) if s_recv == 0 else (0, width)
        src_at, dst_at = 2 - s_send, 2 - s_recv
    elif kind == "y":
        own = (s_send, width - 1 + s_send)
        need = (s_recv - 1, s_recv + width)
        src_at, dst_at = 2 - s_send, 2 - s_recv
    else:
        own = (s_send, width - 1 + s_send)
        need = (-1, width - 1) if s_recv == 0 else (0, width + 1)
        src_at, dst_at = 3 - 2 * s_send, 3 - 2 * s_recv
    plan = []
    for dist in NEAR:
        lo = max(own[0], width * dist + need[0])
        hi = min(own[1], width * dist + need[1])
        if lo <= hi:
            plan.append((dist, lo + src_at, lo - width * dist + dst_at, hi - lo + 1, False))
        if kind != "x" and s_send == 1 and s_recv == 0 and dist >= 0 and need[0] + width * dist <= 0 <= need[1] + width * dist:
            plan.append((dist, src_at, dst_at - width * dist, 1, True))
    return plan


def kernel(dims, x_hbm, w1d_h, w1c_h, wp1_h, w2d_h, w2c_h, wp2_h, w3d_h, w3c_h, wp3_h, b1d_h, b1c_h, b2d_h, b2c_h, b3d_h, b3c_h, out_hbm,
           raw, xh, turned, eye, mix, xs, y1, z1, y2, z2, y3, zo, w1d, w1c, w2d, w2c, w3r, w3d, w3c, w3e, wp3r,
           b1d, b1c, b2d, b2c, b3d, b3c, load_sem, x_sem, col_send, col_recv, row_send, row_recv, out_sem):
    n, h, c0, c1, c2, c3, rows, cols = dims
    h4, h8 = h // 4, h // 8
    ch, ch3 = h4 // NCH, h8 // NCH3
    hh = h // 2
    row = lax.axis_index("row")
    col = lax.axis_index("col")
    s = lax.rem(row, 2)
    is0 = s == 0
    first_extra = (s == 1) & (col == 0)
    last_void = (s == 1) & (col == cols - 1)
    t_first = jnp.where(first_extra, -1, 0)
    fwd_col = jnp.where(is0, col + 1, col - 1)
    bwd_col = jnp.where(is0, col - 1, col + 1)
    has_fwd = (fwd_col >= 0) & (fwd_col < cols)
    has_bwd = (bwd_col >= 0) & (bwd_col < cols)

    load_count = []

    def load(src, dst):
        load_count.append(dst)
        return pltpu.make_async_copy(src, dst, load_sem.at[len(load_count) - 1])

    k1, k2 = 9 * c1, 9 * c2
    pair = 2 * c0
    x_loads = [load(x_hbm.at[:, q], raw.at[q]) for q in range(PAIRS)]
    w1d_loads = [load(b1d_h, b1d.at[0]), load(b1c_h, b1c.at[0])]
    w1c_loads = []
    for p in BOTH:
        lanes = pl.ds(p * c1, c1)
        for kh in range(3):
            w1d_loads.append(load(w1d_h.at[kh], w1d.at[pl.ds((kh + 2 * p) * 2 * pair + c0, 3 * c0), lanes]))
        w1c_loads.append(load(w1c_h, w1c.at[pl.ds(p * 3 * c1, k1), lanes]))
        w1c_loads.append(load(wp1_h, w1c.at[pl.ds(12 * c1 + p * pair, c0), lanes]))
    w2d_loads = [load(w2d_h, w2d), load(b2d_h, b2d.at[0])]
    w2c_loads = [load(w2c_h, w2c.at[pl.ds(0, k2)]), load(wp2_h, w2c.at[pl.ds(k2, c1)]), load(b2c_h, b2c.at[0])]
    w3d_loads = [load(w3d_h, w3r), load(b3d_h, b3d.at[0]), load(wp3_h, wp3r)]
    w3c_loads = [load(w3c_h.at[:, pl.ds(0, c2)], w3c), load(w3c_h.at[:, pl.ds(c2, c3 - c2)], w3e), load(b3c_h, b3c.at[0])]
    for copy in x_loads:
        copy.start()

    def row_refs(name, slots, down, side):
        ref = refs[name]
        last = ref.shape[1] - (2 if ROW_SEM[name][0] == "y" else 1)
        own_at, halo_at = (last, 0) if down else (1, last + 1)
        at = own_at if side == OWN else halo_at
        subs = 1 if len(ref.shape) == 4 else ref.shape[2]
        if subs == 1:
            return ref.at[slots, at]
        return ref.at[slots, at, subs - 1 if down else 0]

    refs = dict(x=xs, y1=y1, z1=z1, y2=y2, z2=z2, y3=y3)
    ROW_SEM = {}
    for name, kind, width in (("x", "x", PAIRS), ("y1", "y", PAIRS), ("z1", "z", PAIRS), ("y2", "y", 2), ("z2", "z", 2), ("y3", "y", 1)):
        ROW_SEM[name] = (kind, width, 2 * MAX_PLAN * len(ROW_SEM))

    def directions(name):
        return (True, False) if ROW_SEM[name][0] == "y" else (True,)

    def dot(lhs, rhs):
        return jnp.dot(lhs, rhs, preferred_element_type=F32)

    def zero_slot(ref, idx):
        ref[idx] = jnp.zeros(ref.shape[1:], ref.dtype)

    def dot(lhs, rhs):
        return jnp.dot(lhs, rhs, preferred_element_type=F32)

    def zero_slot(ref, idx):
        def body(i, carry):
            ref[idx, i] = jnp.zeros(ref.shape[2:], ref.dtype)
            return carry
        loop(ref.shape[1], body)

    for name in ROW_SEM:
        for down in directions(name):
            edge = row_refs(name, slice(None), down, HALO)
            edge[...] = jnp.zeros(edge.shape, BF16)

    @pl.when(col == cols - 1)
    def _():
        for ref in (y1, y2, y3):
            zero_slot(ref, ref.shape[0] - 1)

    barrier = pltpu.get_barrier_semaphore()
    around = 0
    for step in range(-1, 2):
        for dist in NEAR:
            near_row, near_col = row + step, col + dist
            ok = (near_row >= 0) & (near_row < rows) & (near_col >= 0) & (near_col < cols)
            around = around + ok.astype(jnp.int32)

            @pl.when(ok)
            def _():
                pl.semaphore_signal(barrier, inc=1, device_id={"row": near_row, "col": near_col}, device_id_type=pl.DeviceIdType.MESH)

    @pl.when(col == 0)
    def _():
        for ref in (y1, y2, y3):
            zero_slot(ref, 1 - s)
        for ref in (z1, z2):
            zero_slot(ref, 2 - 2 * s)

    @pl.when(first_extra)
    def _():
        zero_slot(xs, 0)

    def zero_xh(first, size):
        def body(i, carry):
            for half in BOTH:
                xh[half, i, pl.ds(first, size)] = jnp.zeros((size, hh), BF16)
            return carry
        loop(n, body)

    @pl.when(is0)
    def _():
        zero_xh(0, c0)

    @pl.when(jnp.logical_not(has_bwd))
    def _():
        zero_xh(0, pair)

    def unit_where(size, source):
        at = lax.broadcasted_iota(jnp.int32, (size, size), 0)
        return (at == source(lax.broadcasted_iota(jnp.int32, (size, size), 1))).astype(F32).astype(BF16)

    eye[...] = unit_where(h, lambda at: at)
    mix[...] = unit_where(n * BLOCK, lambda at: (at & (BLOCK - 1)) * n + (at >> BLOCK.bit_length() - 1))

    def zero_part(ref, first, size, p):
        ref[pl.ds(first, size), pl.ds(p * c1, c1)] = jnp.zeros((size, c1), BF16)

    for p in BOTH:
        for kh in range(5):
            tap_at = kh * 2 * pair
            used = 2 * p <= kh < 2 * p + 3
            zero_part(w1d, tap_at, c0 if used else 2 * pair, p)
        zero_part(w1c, (1 - p) * k1, 3 * c1, p)
        proj_at = 12 * c1
        zero_part(w1c, proj_at + (1 - p) * pair, pair, p)
        zero_part(w1c, proj_at + p * pair + c0, c0, p)
    for copy in x_loads:
        copy.wait()
    pl.semaphore_wait(barrier, around)

    def remote(src, dst, send_sem, recv_sem, to_row, to_col):
        return pltpu.make_async_remote_copy(src_ref=src, dst_ref=dst, send_sem=send_sem, recv_sem=recv_sem,
                                            device_id={"row": to_row, "col": to_col}, device_id_type=pl.DeviceIdType.MESH)

    def x_copy(shift, half):
        lanes = pl.ds(half * hh, hh)
        if shift == 0:
            src, dst = raw.at[PAIRS - 1, :, pl.ds(c0, c0), lanes], xh.at[half, :, pl.ds(c0, c0)]
        else:
            src, dst = raw.at[0, :, :, lanes], xh.at[half]
        return remote(src, dst, x_sem.at[half], x_sem.at[2 + half], row, fwd_col)

    for shift in SHIFTS:
        @pl.when(has_fwd & (s == shift))
        def _():
            for half in BOTH:
                x_copy(shift, half).start()

    def y_copy(ref, width, rows_per, sem0, forward, chunk, nch):
        to_right = is0 if forward else jnp.logical_not(is0)
        src_slot = jnp.where(to_right, width + 1, 2)
        dst_slot = jnp.where(to_right, 1, width + 2)
        part = pl.ds(1 + chunk * rows_per, rows_per)
        sem = sem0 + (0 if forward else nch) + chunk
        return remote(ref.at[src_slot, part], ref.at[dst_slot, part], col_send.at[sem], col_recv.at[sem], row, fwd_col if forward else bwd_col)

    def y_recv(ref, width, rows_per, sem0, forward, chunk, nch):
        to_right = is0 if forward else jnp.logical_not(is0)
        dst_slot = jnp.where(to_right, 1, width + 2)
        part = pl.ds(1 + chunk * rows_per, rows_per)
        sem = sem0 + (0 if forward else nch) + chunk
        return remote(ref.at[dst_slot, part], ref.at[dst_slot, part], col_send.at[sem], col_recv.at[sem], row, bwd_col if forward else fwd_col)

    def z_copy(ref, width, rows_per, sem0, chunk):
        src_slot = jnp.where(is0, width + 2, 2)
        dst_slot = jnp.where(is0, 2, width + 2)
        part = pl.ds(1 + chunk * rows_per, rows_per)
        sem = sem0 + chunk
        return remote(ref.at[src_slot, part], ref.at[dst_slot, part], col_send.at[sem], col_recv.at[sem], row, fwd_col)

    def z_recv(ref, width, rows_per, sem0, chunk):
        dst_slot = jnp.where(is0, 2, width + 2)
        part = pl.ds(1 + chunk * rows_per, rows_per)
        sem = sem0 + chunk
        return remote(ref.at[dst_slot, part], ref.at[dst_slot, part], col_send.at[sem], col_recv.at[sem], row, bwd_col)

    SEM_Y1, SEM_Z1, SEM_Y2, SEM_Z2, SEM_Y3 = (i * 2 * NCH for i in range(5))

    def row_messages(name, act, ways=None):
        kind, width, sem0 = ROW_SEM[name]
        for down in ways or directions(name):
            for s_send, s_recv in zip(SHIFTS, reversed(SHIFTS)):
                step = 1 if down else -1
                for i, (dist, src, dst, count, extra) in enumerate(row_plan(kind, width, s_send, s_recv)):
                    sem = sem0 + i + (0 if down else MAX_PLAN)
                    if act == "recv":
                        from_row, from_col = row - step, col - dist
                        ok = (s == s_recv) & (from_row >= 0) & (from_row < rows) & (from_col >= 0) & (from_col < cols)
                        if extra:
                            ok = ok & (from_col == 0)

                        @pl.when(ok)
                        def _():
                            ref = row_refs(name, pl.ds(dst, count), down, HALO)
                            remote(ref, ref, row_send.at[sem], row_recv.at[sem], from_row, from_col).wait_recv()
                    else:
                        to_row, to_col = row + step, col + dist
                        ok = (s == s_send) & (to_row >= 0) & (to_row < rows) & (to_col >= 0) & (to_col < cols)
                        if extra:
                            ok = ok & (col == 0)

                        @pl.when(ok)
                        def _():
                            copy = remote(row_refs(name, pl.ds(src, count), down, OWN), row_refs(name, pl.ds(dst, count), down, HALO),
                                          row_send.at[sem], row_recv.at[sem], to_row, to_col)
                            if act == "send":
                                copy.start()
                            else:
                                copy.wait_send()

    def send_edges(name, chunk, nch):
        @pl.when(chunk == 0)
        def _():
            row_messages(name, "send", UP)

        @pl.when(chunk == nch - 1)
        def _():
            row_messages(name, "send", DOWN)

    def to_rows(value):
        return value.astype(BF16).reshape(BLOCK // 4, 4, n, pair)

    def turn_group(q):
        def turn(i, carry):
            for j in range(UNROLL):
                at = i * UNROLL + j
                block = raw[pl.ds(q, 2), at].reshape(2 * pair, h)
                turned[at] = lax.dot_general(eye[...], block, NT, preferred_element_type=F32).astype(BF16)
            return carry
        loop(n // UNROLL, turn)

        def place(i, carry):
            for j in range(UNROLL):
                at = i * UNROLL + j
                block = turned[:, pl.ds(at * BLOCK, BLOCK), :].reshape(n * BLOCK, 2 * pair)
                moved = dot(mix[...], block)
                for side in BOTH:
                    xs[q + 2 - s + side, pl.ds(1 + at * (BLOCK // 4), BLOCK // 4)] = to_rows(moved[:, side * pair:(side + 1) * pair])
            return carry
        loop(h // BLOCK // UNROLL, place)

    def turn_halo(half):
        slot = jnp.where(is0, 1, PAIRS + 1)
        unit = eye[:hh, :hh]
        many = min(UNROLL, n // 2)

        def turn(i, carry):
            for j in range(many):
                at = 2 * (i * many + j)
                block = xh[half, pl.ds(at, 2)].reshape(2 * pair, hh)
                both = lax.dot_general(unit, block, NT, preferred_element_type=F32).astype(BF16)
                for side in BOTH:
                    turned[at + side, :hh, :pair] = both[:, side * pair:(side + 1) * pair]
            return carry
        loop(n // 2 // many, turn)

        def place(i):
            blocks = [turned[:, pl.ds((2 * i + j) * BLOCK, BLOCK), :pair].reshape(n * BLOCK, pair) for j in BOTH]
            moved = dot(mix[...], jnp.concatenate(blocks, axis=1))
            for j in BOTH:
                first = 1 + half * (h4 // 2) + (2 * i + j) * (BLOCK // 4)
                xs[slot, pl.ds(first, BLOCK // 4)] = to_rows(moved[:, j * pair:(j + 1) * pair])
        for i in range(hh // BLOCK // 2):
            place(i)

    for copy in w1d_loads + w1c_loads + w2d_loads + w2c_loads + w3d_loads + w3c_loads:
        copy.start()

    def flat(value):
        return value.reshape(value.shape[0] * n, value.shape[-1])

    def parts(first, count):
        size = count // 2
        return tuple((first + i * size, size) for i in BOTH)

    def dot_nt(lhs, rhs):
        return lax.dot_general(lhs, rhs, NT, preferred_element_type=F32)

    def rows_down(at):
        return (at - 1, 1), (at, 0), (at, 1)

    def whole(c):
        return ((1 + c * ch3, ch3),)

    def own_col(t, width):
        return jnp.where(is0, width - 1 - t, t)

    def phase(width, nch, item):
        def body(at, carry):
            item(lax.div(at, nch) - 1, lax.rem(at, nch))
            return carry
        lax.fori_loop((t_first + 1) * nch, (width + 1) * nch, body, 0)

    def y1_job(t, c):
        k = own_col(t, PAIRS)
        at = 1 + c * ch
        taps = []
        for kh in range(5):
            first, sub = (at - 1, 3) if kh == 0 else (at, kh - 1)
            for side in (1, 2):
                taps.append(flat(xs[k + side, pl.ds(first, ch), sub]))
        acc = dot(jnp.concatenate(taps, axis=1), w1d[...])
        void = last_void & (t == 3)
        for p in BOTH:
            val = relu(acc[:, p * c1:(p + 1) * c1] + b1d[...])
            val = jnp.where(void, 0.0, val)
            y1[k + 2, pl.ds(at, ch), p] = val.astype(BF16).reshape(ch, n, c1)

    def own_group(group, carry):
        turn_group(2 * group)
        return carry
    loop(PAIRS // 2, own_group)
    row_messages("x", "send")
    for copy in w1d_loads:
        copy.wait()
    def turn_weight(i, carry):
        for j in range(3):
            tap = 3 * i + j
            w3d[tap] = dot_nt(eye[:c2, :c2], w3r[tap]).astype(BF16)
        return carry

    def turn_weights():
        for copy in w3d_loads:
            copy.wait()
        loop(3, turn_weight)

    early = 3 - t_first

    def y1_item(item, carry):
        @pl.when(item == lax.div(3 * early, 2))
        def _():
            row_messages("x", "recv")

        half = item - 2 * early

        @pl.when((half == 1) & jnp.logical_not(is0))
        def _():
            turn_weights()

        @pl.when(half >= 0)
        def _():
            for shift in SHIFTS:
                @pl.when(has_bwd & (s == shift))
                def _():
                    ref = xh.at[half, :, pl.ds(c0, c0)] if shift == 0 else xh.at[half]
                    remote(ref, ref, x_sem.at[half], x_sem.at[2 + half], row, bwd_col).wait_recv()
            turn_halo(half)

        jobs = []
        for j in BOTH:
            at = 2 * item + j
            t = jnp.where(at < 3 * early, lax.div(at, 3) + t_first, jnp.where(half >= 0, 3, at - 3 * early + t_first))
            c = jnp.where(at < 3 * early, lax.rem(at, 3) + 1, jnp.where(half >= 0, at - NCH * early, 0))
            jobs.append((t, c))
        for t, c in jobs:
            y1_job(t, c)
        send_edges("y1", half, 2)

        for t, c in jobs:
            @pl.when((t == 0) & has_fwd)
            def _():
                y_copy(y1, PAIRS, ch, SEM_Y1, True, c, NCH).start()

            @pl.when((t == 3) & has_bwd)
            def _():
                y_copy(y1, PAIRS, ch, SEM_Y1, False, c, NCH).start()
        return carry
    loop(2 * (PAIRS - t_first), y1_item)
    for copy in w1c_loads:
        copy.wait()

    def wait_halo(ref, width, rows_per, sem0, forward, half, nch):
        exists = has_bwd if forward else has_fwd

        split = nch - nch // 4
        for part in BOTH:
            @pl.when(exists & (half == part))
            def _():
                for c in range(split, nch) if part else range(split):
                    y_recv(ref, width, rows_per, sem0, forward, c, nch).wait_recv()

    def z1_job(t, c):
        k = own_col(t, PAIRS)
        at = 1 + c * ch
        taps = []
        for first, sub in ((at - 1, 1), (at, 0), (at, 1), (at + 1, 0)):
            for side in AROUND:
                taps.append(flat(y1[k + side, pl.ds(first, ch), sub]))
        for sub in (0, 2):
            taps.append(flat(xs[k + 2, pl.ds(at, ch), sub]))
        acc = dot(jnp.concatenate(taps, axis=1), w1c[...])
        for p in BOTH:
            val = relu(acc[:, p * c1:(p + 1) * c1] + b1c[...])
            z1[k + 3 - s, pl.ds(at, ch), p] = val.astype(BF16).reshape(ch, n, c1)

    extra = -t_first

    def z1_item(item, carry):
        inner = item - extra
        edge = inner - NCH - extra
        more = (inner < 0) | (extra == 1) & (inner == NCH)

        @pl.when(inner == 2)
        def _():
            row_messages("y1", "recv")

        half = lax.rem(edge, 2)
        far = edge >= 2

        @pl.when((edge == 0) & is0)
        def _():
            turn_weights()

        @pl.when((edge >= 0) & (edge < 2))
        def _():
            wait_halo(y1, PAIRS, ch, SEM_Y1, False, half, NCH)

        @pl.when(far)
        def _():
            wait_halo(y1, PAIRS, ch, SEM_Y1, True, half, NCH)

        mid = jnp.where(inner < 2, inner + 1, jnp.where(inner == 2, 0, inner))
        edge_col = jnp.where(far, 3, 0)
        for j in BOTH:
            t = jnp.where(more, -1, jnp.where(edge >= 0, edge_col, j + 1))
            c = jnp.where(more, jnp.where(inner < 0, j + 1, 3 * j), jnp.where(edge >= 0, 2 * half + j, mid))
            z1_job(t, c)

        @pl.when((edge >= 0) & (edge < 2) & has_fwd)
        def _():
            for j in BOTH:
                z_copy(z1, PAIRS, ch, SEM_Z1, 2 * half + j).start()
        return carry
    loop(2 * (NCH + extra), z1_item)
    row_messages("z1", "send")
    for copy in w2d_loads:
        copy.wait()

    def y2_job(t, at, size):
        k = own_col(t, 2)
        taps = []
        for first, sub in rows_down(at):
            for side in range(3):
                taps.append(flat(z1[2 * k + 2 + side, pl.ds(first, size), sub]))
        acc = dot(jnp.concatenate(taps, axis=1), w2d[...])
        val = relu(acc + b2d[...])
        val = jnp.where(last_void & (t == 1), 0.0, val)
        y2[k + 2, pl.ds(at, size)] = val.astype(BF16).reshape(size, n, c2)

    def y2_inner(item, carry):
        t = t_first + lax.div(item, 2)
        late = lax.rem(item, 2)

        @pl.when(item == 1)
        def _():
            row_messages("z1", "recv")

        chunks = (1 + 2 * late, 2 - 2 * late)
        for c in chunks:
            y2_job(t, 1 + c * ch, ch)

        @pl.when((t == 0) & has_fwd)
        def _():
            for c in chunks:
                y_copy(y2, 2, ch, SEM_Y2, True, c, NCH).start()
        return carry
    loop(2 + 2 * extra, y2_inner)

    def y2_edge(c, carry):
        @pl.when(has_bwd)
        def _():
            z_recv(z1, PAIRS, ch, SEM_Z1, c).wait_recv()

        for at, size in parts(1 + c * ch, ch):
            y2_job(jnp.int32(1), at, size)

        send_edges("y2", c, NCH)

        @pl.when(has_bwd)
        def _():
            y_copy(y2, 2, ch, SEM_Y2, False, c, NCH).start()
        return carry
    loop(NCH, y2_edge)
    for copy in w2c_loads:
        copy.wait()

    def z2_job(t, c):
        k = own_col(t, 2)
        at = 1 + c * ch
        taps = []
        for first in (at - 1, at, at + 1):
            for side in AROUND:
                taps.append(flat(y2[k + side, pl.ds(first, ch)]))
        taps.append(flat(z1[2 * k + 3, pl.ds(at, ch), 0]))
        acc = dot(jnp.concatenate(taps, axis=1), w2c[...])
        val = relu(acc + b2c[...]).astype(BF16).reshape(ch // 2, 2, n, c2)
        z2[k + 3 - s, pl.ds(1 + c * (ch // 2), ch // 2)] = val

    row_messages("y2", "recv")

    def z2_item(item, carry):
        edge = item - 2 * extra
        half = lax.rem(item, 2)
        near = (edge >= 0) & (edge < 2)

        @pl.when(near)
        def _():
            wait_halo(y2, 2, ch, SEM_Y2, False, half, NCH)

        @pl.when(edge >= 2)
        def _():
            wait_halo(y2, 2, ch, SEM_Y2, True, half, NCH)

        for j in BOTH:
            z2_job(lax.div(edge + 2, 2) - 1, 2 * half + j)

        @pl.when(near & has_fwd)
        def _():
            for j in BOTH:
                z_copy(z2, 2, ch // 2, SEM_Z2, 2 * half + j).start()
        return carry
    loop(NCH + 2 * extra, z2_item)
    row_messages("z2", "send")

    def y3_item(t, c):
        k = t

        @pl.when((t == t_first) & (c == 0))
        def _():
            row_messages("z2", "recv")

        @pl.when((t == 0) & has_bwd)
        def _():
            for j in range(NCH // NCH3):
                z_recv(z2, 2, ch // 2, SEM_Z2, c * (NCH // NCH3) + j).wait_recv()

        for at, size in whole(c):
            taps = [flat(z2[2 * k + 2 + side, pl.ds(first, size), sub]) for first, sub in rows_down(at) for side in range(3)]
            acc = dot(jnp.concatenate(taps, axis=1), w3d[...].reshape(k2, c3)) + b3d[...]
            val = jnp.where(last_void & (t == 0), 0.0, relu(acc))
            y3[k + 2, pl.ds(at, size)] = val.astype(BF16).reshape(size, n, c3)

        @pl.when(t == 0)
        def _():
            send_edges("y3", c, NCH3)

        @pl.when((t == 0) & has_fwd)
        def _():
            y_copy(y3, 1, ch3, SEM_Y3, True, c, NCH3).start()

        @pl.when((t == 0) & has_bwd)
        def _():
            y_copy(y3, 1, ch3, SEM_Y3, False, c, NCH3).start()
    phase(1, NCH3, y3_item)
    for copy in w3c_loads:
        copy.wait()

    ships = (s == 1) & has_bwd
    z3_parts = ((0, ch3 - 1), (ch3 - 1, ch3 + 1))

    def ship(c, to_col):
        part = pl.ds(*z3_parts[c])
        return remote(zo.at[1, part], out_hbm.at[part], out_sem.at[c], out_sem.at[NCH3 + c], row, to_col)

    keep = jnp.where(is0, 1, 0)

    def put(c):
        part = pl.ds(*z3_parts[c])
        return pltpu.make_async_copy(zo.at[keep, part], out_hbm.at[part], out_sem.at[2 * NCH3 + c])

    def z3_col(i, carry):
        k = t_first + i

        @pl.when(i == 0)
        def _():
            row_messages("y3", "recv")

        for c, (first, size) in enumerate(z3_parts):
            @pl.when(k == 0)
            def _():
                for forward, exists in ((False, has_fwd), (True, has_bwd)):
                    @pl.when(exists)
                    def _():
                        y_recv(y3, 1, ch3, SEM_Y3, forward, c, NCH3).wait_recv()

            acc = dot_nt(flat(z2[2 * k + 3, pl.ds(1 + first, size), 0]), wp3r[...]) + b3c[...]
            taps = [flat(y3[k + side, pl.ds(first + down, size)]) for down in range(3) for side in AROUND]
            acc = acc + dot(jnp.concatenate([tap[:, :c2] for tap in taps], axis=1), w3c[...].reshape(k2, c3))
            acc = acc + dot(jnp.concatenate([tap[:, c2:] for tap in taps], axis=1), w3e[...].reshape(9 * (c3 - c2), c3))
            zo[k + 1, pl.ds(first, size)] = relu(acc).astype(BF16).reshape(size, n, c3)

            @pl.when((k == 0) & ships)
            def _():
                ship(c, bwd_col).start()

            @pl.when(((k == 0) & is0) | (k == -1))
            def _():
                put(c).start()
        return carry
    loop(1 + extra, z3_col)

    for shift in SHIFTS:
        @pl.when(has_fwd & (s == shift))
        def _():
            for half in BOTH:
                x_copy(shift, half).wait_send()

    def drain(c, carry):
        @pl.when(has_fwd)
        def _():
            y_copy(y1, PAIRS, ch, SEM_Y1, True, c, NCH).wait_send()
            z_copy(z1, PAIRS, ch, SEM_Z1, c).wait_send()
            y_copy(y2, 2, ch, SEM_Y2, True, c, NCH).wait_send()
            z_copy(z2, 2, ch // 2, SEM_Z2, c).wait_send()

        @pl.when(has_bwd)
        def _():
            y_copy(y1, PAIRS, ch, SEM_Y1, False, c, NCH).wait_send()
            y_copy(y2, 2, ch, SEM_Y2, False, c, NCH).wait_send()
        return carry
    loop(NCH, drain)

    def drain3(c):
        @pl.when(has_fwd)
        def _():
            y_copy(y3, 1, ch3, SEM_Y3, True, c, NCH3).wait_send()

        @pl.when(has_bwd)
        def _():
            y_copy(y3, 1, ch3, SEM_Y3, False, c, NCH3).wait_send()

        @pl.when(ships)
        def _():
            ship(c, bwd_col).wait_send()

        @pl.when((s == 1) & has_fwd)
        def _():
            ship(c, fwd_col).wait_recv()

        @pl.when(is0 | first_extra)
        def _():
            put(c).wait()
    for c in range(NCH3):
        drain3(c)
    for name in ROW_SEM:
        row_messages(name, "sent")


def solution(mesh):
    rows = mesh.shape["row"]
    cols = mesh.shape["col"]
    tile_spec = P("batch", "row", "col")

    def local_blocks(x, w1d, b1d, w1c, b1c, wp1, w2d, b2d, w2c, b2c, wp2, w3d, b3d, w3c, b3c, wp3):
        n, h, w, c0 = x.shape
        c1, c2, c3 = w1d.shape[3], w2d.shape[3], w3d.shape[3]
        h4, h8 = h // 4, h // 8
        dims = (n, h, c0, c1, c2, c3, rows, cols)
        pair = 2 * c0
        xt = jnp.moveaxis(x, 1, 3).reshape(n, PAIRS, pair, h)
        args = (xt, w1d.reshape(3, 3 * c0, c1), w1c.reshape(9 * c1, c1), wp1, w2d.reshape(9 * c1, c2), w2c.reshape(9 * c2, c2), wp2,
                jnp.swapaxes(w3d.reshape(9, c2, c3), 1, 2), w3c.reshape(9, c3, c3), wp3.T,
                b1d, b1c, b2d, b2c, b3d, b3c)
        vm = pltpu.VMEM
        dma = pltpu.SemaphoreType.DMA
        flops = 14 * x.size * (c0 + c1)
        out = pl.pallas_call(
            functools.partial(kernel, dims),
            out_shape=jax.ShapeDtypeStruct((h8, n, c3), BF16),
            in_specs=[pl.BlockSpec(memory_space=pl.ANY)] * len(args),
            out_specs=pl.BlockSpec(memory_space=pl.ANY),
            scratch_shapes=[
                vm(shape, BF16) for shape in (
                    (PAIRS, n, pair, h), (2, n, pair, h // 2), (n, h, 2 * pair), (h, h), (n * BLOCK, n * BLOCK),
                    (6, h4 + 1, 4, n, pair), (7, h4 + 2, 2, n, c1), (7, h4 + 1, 2, n, c1),
                    (5, h4 + 2, n, c2), (5, h8 + 1, 2, n, c2), (4, h8 + 2, n, c3), (2, h8, n, c3),
                    (10 * pair, 2 * c1), (12 * c1 + 2 * pair, 2 * c1), (9 * c1, c2), (9 * c2 + c1, c2),
                    (9, c3, c2), (9, c2, c3), (9, c2, c3), (9, c3 - c2, c3), (c3, c2))
            ] + [vm((1, width), F32) for width in (c1, c1, c2, c2, c3, c3)] + [
                dma((count,)) for count in (32, 4, 10 * NCH, 10 * NCH, 12 * MAX_PLAN, 12 * MAX_PLAN, 3 * NCH3)],
            compiler_params=pltpu.CompilerParams(collective_id=0, has_side_effects=True, vmem_limit_bytes=63 << 20),
            cost_estimate=pl.CostEstimate(flops=flops, bytes_accessed=x.size * 4, transcendentals=0),
        )(*args)
        return jnp.swapaxes(out, 0, 1).reshape(n, h8, 1, c3)

    return jax.shard_map(local_blocks, mesh=mesh, in_specs=(tile_spec,) + (P(),) * 15, out_specs=tile_spec, check_vma=False)
```

```python
import functools

import jax
import jax.numpy as jnp
from jax import lax
from jax.experimental import pallas as pl
from jax.experimental.pallas import tpu as pltpu
from jax.sharding import PartitionSpec as P

BF16 = jnp.bfloat16
F32 = jnp.float32
SHIFTS = (0, 1)
NCH = 4
NCH3 = 2
PAIRS = 4
MAX_PLAN = 5
BLOCK = 16
UNROLL = 8
OWN, HALO = BOTH = range(2)
AROUND = (1, 2, 3)
NEAR = range(-2, 3)
UP, DOWN = (False,), (True,)
NT = (((1,), (1,)), ((), ()))


def relu(value):
    return jnp.maximum(value, 0.0)


def loop(count, body):
    lax.fori_loop(0, count, body, 0)


def row_plan(kind, width, s_send, s_recv):
    if kind == "x":
        own = (0, width - 1)
        need = (-1, width - 1) if s_recv == 0 else (0, width)
        src_at, dst_at = 2 - s_send, 2 - s_recv
    elif kind == "y":
        own = (s_send, width - 1 + s_send)
        need = (s_recv - 1, s_recv + width)
        src_at, dst_at = 2 - s_send, 2 - s_recv
    else:
        own = (s_send, width - 1 + s_send)
        need = (-1, width - 1) if s_recv == 0 else (0, width + 1)
        src_at, dst_at = 3 - 2 * s_send, 3 - 2 * s_recv
    plan = []
    for dist in NEAR:
        lo = max(own[0], width * dist + need[0])
        hi = min(own[1], width * dist + need[1])
        if lo <= hi:
            plan.append((dist, lo + src_at, lo - width * dist + dst_at, hi - lo + 1, False))
        if kind != "x" and s_send == 1 and s_recv == 0 and dist >= 0 and need[0] + width * dist <= 0 <= need[1] + width * dist:
            plan.append((dist, src_at, dst_at - width * dist, 1, True))
    return plan


def kernel(dims, x_hbm, w1d_h, w1c_h, wp1_h, w2d_h, w2c_h, wp2_h, w3d_h, w3c_h, wp3_h, b1d_h, b1c_h, b2d_h, b2c_h, b3d_h, b3c_h, out_hbm,
           raw, xh, turned, eye, mix, xs, y1, z1, y2, z2, y3, zo, w1d, w1c, w2d, w2c, w3r, w3d, w3c, w3e, wp3r,
           b1d, b1c, b2d, b2c, b3d, b3c, load_sem, x_sem, col_send, col_recv, row_send, row_recv, out_sem):
    n, h, c0, c1, c2, c3, rows, cols = dims
    h4, h8 = h // 4, h // 8
    ch, ch3 = h4 // NCH, h8 // NCH3
    hh = h // 2
    row = lax.axis_index("row")
    col = lax.axis_index("col")
    s = lax.rem(row, 2)
    is0 = s == 0
    first_extra = (s == 1) & (col == 0)
    last_void = (s == 1) & (col == cols - 1)
    t_first = jnp.where(first_extra, -1, 0)
    fwd_col = jnp.where(is0, col + 1, col - 1)
    bwd_col = jnp.where(is0, col - 1, col + 1)
    has_fwd = (fwd_col >= 0) & (fwd_col < cols)
    has_bwd = (bwd_col >= 0) & (bwd_col < cols)

    load_count = []

    def load(src, dst):
        load_count.append(dst)
        return pltpu.make_async_copy(src, dst, load_sem.at[len(load_count) - 1])

    k1, k2 = 9 * c1, 9 * c2
    pair = 2 * c0
    x_loads = [load(x_hbm.at[:, q], raw.at[q]) for q in range(PAIRS)]
    w1d_loads = [load(b1d_h, b1d.at[0]), load(b1c_h, b1c.at[0])]
    w1c_loads = []
    for p in BOTH:
        lanes = pl.ds(p * c1, c1)
        for kh in range(3):
            w1d_loads.append(load(w1d_h.at[kh], w1d.at[pl.ds((kh + 2 * p) * 2 * pair + c0, 3 * c0), lanes]))
        w1c_loads.append(load(w1c_h, w1c.at[pl.ds(p * 3 * c1, k1), lanes]))
        w1c_loads.append(load(wp1_h, w1c.at[pl.ds(12 * c1 + p * pair, c0), lanes]))
    w2d_loads = [load(w2d_h, w2d), load(b2d_h, b2d.at[0])]
    w2c_loads = [load(w2c_h, w2c.at[pl.ds(0, k2)]), load(wp2_h, w2c.at[pl.ds(k2, c1)]), load(b2c_h, b2c.at[0])]
    w3d_loads = [load(w3d_h, w3r), load(b3d_h, b3d.at[0]), load(wp3_h, wp3r)]
    w3c_loads = [load(w3c_h.at[:, pl.ds(0, c2)], w3c), load(w3c_h.at[:, pl.ds(c2, c3 - c2)], w3e), load(b3c_h, b3c.at[0])]
    for copy in x_loads:
        copy.start()

    def row_refs(name, slots, down, side):
        ref = refs[name]
        last = ref.shape[1] - (2 if ROW_SEM[name][0] == "y" else 1)
        own_at, halo_at = (last, 0) if down else (1, last + 1)
        at = own_at if side == OWN else halo_at
        subs = 1 if len(ref.shape) == 4 else ref.shape[2]
        if subs == 1:
            return ref.at[slots, at]
        return ref.at[slots, at, subs - 1 if down else 0]

    refs = dict(x=xs, y1=y1, z1=z1, y2=y2, z2=z2, y3=y3)
    ROW_SEM = {}
    for name, kind, width in (("x", "x", PAIRS), ("y1", "y", PAIRS), ("z1", "z", PAIRS), ("y2", "y", 2), ("z2", "z", 2), ("y3", "y", 1)):
        ROW_SEM[name] = (kind, width, 2 * MAX_PLAN * len(ROW_SEM))

    def directions(name):
        return (True, False) if ROW_SEM[name][0] == "y" else (True,)

    def dot(lhs, rhs):
        return jnp.dot(lhs, rhs, preferred_element_type=F32)

    def zero_slot(ref, idx):
        ref[idx] = jnp.zeros(ref.shape[1:], ref.dtype)

    def dot(lhs, rhs):
        return jnp.dot(lhs, rhs, preferred_element_type=F32)

    def zero_slot(ref, idx):
        def body(i, carry):
            ref[idx, i] = jnp.zeros(ref.shape[2:], ref.dtype)
            return carry
        loop(ref.shape[1], body)

    for name in ROW_SEM:
        for down in directions(name):
            edge = row_refs(name, slice(None), down, HALO)
            edge[...] = jnp.zeros(edge.shape, BF16)

    @pl.when(col == cols - 1)
    def _():
        for ref in (y1, y2, y3):
            zero_slot(ref, ref.shape[0] - 1)

    barrier = pltpu.get_barrier_semaphore()
    around = 0
    for step in range(-1, 2):
        for dist in NEAR:
            near_row, near_col = row + step, col + dist
            ok = (near_row >= 0) & (near_row < rows) & (near_col >= 0) & (near_col < cols)
            around = around + ok.astype(jnp.int32)

            @pl.when(ok)
            def _():
                pl.semaphore_signal(barrier, inc=1, device_id={"row": near_row, "col": near_col}, device_id_type=pl.DeviceIdType.MESH)

    @pl.when(col == 0)
    def _():
        for ref in (y1, y2, y3):
            zero_slot(ref, 1 - s)
        for ref in (z1, z2):
            zero_slot(ref, 2 - 2 * s)

    @pl.when(first_extra)
    def _():
        zero_slot(xs, 0)

    def zero_xh(first, size):
        def body(i, carry):
            for half in BOTH:
                xh[half, i, pl.ds(first, size)] = jnp.zeros((size, hh), BF16)
            return carry
        loop(n, body)

    @pl.when(is0)
    def _():
        zero_xh(0, c0)

    @pl.when(jnp.logical_not(has_bwd))
    def _():
        zero_xh(0, pair)

    def unit_where(size, source):
        at = lax.broadcasted_iota(jnp.int32, (size, size), 0)
        return (at == source(lax.broadcasted_iota(jnp.int32, (size, size), 1))).astype(F32).astype(BF16)

    eye[...] = unit_where(h, lambda at: at)
    mix[...] = unit_where(n * BLOCK, lambda at: (at & (BLOCK - 1)) * n + (at >> BLOCK.bit_length() - 1))

    def zero_part(ref, first, size, p):
        ref[pl.ds(first, size), pl.ds(p * c1, c1)] = jnp.zeros((size, c1), BF16)

    for p in BOTH:
        for kh in range(5):
            tap_at = kh * 2 * pair
            used = 2 * p <= kh < 2 * p + 3
            zero_part(w1d, tap_at, c0 if used else 2 * pair, p)
        zero_part(w1c, (1 - p) * k1, 3 * c1, p)
        proj_at = 12 * c1
        zero_part(w1c, proj_at + (1 - p) * pair, pair, p)
        zero_part(w1c, proj_at + p * pair + c0, c0, p)
    for copy in x_loads:
        copy.wait()
    pl.semaphore_wait(barrier, around)

    def remote(src, dst, send_sem, recv_sem, to_row, to_col):
        return pltpu.make_async_remote_copy(src_ref=src, dst_ref=dst, send_sem=send_sem, recv_sem=recv_sem,
                                            device_id={"row": to_row, "col": to_col}, device_id_type=pl.DeviceIdType.MESH)

    def x_copy(shift, half):
        lanes = pl.ds(half * hh, hh)
        if shift == 0:
            src, dst = raw.at[PAIRS - 1, :, pl.ds(c0, c0), lanes], xh.at[half, :, pl.ds(c0, c0)]
        else:
            src, dst = raw.at[0, :, :, lanes], xh.at[half]
        return remote(src, dst, x_sem.at[half], x_sem.at[2 + half], row, fwd_col)

    for shift in SHIFTS:
        @pl.when(has_fwd & (s == shift))
        def _():
            for half in BOTH:
                x_copy(shift, half).start()

    def y_copy(ref, width, rows_per, sem0, forward, chunk, nch):
        to_right = is0 if forward else jnp.logical_not(is0)
        src_slot = jnp.where(to_right, width + 1, 2)
        dst_slot = jnp.where(to_right, 1, width + 2)
        part = pl.ds(1 + chunk * rows_per, rows_per)
        sem = sem0 + (0 if forward else nch) + chunk
        return remote(ref.at[src_slot, part], ref.at[dst_slot, part], col_send.at[sem], col_recv.at[sem], row, fwd_col if forward else bwd_col)

    def y_recv(ref, width, rows_per, sem0, forward, chunk, nch):
        to_right = is0 if forward else jnp.logical_not(is0)
        dst_slot = jnp.where(to_right, 1, width + 2)
        part = pl.ds(1 + chunk * rows_per, rows_per)
        sem = sem0 + (0 if forward else nch) + chunk
        return remote(ref.at[dst_slot, part], ref.at[dst_slot, part], col_send.at[sem], col_recv.at[sem], row, bwd_col if forward else fwd_col)

    def z_copy(ref, width, rows_per, sem0, chunk):
        src_slot = jnp.where(is0, width + 2, 2)
        dst_slot = jnp.where(is0, 2, width + 2)
        part = pl.ds(1 + chunk * rows_per, rows_per)
        sem = sem0 + chunk
        return remote(ref.at[src_slot, part], ref.at[dst_slot, part], col_send.at[sem], col_recv.at[sem], row, fwd_col)

    def z_recv(ref, width, rows_per, sem0, chunk):
        dst_slot = jnp.where(is0, 2, width + 2)
        part = pl.ds(1 + chunk * rows_per, rows_per)
        sem = sem0 + chunk
        return remote(ref.at[dst_slot, part], ref.at[dst_slot, part], col_send.at[sem], col_recv.at[sem], row, bwd_col)

    SEM_Y1, SEM_Z1, SEM_Y2, SEM_Z2, SEM_Y3 = (i * 2 * NCH for i in range(5))

    def row_messages(name, act, ways=None):
        kind, width, sem0 = ROW_SEM[name]
        for down in ways or directions(name):
            for s_send, s_recv in zip(SHIFTS, reversed(SHIFTS)):
                step = 1 if down else -1
                for i, (dist, src, dst, count, extra) in enumerate(row_plan(kind, width, s_send, s_recv)):
                    sem = sem0 + i + (0 if down else MAX_PLAN)
                    if act == "recv":
                        from_row, from_col = row - step, col - dist
                        ok = (s == s_recv) & (from_row >= 0) & (from_row < rows) & (from_col >= 0) & (from_col < cols)
                        if extra:
                            ok = ok & (from_col == 0)

                        @pl.when(ok)
                        def _():
                            ref = row_refs(name, pl.ds(dst, count), down, HALO)
                            remote(ref, ref, row_send.at[sem], row_recv.at[sem], from_row, from_col).wait_recv()
                    else:
                        to_row, to_col = row + step, col + dist
                        ok = (s == s_send) & (to_row >= 0) & (to_row < rows) & (to_col >= 0) & (to_col < cols)
                        if extra:
                            ok = ok & (col == 0)

                        @pl.when(ok)
                        def _():
                            copy = remote(row_refs(name, pl.ds(src, count), down, OWN), row_refs(name, pl.ds(dst, count), down, HALO),
                                          row_send.at[sem], row_recv.at[sem], to_row, to_col)
                            if act == "send":
                                copy.start()
                            else:
                                copy.wait_send()

    def send_edges(name, chunk, nch):
        @pl.when(chunk == 0)
        def _():
            row_messages(name, "send", UP)

        @pl.when(chunk == nch - 1)
        def _():
            row_messages(name, "send", DOWN)

    def to_rows(value):
        return value.astype(BF16).reshape(BLOCK // 4, 4, n, pair)

    def turn_group(q):
        def turn(i, carry):
            for j in range(UNROLL):
                at = i * UNROLL + j
                block = raw[pl.ds(q, 2), at].reshape(2 * pair, h)
                turned[at] = lax.dot_general(eye[...], block, NT, preferred_element_type=F32).astype(BF16)
            return carry
        loop(n // UNROLL, turn)

        def place(i, carry):
            for j in range(UNROLL):
                at = i * UNROLL + j
                block = turned[:, pl.ds(at * BLOCK, BLOCK), :].reshape(n * BLOCK, 2 * pair)
                moved = dot(mix[...], block)
                for side in BOTH:
                    xs[q + 2 - s + side, pl.ds(1 + at * (BLOCK // 4), BLOCK // 4)] = to_rows(moved[:, side * pair:(side + 1) * pair])
            return carry
        loop(h // BLOCK // UNROLL, place)

    def turn_halo(half):
        slot = jnp.where(is0, 1, PAIRS + 1)
        unit = eye[:hh, :hh]
        many = min(UNROLL, n // 2)

        def turn(i, carry):
            for j in range(many):
                at = 2 * (i * many + j)
                block = xh[half, pl.ds(at, 2)].reshape(2 * pair, hh)
                both = lax.dot_general(unit, block, NT, preferred_element_type=F32).astype(BF16)
                for side in BOTH:
                    turned[at + side, :hh, :pair] = both[:, side * pair:(side + 1) * pair]
            return carry
        loop(n // 2 // many, turn)

        def place(i):
            blocks = [turned[:, pl.ds((2 * i + j) * BLOCK, BLOCK), :pair].reshape(n * BLOCK, pair) for j in BOTH]
            moved = dot(mix[...], jnp.concatenate(blocks, axis=1))
            for j in BOTH:
                first = 1 + half * (h4 // 2) + (2 * i + j) * (BLOCK // 4)
                xs[slot, pl.ds(first, BLOCK // 4)] = to_rows(moved[:, j * pair:(j + 1) * pair])
        for i in range(hh // BLOCK // 2):
            place(i)

    for copy in w1d_loads + w1c_loads + w2d_loads + w2c_loads + w3d_loads + w3c_loads:
        copy.start()

    def flat(value):
        return value.reshape(value.shape[0] * n, value.shape[-1])

    def parts(first, count):
        size = count // 2
        return tuple((first + i * size, size) for i in BOTH)

    def dot_nt(lhs, rhs):
        return lax.dot_general(lhs, rhs, NT, preferred_element_type=F32)

    def rows_down(at):
        return (at - 1, 1), (at, 0), (at, 1)

    def whole(c):
        return ((1 + c * ch3, ch3),)

    def own_col(t, width):
        return jnp.where(is0, width - 1 - t, t)

    def phase(width, nch, item):
        def body(at, carry):
            item(lax.div(at, nch) - 1, lax.rem(at, nch))
            return carry
        lax.fori_loop((t_first + 1) * nch, (width + 1) * nch, body, 0)

    def y1_job(t, c):
        k = own_col(t, PAIRS)
        at = 1 + c * ch
        taps = []
        for kh in range(5):
            first, sub = (at - 1, 3) if kh == 0 else (at, kh - 1)
            for side in (1, 2):
                taps.append(flat(xs[k + side, pl.ds(first, ch), sub]))
        acc = dot(jnp.concatenate(taps, axis=1), w1d[...])
        void = last_void & (t == 3)
        for p in BOTH:
            val = relu(acc[:, p * c1:(p + 1) * c1] + b1d[...])
            val = jnp.where(void, 0.0, val)
            y1[k + 2, pl.ds(at, ch), p] = val.astype(BF16).reshape(ch, n, c1)

    def own_group(group, carry):
        turn_group(2 * group)
        return carry
    loop(PAIRS // 2, own_group)
    row_messages("x", "send")
    for copy in w1d_loads:
        copy.wait()
    def turn_weight(i, carry):
        for j in range(3):
            tap = 3 * i + j
            w3d[tap] = dot_nt(eye[:c2, :c2], w3r[tap]).astype(BF16)
        return carry

    def turn_weights():
        for copy in w3d_loads:
            copy.wait()
        loop(3, turn_weight)

    early = 3 - t_first

    def y1_item(item, carry):
        @pl.when(item == lax.div(3 * early, 2))
        def _():
            row_messages("x", "recv")

        half = item - 2 * early

        @pl.when(half >= 0)
        def _():
            for shift in SHIFTS:
                @pl.when(has_bwd & (s == shift))
                def _():
                    ref = xh.at[half, :, pl.ds(c0, c0)] if shift == 0 else xh.at[half]
                    remote(ref, ref, x_sem.at[half], x_sem.at[2 + half], row, bwd_col).wait_recv()
            turn_halo(half)

        jobs = []
        for j in BOTH:
            at = 2 * item + j
            t = jnp.where(at < 3 * early, lax.div(at, 3) + t_first, jnp.where(half >= 0, 3, at - 3 * early + t_first))
            c = jnp.where(at < 3 * early, lax.rem(at, 3) + 1, jnp.where(half >= 0, at - NCH * early, 0))
            jobs.append((t, c))
        for t, c in jobs:
            y1_job(t, c)
        send_edges("y1", half, 2)

        for t, c in jobs:
            @pl.when((t == 0) & has_fwd)
            def _():
                y_copy(y1, PAIRS, ch, SEM_Y1, True, c, NCH).start()

            @pl.when((t == 3) & has_bwd)
            def _():
                y_copy(y1, PAIRS, ch, SEM_Y1, False, c, NCH).start()
        return carry
    loop(2 * (PAIRS - t_first), y1_item)
    for copy in w1c_loads:
        copy.wait()

    def wait_halo(ref, width, rows_per, sem0, forward, half, nch):
        exists = has_bwd if forward else has_fwd

        split = nch - nch // 4
        for part in BOTH:
            @pl.when(exists & (half == part))
            def _():
                for c in range(split, nch) if part else range(split):
                    y_recv(ref, width, rows_per, sem0, forward, c, nch).wait_recv()

    def z1_job(t, c):
        k = own_col(t, PAIRS)
        at = 1 + c * ch
        taps = []
        for first, sub in ((at - 1, 1), (at, 0), (at, 1), (at + 1, 0)):
            for side in AROUND:
                taps.append(flat(y1[k + side, pl.ds(first, ch), sub]))
        for sub in (0, 2):
            taps.append(flat(xs[k + 2, pl.ds(at, ch), sub]))
        acc = dot(jnp.concatenate(taps, axis=1), w1c[...])
        for p in BOTH:
            val = relu(acc[:, p * c1:(p + 1) * c1] + b1c[...])
            z1[k + 3 - s, pl.ds(at, ch), p] = val.astype(BF16).reshape(ch, n, c1)

    extra = -t_first

    def z1_item(item, carry):
        inner = item - extra
        edge = inner - NCH - extra
        more = (inner < 0) | (extra == 1) & (inner == NCH)

        @pl.when(inner == 2)
        def _():
            row_messages("y1", "recv")

        half = lax.rem(edge, 2)
        far = edge >= 2

        @pl.when((edge == 0) & is0)
        def _():
            turn_weights()

        @pl.when((edge >= 0) & (edge < 2))
        def _():
            wait_halo(y1, PAIRS, ch, SEM_Y1, False, half, NCH)

        @pl.when(far)
        def _():
            wait_halo(y1, PAIRS, ch, SEM_Y1, True, half, NCH)

        mid = jnp.where(inner < 2, inner + 1, jnp.where(inner == 2, 0, inner))
        edge_col = jnp.where(far, 3, 0)
        for j in BOTH:
            t = jnp.where(more, -1, jnp.where(edge >= 0, edge_col, j + 1))
            c = jnp.where(more, jnp.where(inner < 0, j + 1, 3 * j), jnp.where(edge >= 0, 2 * half + j, mid))
            z1_job(t, c)

        @pl.when((edge >= 0) & (edge < 2) & has_fwd)
        def _():
            for j in BOTH:
                z_copy(z1, PAIRS, ch, SEM_Z1, 2 * half + j).start()
        return carry
    loop(2 * (NCH + extra), z1_item)
    row_messages("z1", "send")
    for copy in w2d_loads:
        copy.wait()

    def y2_job(t, at, size):
        k = own_col(t, 2)
        taps = []
        for first, sub in rows_down(at):
            for side in range(3):
                taps.append(flat(z1[2 * k + 2 + side, pl.ds(first, size), sub]))
        acc = dot(jnp.concatenate(taps, axis=1), w2d[...])
        val = relu(acc + b2d[...])
        val = jnp.where(last_void & (t == 1), 0.0, val)
        y2[k + 2, pl.ds(at, size)] = val.astype(BF16).reshape(size, n, c2)

    def y2_inner(item, carry):
        t = t_first + lax.div(item, 2)
        late = lax.rem(item, 2)

        @pl.when(item == 1)
        def _():
            row_messages("z1", "recv")

        chunks = (1 + 2 * late, 2 - 2 * late)
        for c in chunks:
            y2_job(t, 1 + c * ch, ch)

        @pl.when((t == 0) & has_fwd)
        def _():
            for c in chunks:
                y_copy(y2, 2, ch, SEM_Y2, True, c, NCH).start()
        return carry
    loop(2 + 2 * extra, y2_inner)

    def y2_edge(c, carry):
        @pl.when(has_bwd)
        def _():
            z_recv(z1, PAIRS, ch, SEM_Z1, c).wait_recv()

        for at, size in parts(1 + c * ch, ch):
            y2_job(jnp.int32(1), at, size)

        send_edges("y2", c, NCH)

        @pl.when(has_bwd)
        def _():
            y_copy(y2, 2, ch, SEM_Y2, False, c, NCH).start()
        return carry
    loop(NCH, y2_edge)
    for copy in w2c_loads:
        copy.wait()

    def z2_job(t, c):
        k = own_col(t, 2)
        at = 1 + c * ch
        taps = []
        for first in (at - 1, at, at + 1):
            for side in AROUND:
                taps.append(flat(y2[k + side, pl.ds(first, ch)]))
        taps.append(flat(z1[2 * k + 3, pl.ds(at, ch), 0]))
        acc = dot(jnp.concatenate(taps, axis=1), w2c[...])
        val = relu(acc + b2c[...]).astype(BF16).reshape(ch // 2, 2, n, c2)
        z2[k + 3 - s, pl.ds(1 + c * (ch // 2), ch // 2)] = val

    @pl.when(jnp.logical_not(is0))
    def _():
        turn_weights()

    row_messages("y2", "recv")

    def z2_item(item, carry):
        edge = item - 2 * extra
        half = lax.rem(item, 2)
        near = (edge >= 0) & (edge < 2)

        @pl.when(near)
        def _():
            wait_halo(y2, 2, ch, SEM_Y2, False, half, NCH)

        @pl.when(edge >= 2)
        def _():
            wait_halo(y2, 2, ch, SEM_Y2, True, half, NCH)

        for j in BOTH:
            z2_job(lax.div(edge + 2, 2) - 1, 2 * half + j)

        @pl.when(near & has_fwd)
        def _():
            for j in BOTH:
                z_copy(z2, 2, ch // 2, SEM_Z2, 2 * half + j).start()
        return carry
    loop(NCH + 2 * extra, z2_item)
    row_messages("z2", "send")

    def y3_item(t, c):
        k = t

        @pl.when((t == t_first) & (c == 0))
        def _():
            row_messages("z2", "recv")

        @pl.when((t == 0) & has_bwd)
        def _():
            for j in range(NCH // NCH3):
                z_recv(z2, 2, ch // 2, SEM_Z2, c * (NCH // NCH3) + j).wait_recv()

        for at, size in whole(c):
            taps = [flat(z2[2 * k + 2 + side, pl.ds(first, size), sub]) for first, sub in rows_down(at) for side in range(3)]
            acc = dot(jnp.concatenate(taps, axis=1), w3d[...].reshape(k2, c3)) + b3d[...]
            val = jnp.where(last_void & (t == 0), 0.0, relu(acc))
            y3[k + 2, pl.ds(at, size)] = val.astype(BF16).reshape(size, n, c3)

        @pl.when(t == 0)
        def _():
            send_edges("y3", c, NCH3)

        @pl.when((t == 0) & has_fwd)
        def _():
            y_copy(y3, 1, ch3, SEM_Y3, True, c, NCH3).start()

        @pl.when((t == 0) & has_bwd)
        def _():
            y_copy(y3, 1, ch3, SEM_Y3, False, c, NCH3).start()
    phase(1, NCH3, y3_item)
    for copy in w3c_loads:
        copy.wait()

    ships = (s == 1) & has_bwd
    z3_parts = ((0, ch3 - 1), (ch3 - 1, ch3 + 1))

    def ship(c, to_col):
        part = pl.ds(*z3_parts[c])
        return remote(zo.at[1, part], out_hbm.at[part], out_sem.at[c], out_sem.at[NCH3 + c], row, to_col)

    keep = jnp.where(is0, 1, 0)

    def put(c):
        part = pl.ds(*z3_parts[c])
        return pltpu.make_async_copy(zo.at[keep, part], out_hbm.at[part], out_sem.at[2 * NCH3 + c])

    def z3_col(i, carry):
        k = t_first + i

        @pl.when(i == 0)
        def _():
            row_messages("y3", "recv")

        for c, (first, size) in enumerate(z3_parts):
            @pl.when(k == 0)
            def _():
                for forward, exists in ((False, has_fwd), (True, has_bwd)):
                    @pl.when(exists)
                    def _():
                        y_recv(y3, 1, ch3, SEM_Y3, forward, c, NCH3).wait_recv()

            acc = dot_nt(flat(z2[2 * k + 3, pl.ds(1 + first, size), 0]), wp3r[...]) + b3c[...]
            taps = [flat(y3[k + side, pl.ds(first + down, size)]) for down in range(3) for side in AROUND]
            acc = acc + dot(jnp.concatenate([tap[:, :c2] for tap in taps], axis=1), w3c[...].reshape(k2, c3))
            acc = acc + dot(jnp.concatenate([tap[:, c2:] for tap in taps], axis=1), w3e[...].reshape(9 * (c3 - c2), c3))
            zo[k + 1, pl.ds(first, size)] = relu(acc).astype(BF16).reshape(size, n, c3)

            @pl.when((k == 0) & ships)
            def _():
                ship(c, bwd_col).start()

            @pl.when(((k == 0) & is0) | (k == -1))
            def _():
                put(c).start()
        return carry
    loop(1 + extra, z3_col)

    for shift in SHIFTS:
        @pl.when(has_fwd & (s == shift))
        def _():
            for half in BOTH:
                x_copy(shift, half).wait_send()

    def drain(c, carry):
        @pl.when(has_fwd)
        def _():
            y_copy(y1, PAIRS, ch, SEM_Y1, True, c, NCH).wait_send()
            z_copy(z1, PAIRS, ch, SEM_Z1, c).wait_send()
            y_copy(y2, 2, ch, SEM_Y2, True, c, NCH).wait_send()
            z_copy(z2, 2, ch // 2, SEM_Z2, c).wait_send()

        @pl.when(has_bwd)
        def _():
            y_copy(y1, PAIRS, ch, SEM_Y1, False, c, NCH).wait_send()
            y_copy(y2, 2, ch, SEM_Y2, False, c, NCH).wait_send()
        return carry
    loop(NCH, drain)

    def drain3(c):
        @pl.when(has_fwd)
        def _():
            y_copy(y3, 1, ch3, SEM_Y3, True, c, NCH3).wait_send()

        @pl.when(has_bwd)
        def _():
            y_copy(y3, 1, ch3, SEM_Y3, False, c, NCH3).wait_send()

        @pl.when(ships)
        def _():
            ship(c, bwd_col).wait_send()

        @pl.when((s == 1) & has_fwd)
        def _():
            ship(c, fwd_col).wait_recv()

        @pl.when(is0 | first_extra)
        def _():
            put(c).wait()
    for c in range(NCH3):
        drain3(c)
    for name in ROW_SEM:
        row_messages(name, "sent")


def solution(mesh):
    rows = mesh.shape["row"]
    cols = mesh.shape["col"]
    tile_spec = P("batch", "row", "col")

    def local_blocks(x, w1d, b1d, w1c, b1c, wp1, w2d, b2d, w2c, b2c, wp2, w3d, b3d, w3c, b3c, wp3):
        n, h, w, c0 = x.shape
        c1, c2, c3 = w1d.shape[3], w2d.shape[3], w3d.shape[3]
        h4, h8 = h // 4, h // 8
        dims = (n, h, c0, c1, c2, c3, rows, cols)
        pair = 2 * c0
        xt = jnp.moveaxis(x, 1, 3).reshape(n, PAIRS, pair, h)
        args = (xt, w1d.reshape(3, 3 * c0, c1), w1c.reshape(9 * c1, c1), wp1, w2d.reshape(9 * c1, c2), w2c.reshape(9 * c2, c2), wp2,
                jnp.swapaxes(w3d.reshape(9, c2, c3), 1, 2), w3c.reshape(9, c3, c3), wp3.T,
                b1d, b1c, b2d, b2c, b3d, b3c)
        vm = pltpu.VMEM
        dma = pltpu.SemaphoreType.DMA
        flops = 14 * x.size * (c0 + c1)
        out = pl.pallas_call(
            functools.partial(kernel, dims),
            out_shape=jax.ShapeDtypeStruct((h8, n, c3), BF16),
            in_specs=[pl.BlockSpec(memory_space=pl.ANY)] * len(args),
            out_specs=pl.BlockSpec(memory_space=pl.ANY),
            scratch_shapes=[
                vm(shape, BF16) for shape in (
                    (PAIRS, n, pair, h), (2, n, pair, h // 2), (n, h, 2 * pair), (h, h), (n * BLOCK, n * BLOCK),
                    (6, h4 + 1, 4, n, pair), (7, h4 + 2, 2, n, c1), (7, h4 + 1, 2, n, c1),
                    (5, h4 + 2, n, c2), (5, h8 + 1, 2, n, c2), (4, h8 + 2, n, c3), (2, h8, n, c3),
                    (10 * pair, 2 * c1), (12 * c1 + 2 * pair, 2 * c1), (9 * c1, c2), (9 * c2 + c1, c2),
                    (9, c3, c2), (9, c2, c3), (9, c2, c3), (9, c3 - c2, c3), (c3, c2))
            ] + [vm((1, width), F32) for width in (c1, c1, c2, c2, c3, c3)] + [
                dma((count,)) for count in (32, 4, 10 * NCH, 10 * NCH, 12 * MAX_PLAN, 12 * MAX_PLAN, 3 * NCH3)],
            compiler_params=pltpu.CompilerParams(collective_id=0, has_side_effects=True, vmem_limit_bytes=63 << 20),
            cost_estimate=pl.CostEstimate(flops=flops, bytes_accessed=x.size * 4, transcendentals=0),
        )(*args)
        return jnp.swapaxes(out, 0, 1).reshape(n, h8, 1, c3)

    return jax.shard_map(local_blocks, mesh=mesh, in_specs=(tile_spec,) + (P(),) * 15, out_specs=tile_spec, check_vma=False)
```

```python
import functools

import jax
import jax.numpy as jnp
from jax import lax
from jax.experimental import pallas as pl
from jax.experimental.pallas import tpu as pltpu
from jax.sharding import PartitionSpec as P

BF16 = jnp.bfloat16
F32 = jnp.float32
SHIFTS = (0, 1)
NCH = 4
NCH3 = 2
PAIRS = 4
MAX_PLAN = 5
BLOCK = 16
UNROLL = 8
OWN, HALO = BOTH = range(2)
AROUND = (1, 2, 3)
NEAR = range(-2, 3)
UP, DOWN = (False,), (True,)
NT = (((1,), (1,)), ((), ()))


def relu(value):
    return jnp.maximum(value, 0.0)


def loop(count, body):
    lax.fori_loop(0, count, body, 0)


def row_plan(kind, width, s_send, s_recv):
    if kind == "x":
        own = (0, width - 1)
        need = (-1, width - 1) if s_recv == 0 else (0, width)
        src_at, dst_at = 2 - s_send, 2 - s_recv
    elif kind == "y":
        own = (s_send, width - 1 + s_send)
        need = (s_recv - 1, s_recv + width)
        src_at, dst_at = 2 - s_send, 2 - s_recv
    else:
        own = (s_send, width - 1 + s_send)
        need = (-1, width - 1) if s_recv == 0 else (0, width + 1)
        src_at, dst_at = 3 - 2 * s_send, 3 - 2 * s_recv
    plan = []
    for dist in NEAR:
        lo = max(own[0], width * dist + need[0])
        hi = min(own[1], width * dist + need[1])
        if lo <= hi:
            plan.append((dist, lo + src_at, lo - width * dist + dst_at, hi - lo + 1, False))
        if kind != "x" and s_send == 1 and s_recv == 0 and dist >= 0 and need[0] + width * dist <= 0 <= need[1] + width * dist:
            plan.append((dist, src_at, dst_at - width * dist, 1, True))
    return plan


def kernel(dims, x_hbm, w1d_h, w1c_h, wp1_h, w2d_h, w2c_h, wp2_h, w3d_h, w3c_h, wp3_h, b1d_h, b1c_h, b2d_h, b2c_h, b3d_h, b3c_h, out_hbm,
           raw, xh, turned, eye, mix, xs, y1, z1, y2, z2, y3, zo, w1d, w1c, w2d, w2c, w3r, w3d, w3c, w3e, wp3r,
           b1d, b1c, b2d, b2c, b3d, b3c, load_sem, x_sem, col_send, col_recv, row_send, row_recv, out_sem):
    n, h, c0, c1, c2, c3, rows, cols = dims
    h4, h8 = h // 4, h // 8
    ch, ch3 = h4 // NCH, h8 // NCH3
    hh = h // 2
    row = lax.axis_index("row")
    col = lax.axis_index("col")
    s = lax.rem(row, 2)
    is0 = s == 0
    first_extra = (s == 1) & (col == 0)
    last_void = (s == 1) & (col == cols - 1)
    t_first = jnp.where(first_extra, -1, 0)
    fwd_col = jnp.where(is0, col + 1, col - 1)
    bwd_col = jnp.where(is0, col - 1, col + 1)
    has_fwd = (fwd_col >= 0) & (fwd_col < cols)
    has_bwd = (bwd_col >= 0) & (bwd_col < cols)

    load_count = []

    def load(src, dst):
        load_count.append(dst)
        return pltpu.make_async_copy(src, dst, load_sem.at[len(load_count) - 1])

    k1, k2 = 9 * c1, 9 * c2
    pair = 2 * c0
    x_loads = [load(x_hbm.at[:, q], raw.at[q]) for q in range(PAIRS)]
    w1d_loads = [load(b1d_h, b1d.at[0]), load(b1c_h, b1c.at[0])]
    w1c_loads = []
    for p in BOTH:
        lanes = pl.ds(p * c1, c1)
        for kh in range(3):
            w1d_loads.append(load(w1d_h.at[kh], w1d.at[pl.ds((kh + 2 * p) * 2 * pair + c0, 3 * c0), lanes]))
        w1c_loads.append(load(w1c_h, w1c.at[pl.ds(p * 3 * c1, k1), lanes]))
        w1c_loads.append(load(wp1_h, w1c.at[pl.ds(12 * c1 + p * pair, c0), lanes]))
    w2d_loads = [load(w2d_h, w2d), load(b2d_h, b2d.at[0])]
    w2c_loads = [load(w2c_h, w2c.at[pl.ds(0, k2)]), load(wp2_h, w2c.at[pl.ds(k2, c1)]), load(b2c_h, b2c.at[0])]
    w3d_loads = [load(w3d_h, w3r), load(b3d_h, b3d.at[0]), load(wp3_h, wp3r)]
    w3c_loads = [load(w3c_h.at[:, pl.ds(0, c2)], w3c), load(w3c_h.at[:, pl.ds(c2, c3 - c2)], w3e), load(b3c_h, b3c.at[0])]
    for copy in x_loads:
        copy.start()

    def row_refs(name, slots, down, side):
        ref = refs[name]
        last = ref.shape[1] - (2 if ROW_SEM[name][0] == "y" else 1)
        own_at, halo_at = (last, 0) if down else (1, last + 1)
        at = own_at if side == OWN else halo_at
        subs = 1 if len(ref.shape) == 4 else ref.shape[2]
        if subs == 1:
            return ref.at[slots, at]
        return ref.at[slots, at, subs - 1 if down else 0]

    refs = dict(x=xs, y1=y1, z1=z1, y2=y2, z2=z2, y3=y3)
    ROW_SEM = {}
    for name, kind, width in (("x", "x", PAIRS), ("y1", "y", PAIRS), ("z1", "z", PAIRS), ("y2", "y", 2), ("z2", "z", 2), ("y3", "y", 1)):
        ROW_SEM[name] = (kind, width, 2 * MAX_PLAN * len(ROW_SEM))

    def directions(name):
        return (True, False) if ROW_SEM[name][0] == "y" else (True,)

    def dot(lhs, rhs):
        return jnp.dot(lhs, rhs, preferred_element_type=F32)

    def zero_slot(ref, idx):
        ref[idx] = jnp.zeros(ref.shape[1:], ref.dtype)

    def dot(lhs, rhs):
        return jnp.dot(lhs, rhs, preferred_element_type=F32)

    def zero_slot(ref, idx):
        def body(i, carry):
            ref[idx, i] = jnp.zeros(ref.shape[2:], ref.dtype)
            return carry
        loop(ref.shape[1], body)

    for name in ROW_SEM:
        for down in directions(name):
            edge = row_refs(name, slice(None), down, HALO)
            edge[...] = jnp.zeros(edge.shape, BF16)

    @pl.when(col == cols - 1)
    def _():
        for ref in (y1, y2, y3):
            zero_slot(ref, ref.shape[0] - 1)

    barrier = pltpu.get_barrier_semaphore()
    around = 0
    for step in range(-1, 2):
        for dist in NEAR:
            near_row, near_col = row + step, col + dist
            ok = (near_row >= 0) & (near_row < rows) & (near_col >= 0) & (near_col < cols)
            around = around + ok.astype(jnp.int32)

            @pl.when(ok)
            def _():
                pl.semaphore_signal(barrier, inc=1, device_id={"row": near_row, "col": near_col}, device_id_type=pl.DeviceIdType.MESH)

    @pl.when(col == 0)
    def _():
        for ref in (y1, y2, y3):
            zero_slot(ref, 1 - s)
        for ref in (z1, z2):
            zero_slot(ref, 2 - 2 * s)

    @pl.when(first_extra)
    def _():
        zero_slot(xs, 0)

    def zero_xh(first, size):
        def body(i, carry):
            for half in BOTH:
                xh[half, i, pl.ds(first, size)] = jnp.zeros((size, hh), BF16)
            return carry
        loop(n, body)

    @pl.when(is0)
    def _():
        zero_xh(0, c0)

    @pl.when(jnp.logical_not(has_bwd))
    def _():
        zero_xh(0, pair)

    def unit_where(size, source):
        at = lax.broadcasted_iota(jnp.int32, (size, size), 0)
        return (at == source(lax.broadcasted_iota(jnp.int32, (size, size), 1))).astype(F32).astype(BF16)

    eye[...] = unit_where(h, lambda at: at)
    mix[...] = unit_where(n * BLOCK, lambda at: (at & (BLOCK - 1)) * n + (at >> BLOCK.bit_length() - 1))

    def zero_part(ref, first, size, p):
        ref[pl.ds(first, size), pl.ds(p * c1, c1)] = jnp.zeros((size, c1), BF16)

    for p in BOTH:
        for kh in range(5):
            tap_at = kh * 2 * pair
            used = 2 * p <= kh < 2 * p + 3
            zero_part(w1d, tap_at, c0 if used else 2 * pair, p)
        zero_part(w1c, (1 - p) * k1, 3 * c1, p)
        proj_at = 12 * c1
        zero_part(w1c, proj_at + (1 - p) * pair, pair, p)
        zero_part(w1c, proj_at + p * pair + c0, c0, p)
    for copy in x_loads:
        copy.wait()
    pl.semaphore_wait(barrier, around)

    def remote(src, dst, send_sem, recv_sem, to_row, to_col):
        return pltpu.make_async_remote_copy(src_ref=src, dst_ref=dst, send_sem=send_sem, recv_sem=recv_sem,
                                            device_id={"row": to_row, "col": to_col}, device_id_type=pl.DeviceIdType.MESH)

    def x_copy(shift, half):
        lanes = pl.ds(half * hh, hh)
        if shift == 0:
            src, dst = raw.at[PAIRS - 1, :, pl.ds(c0, c0), lanes], xh.at[half, :, pl.ds(c0, c0)]
        else:
            src, dst = raw.at[0, :, :, lanes], xh.at[half]
        return remote(src, dst, x_sem.at[half], x_sem.at[2 + half], row, fwd_col)

    for shift in SHIFTS:
        @pl.when(has_fwd & (s == shift))
        def _():
            for half in BOTH:
                x_copy(shift, half).start()

    def y_copy(ref, width, rows_per, sem0, forward, chunk, nch):
        to_right = is0 if forward else jnp.logical_not(is0)
        src_slot = jnp.where(to_right, width + 1, 2)
        dst_slot = jnp.where(to_right, 1, width + 2)
        part = pl.ds(1 + chunk * rows_per, rows_per)
        sem = sem0 + (0 if forward else nch) + chunk
        return remote(ref.at[src_slot, part], ref.at[dst_slot, part], col_send.at[sem], col_recv.at[sem], row, fwd_col if forward else bwd_col)

    def y_recv(ref, width, rows_per, sem0, forward, chunk, nch):
        to_right = is0 if forward else jnp.logical_not(is0)
        dst_slot = jnp.where(to_right, 1, width + 2)
        part = pl.ds(1 + chunk * rows_per, rows_per)
        sem = sem0 + (0 if forward else nch) + chunk
        return remote(ref.at[dst_slot, part], ref.at[dst_slot, part], col_send.at[sem], col_recv.at[sem], row, bwd_col if forward else fwd_col)

    def z_copy(ref, width, rows_per, sem0, chunk):
        src_slot = jnp.where(is0, width + 2, 2)
        dst_slot = jnp.where(is0, 2, width + 2)
        part = pl.ds(1 + chunk * rows_per, rows_per)
        sem = sem0 + chunk
        return remote(ref.at[src_slot, part], ref.at[dst_slot, part], col_send.at[sem], col_recv.at[sem], row, fwd_col)

    def z_recv(ref, width, rows_per, sem0, chunk):
        dst_slot = jnp.where(is0, 2, width + 2)
        part = pl.ds(1 + chunk * rows_per, rows_per)
        sem = sem0 + chunk
        return remote(ref.at[dst_slot, part], ref.at[dst_slot, part], col_send.at[sem], col_recv.at[sem], row, bwd_col)

    SEM_Y1, SEM_Z1, SEM_Y2, SEM_Z2, SEM_Y3 = (i * 2 * NCH for i in range(5))
    y1_whole = (y1, PAIRS, h4, SEM_Y1, True, 0, 1)
    z1_half = (z1, PAIRS, 2 * ch, SEM_Z1)
    z2_half = (z2, 2, ch, SEM_Z2)

    def row_messages(name, act, ways=None):
        kind, width, sem0 = ROW_SEM[name]
        for down in ways or directions(name):
            for s_send, s_recv in zip(SHIFTS, reversed(SHIFTS)):
                step = 1 if down else -1
                for i, (dist, src, dst, count, extra) in enumerate(row_plan(kind, width, s_send, s_recv)):
                    sem = sem0 + i + (0 if down else MAX_PLAN)
                    if act == "recv":
                        from_row, from_col = row - step, col - dist
                        ok = (s == s_recv) & (from_row >= 0) & (from_row < rows) & (from_col >= 0) & (from_col < cols)
                        if extra:
                            ok = ok & (from_col == 0)

                        @pl.when(ok)
                        def _():
                            ref = row_refs(name, pl.ds(dst, count), down, HALO)
                            remote(ref, ref, row_send.at[sem], row_recv.at[sem], from_row, from_col).wait_recv()
                    else:
                        to_row, to_col = row + step, col + dist
                        ok = (s == s_send) & (to_row >= 0) & (to_row < rows) & (to_col >= 0) & (to_col < cols)
                        if extra:
                            ok = ok & (col == 0)

                        @pl.when(ok)
                        def _():
                            copy = remote(row_refs(name, pl.ds(src, count), down, OWN), row_refs(name, pl.ds(dst, count), down, HALO),
                                          row_send.at[sem], row_recv.at[sem], to_row, to_col)
                            if act == "send":
                                copy.start()
                            else:
                                copy.wait_send()

    def send_edges(name, chunk, nch):
        @pl.when(chunk == 0)
        def _():
            row_messages(name, "send", UP)

        @pl.when(chunk == nch - 1)
        def _():
            row_messages(name, "send", DOWN)

    def to_rows(value):
        return value.astype(BF16).reshape(BLOCK // 4, 4, n, pair)

    def turn_group(q):
        def turn(i, carry):
            for j in range(UNROLL):
                at = i * UNROLL + j
                block = raw[pl.ds(q, 2), at].reshape(2 * pair, h)
                turned[at] = lax.dot_general(eye[...], block, NT, preferred_element_type=F32).astype(BF16)
            return carry
        loop(n // UNROLL, turn)

        def place(i, carry):
            for j in range(UNROLL):
                at = i * UNROLL + j
                block = turned[:, pl.ds(at * BLOCK, BLOCK), :].reshape(n * BLOCK, 2 * pair)
                moved = dot(mix[...], block)
                for side in BOTH:
                    xs[q + 2 - s + side, pl.ds(1 + at * (BLOCK // 4), BLOCK // 4)] = to_rows(moved[:, side * pair:(side + 1) * pair])
            return carry
        loop(h // BLOCK // UNROLL, place)

    def turn_halo(half):
        slot = jnp.where(is0, 1, PAIRS + 1)
        unit = eye[:hh, :hh]
        many = min(UNROLL, n // 2)

        def turn(i, carry):
            for j in range(many):
                at = 2 * (i * many + j)
                block = xh[half, pl.ds(at, 2)].reshape(2 * pair, hh)
                both = lax.dot_general(unit, block, NT, preferred_element_type=F32).astype(BF16)
                for side in BOTH:
                    turned[at + side, :hh, :pair] = both[:, side * pair:(side + 1) * pair]
            return carry
        loop(n // 2 // many, turn)

        def place(i):
            blocks = [turned[:, pl.ds((2 * i + j) * BLOCK, BLOCK), :pair].reshape(n * BLOCK, pair) for j in BOTH]
            moved = dot(mix[...], jnp.concatenate(blocks, axis=1))
            for j in BOTH:
                first = 1 + half * (h4 // 2) + (2 * i + j) * (BLOCK // 4)
                xs[slot, pl.ds(first, BLOCK // 4)] = to_rows(moved[:, j * pair:(j + 1) * pair])
        for i in range(hh // BLOCK // 2):
            place(i)

    for copy in w1d_loads + w1c_loads + w2d_loads + w2c_loads + w3d_loads + w3c_loads:
        copy.start()

    def flat(value):
        return value.reshape(value.shape[0] * n, value.shape[-1])

    def parts(first, count):
        size = count // 2
        return tuple((first + i * size, size) for i in BOTH)

    def dot_nt(lhs, rhs):
        return lax.dot_general(lhs, rhs, NT, preferred_element_type=F32)

    def rows_down(at):
        return (at - 1, 1), (at, 0), (at, 1)

    def whole(c):
        return ((1 + c * ch3, ch3),)

    def own_col(t, width):
        return jnp.where(is0, width - 1 - t, t)

    def phase(width, nch, item):
        def body(at, carry):
            item(lax.div(at, nch) - 1, lax.rem(at, nch))
            return carry
        lax.fori_loop((t_first + 1) * nch, (width + 1) * nch, body, 0)

    def y1_job(t, c):
        k = own_col(t, PAIRS)
        at = 1 + c * ch
        taps = []
        for kh in range(5):
            first, sub = (at - 1, 3) if kh == 0 else (at, kh - 1)
            for side in (1, 2):
                taps.append(flat(xs[k + side, pl.ds(first, ch), sub]))
        acc = dot(jnp.concatenate(taps, axis=1), w1d[...])
        void = last_void & (t == 3)
        for p in BOTH:
            val = relu(acc[:, p * c1:(p + 1) * c1] + b1d[...])
            val = jnp.where(void, 0.0, val)
            y1[k + 2, pl.ds(at, ch), p] = val.astype(BF16).reshape(ch, n, c1)

    def own_group(group, carry):
        turn_group(2 * group)
        return carry
    loop(PAIRS // 2, own_group)
    row_messages("x", "send")
    for copy in w1d_loads:
        copy.wait()
    def turn_weight(i, carry):
        for j in range(3):
            tap = 3 * i + j
            w3d[tap] = dot_nt(eye[:c2, :c2], w3r[tap]).astype(BF16)
        return carry

    def turn_weights():
        for copy in w3d_loads:
            copy.wait()
        loop(3, turn_weight)

    early = 3 - t_first

    def y1_item(item, carry):
        @pl.when(item == lax.div(3 * early, 2))
        def _():
            row_messages("x", "recv")

        half = item - 2 * early

        @pl.when(half >= 0)
        def _():
            for shift in SHIFTS:
                @pl.when(has_bwd & (s == shift))
                def _():
                    ref = xh.at[half, :, pl.ds(c0, c0)] if shift == 0 else xh.at[half]
                    remote(ref, ref, x_sem.at[half], x_sem.at[2 + half], row, bwd_col).wait_recv()
            turn_halo(half)

        jobs = []
        for j in BOTH:
            at = 2 * item + j
            t = jnp.where(at < 3 * early, lax.div(at, 3) + t_first, jnp.where(half >= 0, 3, at - 3 * early + t_first))
            c = jnp.where(at < 3 * early, lax.rem(at, 3) + 1, jnp.where(half >= 0, at - NCH * early, 0))
            jobs.append((t, c))
        for t, c in jobs:
            y1_job(t, c)
        send_edges("y1", half, 2)

        for t, c in jobs:
            @pl.when((t == 0) & (c == 0) & has_fwd)
            def _():
                y_copy(*y1_whole).start()

            @pl.when((t == 3) & has_bwd)
            def _():
                y_copy(y1, PAIRS, ch, SEM_Y1, False, c, NCH).start()
        return carry
    loop(2 * (PAIRS - t_first), y1_item)
    for copy in w1c_loads:
        copy.wait()

    def wait_halo(ref, width, rows_per, sem0, forward, half, nch):
        exists = has_bwd if forward else has_fwd

        split = nch - nch // 4
        for part in BOTH:
            @pl.when(exists & (half == part))
            def _():
                for c in range(split, nch) if part else range(split):
                    y_recv(ref, width, rows_per, sem0, forward, c, nch).wait_recv()

    def z1_job(t, c):
        k = own_col(t, PAIRS)
        at = 1 + c * ch
        taps = []
        for first, sub in ((at - 1, 1), (at, 0), (at, 1), (at + 1, 0)):
            for side in AROUND:
                taps.append(flat(y1[k + side, pl.ds(first, ch), sub]))
        for sub in (0, 2):
            taps.append(flat(xs[k + 2, pl.ds(at, ch), sub]))
        acc = dot(jnp.concatenate(taps, axis=1), w1c[...])
        for p in BOTH:
            val = relu(acc[:, p * c1:(p + 1) * c1] + b1c[...])
            z1[k + 3 - s, pl.ds(at, ch), p] = val.astype(BF16).reshape(ch, n, c1)

    extra = -t_first

    def z1_item(item, carry):
        inner = item - extra
        edge = inner - NCH - extra
        more = (inner < 0) | (extra == 1) & (inner == NCH)

        @pl.when(inner == 2)
        def _():
            row_messages("y1", "recv")

        half = lax.rem(edge, 2)
        far = edge >= 2

        @pl.when((edge == 0) & is0)
        def _():
            turn_weights()

        @pl.when((edge >= 0) & (edge < 2))
        def _():
            wait_halo(y1, PAIRS, ch, SEM_Y1, False, half, NCH)

        @pl.when((edge == 2) & has_bwd)
        def _():
            y_recv(*y1_whole).wait_recv()

        mid = jnp.where(inner < 2, inner + 1, jnp.where(inner == 2, 0, inner))
        edge_col = jnp.where(far, 3, 0)
        for j in BOTH:
            t = jnp.where(more, -1, jnp.where(edge >= 0, edge_col, j + 1))
            c = jnp.where(more, jnp.where(inner < 0, j + 1, 3 * j), jnp.where(edge >= 0, 2 * half + j, mid))
            z1_job(t, c)

        @pl.when((edge >= 0) & (edge < 2) & has_fwd)
        def _():
            z_copy(*z1_half, half).start()
        return carry
    loop(2 * (NCH + extra), z1_item)
    row_messages("z1", "send")
    for copy in w2d_loads:
        copy.wait()

    def y2_job(t, at, size):
        k = own_col(t, 2)
        taps = []
        for first, sub in rows_down(at):
            for side in range(3):
                taps.append(flat(z1[2 * k + 2 + side, pl.ds(first, size), sub]))
        acc = dot(jnp.concatenate(taps, axis=1), w2d[...])
        val = relu(acc + b2d[...])
        val = jnp.where(last_void & (t == 1), 0.0, val)
        y2[k + 2, pl.ds(at, size)] = val.astype(BF16).reshape(size, n, c2)

    def y2_inner(item, carry):
        t = t_first + lax.div(item, 2)
        late = lax.rem(item, 2)

        @pl.when(item == 1)
        def _():
            row_messages("z1", "recv")

        chunks = (1 + 2 * late, 2 - 2 * late)
        for c in chunks:
            y2_job(t, 1 + c * ch, ch)

        @pl.when((t == 0) & has_fwd)
        def _():
            for c in chunks:
                y_copy(y2, 2, ch, SEM_Y2, True, c, NCH).start()
        return carry
    loop(2 + 2 * extra, y2_inner)

    def y2_edge(c, carry):
        @pl.when(has_bwd & (lax.rem(c, 2) == 0))
        def _():
            z_recv(*z1_half, lax.div(c, 2)).wait_recv()

        for at, size in parts(1 + c * ch, ch):
            y2_job(jnp.int32(1), at, size)

        send_edges("y2", c, NCH)

        @pl.when(has_bwd)
        def _():
            y_copy(y2, 2, ch, SEM_Y2, False, c, NCH).start()
        return carry
    loop(NCH, y2_edge)
    for copy in w2c_loads:
        copy.wait()

    def z2_job(t, c):
        k = own_col(t, 2)
        at = 1 + c * ch
        taps = []
        for first in (at - 1, at, at + 1):
            for side in AROUND:
                taps.append(flat(y2[k + side, pl.ds(first, ch)]))
        taps.append(flat(z1[2 * k + 3, pl.ds(at, ch), 0]))
        acc = dot(jnp.concatenate(taps, axis=1), w2c[...])
        val = relu(acc + b2c[...]).astype(BF16).reshape(ch // 2, 2, n, c2)
        z2[k + 3 - s, pl.ds(1 + c * (ch // 2), ch // 2)] = val

    @pl.when(jnp.logical_not(is0))
    def _():
        turn_weights()

    row_messages("y2", "recv")

    def z2_item(item, carry):
        edge = item - 2 * extra
        half = lax.rem(item, 2)
        near = (edge >= 0) & (edge < 2)

        @pl.when(near)
        def _():
            wait_halo(y2, 2, ch, SEM_Y2, False, half, NCH)

        @pl.when(edge >= 2)
        def _():
            wait_halo(y2, 2, ch, SEM_Y2, True, half, NCH)

        for j in BOTH:
            z2_job(lax.div(edge + 2, 2) - 1, 2 * half + j)

        @pl.when(near & has_fwd)
        def _():
            z_copy(*z2_half, half).start()
        return carry
    loop(NCH + 2 * extra, z2_item)
    row_messages("z2", "send")

    def y3_item(t, c):
        k = t

        @pl.when((t == t_first) & (c == 0))
        def _():
            row_messages("z2", "recv")

        @pl.when((t == 0) & has_bwd)
        def _():
            z_recv(*z2_half, c).wait_recv()

        for at, size in whole(c):
            taps = [flat(z2[2 * k + 2 + side, pl.ds(first, size), sub]) for first, sub in rows_down(at) for side in range(3)]
            acc = dot(jnp.concatenate(taps, axis=1), w3d[...].reshape(k2, c3)) + b3d[...]
            val = jnp.where(last_void & (t == 0), 0.0, relu(acc))
            y3[k + 2, pl.ds(at, size)] = val.astype(BF16).reshape(size, n, c3)

        @pl.when(t == 0)
        def _():
            send_edges("y3", c, NCH3)

        @pl.when((t == 0) & has_fwd)
        def _():
            y_copy(y3, 1, ch3, SEM_Y3, True, c, NCH3).start()

        @pl.when((t == 0) & has_bwd)
        def _():
            y_copy(y3, 1, ch3, SEM_Y3, False, c, NCH3).start()
    phase(1, NCH3, y3_item)
    for copy in w3c_loads:
        copy.wait()

    ships = (s == 1) & has_bwd
    z3_parts = ((0, ch3 - 1), (ch3 - 1, ch3 + 1))

    def ship(c, to_col):
        part = pl.ds(*z3_parts[c])
        return remote(zo.at[1, part], out_hbm.at[part], out_sem.at[c], out_sem.at[NCH3 + c], row, to_col)

    keep = jnp.where(is0, 1, 0)

    def put(c):
        part = pl.ds(*z3_parts[c])
        return pltpu.make_async_copy(zo.at[keep, part], out_hbm.at[part], out_sem.at[2 * NCH3 + c])

    def z3_col(i, carry):
        k = t_first + i

        @pl.when(i == 0)
        def _():
            row_messages("y3", "recv")

        for c, (first, size) in enumerate(z3_parts):
            @pl.when(k == 0)
            def _():
                for forward, exists in ((False, has_fwd), (True, has_bwd)):
                    @pl.when(exists)
                    def _():
                        y_recv(y3, 1, ch3, SEM_Y3, forward, c, NCH3).wait_recv()

            acc = dot_nt(flat(z2[2 * k + 3, pl.ds(1 + first, size), 0]), wp3r[...]) + b3c[...]
            taps = [flat(y3[k + side, pl.ds(first + down, size)]) for down in range(3) for side in AROUND]
            acc = acc + dot(jnp.concatenate([tap[:, :c2] for tap in taps], axis=1), w3c[...].reshape(k2, c3))
            acc = acc + dot(jnp.concatenate([tap[:, c2:] for tap in taps], axis=1), w3e[...].reshape(9 * (c3 - c2), c3))
            zo[k + 1, pl.ds(first, size)] = relu(acc).astype(BF16).reshape(size, n, c3)

            @pl.when((k == 0) & ships)
            def _():
                ship(c, bwd_col).start()

            @pl.when(((k == 0) & is0) | (k == -1))
            def _():
                put(c).start()
        return carry
    loop(1 + extra, z3_col)

    for shift in SHIFTS:
        @pl.when(has_fwd & (s == shift))
        def _():
            for half in BOTH:
                x_copy(shift, half).wait_send()

    def drain(c, carry):
        @pl.when(has_fwd)
        def _():
            y_copy(y2, 2, ch, SEM_Y2, True, c, NCH).wait_send()

        @pl.when(has_bwd)
        def _():
            y_copy(y1, PAIRS, ch, SEM_Y1, False, c, NCH).wait_send()
            y_copy(y2, 2, ch, SEM_Y2, False, c, NCH).wait_send()
        return carry
    loop(NCH, drain)

    @pl.when(has_fwd)
    def _():
        y_copy(*y1_whole).wait_send()
        for half in BOTH:
            z_copy(*z1_half, half).wait_send()
            z_copy(*z2_half, half).wait_send()

    def drain3(c):
        @pl.when(has_fwd)
        def _():
            y_copy(y3, 1, ch3, SEM_Y3, True, c, NCH3).wait_send()

        @pl.when(has_bwd)
        def _():
            y_copy(y3, 1, ch3, SEM_Y3, False, c, NCH3).wait_send()

        @pl.when(ships)
        def _():
            ship(c, bwd_col).wait_send()

        @pl.when((s == 1) & has_fwd)
        def _():
            ship(c, fwd_col).wait_recv()

        @pl.when(is0 | first_extra)
        def _():
            put(c).wait()
    for c in range(NCH3):
        drain3(c)
    for name in ROW_SEM:
        row_messages(name, "sent")


def solution(mesh):
    rows = mesh.shape["row"]
    cols = mesh.shape["col"]
    tile_spec = P("batch", "row", "col")

    def local_blocks(x, w1d, b1d, w1c, b1c, wp1, w2d, b2d, w2c, b2c, wp2, w3d, b3d, w3c, b3c, wp3):
        n, h, w, c0 = x.shape
        c1, c2, c3 = w1d.shape[3], w2d.shape[3], w3d.shape[3]
        h4, h8 = h // 4, h // 8
        dims = (n, h, c0, c1, c2, c3, rows, cols)
        pair = 2 * c0
        xt = jnp.moveaxis(x, 1, 3).reshape(n, PAIRS, pair, h)
        args = (xt, w1d.reshape(3, 3 * c0, c1), w1c.reshape(9 * c1, c1), wp1, w2d.reshape(9 * c1, c2), w2c.reshape(9 * c2, c2), wp2,
                jnp.swapaxes(w3d.reshape(9, c2, c3), 1, 2), w3c.reshape(9, c3, c3), wp3.T,
                b1d, b1c, b2d, b2c, b3d, b3c)
        vm = pltpu.VMEM
        dma = pltpu.SemaphoreType.DMA
        flops = 14 * x.size * (c0 + c1)
        out = pl.pallas_call(
            functools.partial(kernel, dims),
            out_shape=jax.ShapeDtypeStruct((h8, n, c3), BF16),
            in_specs=[pl.BlockSpec(memory_space=pl.ANY)] * len(args),
            out_specs=pl.BlockSpec(memory_space=pl.ANY),
            scratch_shapes=[
                vm(shape, BF16) for shape in (
                    (PAIRS, n, pair, h), (2, n, pair, h // 2), (n, h, 2 * pair), (h, h), (n * BLOCK, n * BLOCK),
                    (6, h4 + 1, 4, n, pair), (7, h4 + 2, 2, n, c1), (7, h4 + 1, 2, n, c1),
                    (5, h4 + 2, n, c2), (5, h8 + 1, 2, n, c2), (4, h8 + 2, n, c3), (2, h8, n, c3),
                    (10 * pair, 2 * c1), (12 * c1 + 2 * pair, 2 * c1), (9 * c1, c2), (9 * c2 + c1, c2),
                    (9, c3, c2), (9, c2, c3), (9, c2, c3), (9, c3 - c2, c3), (c3, c2))
            ] + [vm((1, width), F32) for width in (c1, c1, c2, c2, c3, c3)] + [
                dma((count,)) for count in (32, 4, 10 * NCH, 10 * NCH, 12 * MAX_PLAN, 12 * MAX_PLAN, 3 * NCH3)],
            compiler_params=pltpu.CompilerParams(collective_id=0, has_side_effects=True, vmem_limit_bytes=63 << 20),
            cost_estimate=pl.CostEstimate(flops=flops, bytes_accessed=x.size * 4, transcendentals=0),
        )(*args)
        return jnp.swapaxes(out, 0, 1).reshape(n, h8, 1, c3)

    return jax.shard_map(local_blocks, mesh=mesh, in_specs=(tile_spec,) + (P(),) * 15, out_specs=tile_spec, check_vma=False)
```

```python
import functools

import jax
import jax.numpy as jnp
from jax import lax
from jax.experimental import pallas as pl
from jax.experimental.pallas import tpu as pltpu
from jax.sharding import PartitionSpec as P

BF16 = jnp.bfloat16
F32 = jnp.float32
SHIFTS = (0, 1)
NCH = 4
NCH3 = 2
PAIRS = 4
MAX_PLAN = 5
BLOCK = 16
UNROLL = 8
OWN, HALO = BOTH = range(2)
AROUND = (1, 2, 3)
NEAR = range(-2, 3)
UP, DOWN = (False,), (True,)
NT = (((1,), (1,)), ((), ()))


def relu(value):
    return jnp.maximum(value, 0.0)


def loop(count, body):
    lax.fori_loop(0, count, body, 0)


def row_plan(kind, width, s_send, s_recv):
    if kind == "x":
        own = (0, width - 1)
        need = (-1, width - 1) if s_recv == 0 else (0, width)
        src_at, dst_at = 2 - s_send, 2 - s_recv
    elif kind == "y":
        own = (s_send, width - 1 + s_send)
        need = (s_recv - 1, s_recv + width)
        src_at, dst_at = 2 - s_send, 2 - s_recv
    else:
        own = (s_send, width - 1 + s_send)
        need = (-1, width - 1) if s_recv == 0 else (0, width + 1)
        src_at, dst_at = 3 - 2 * s_send, 3 - 2 * s_recv
    plan = []
    for dist in NEAR:
        lo = max(own[0], width * dist + need[0])
        hi = min(own[1], width * dist + need[1])
        if lo <= hi:
            plan.append((dist, lo + src_at, lo - width * dist + dst_at, hi - lo + 1, False))
        if kind != "x" and s_send == 1 and s_recv == 0 and dist >= 0 and need[0] + width * dist <= 0 <= need[1] + width * dist:
            plan.append((dist, src_at, dst_at - width * dist, 1, True))
    return plan


def kernel(dims, x_hbm, w1d_h, w1c_h, wp1_h, w2d_h, w2c_h, wp2_h, w3d_h, w3c_h, wp3_h, b1d_h, b1c_h, b2d_h, b2c_h, b3d_h, b3c_h, out_hbm,
           raw, xh, turned, eye, mix, xs, y1, z1, y2, z2, y3, zo, w1d, w1c, w2d, w2c, w3r, w3d, w3c, w3e, wp3r,
           b1d, b1c, b2d, b2c, b3d, b3c, load_sem, x_sem, col_send, col_recv, row_send, row_recv, out_sem):
    n, h, c0, c1, c2, c3, rows, cols = dims
    h4, h8 = h // 4, h // 8
    ch, ch3 = h4 // NCH, h8 // NCH3
    hh = h // 2
    row = lax.axis_index("row")
    col = lax.axis_index("col")
    s = lax.rem(row, 2)
    is0 = s == 0
    first_extra = (s == 1) & (col == 0)
    last_void = (s == 1) & (col == cols - 1)
    t_first = jnp.where(first_extra, -1, 0)
    fwd_col = jnp.where(is0, col + 1, col - 1)
    bwd_col = jnp.where(is0, col - 1, col + 1)
    has_fwd = (fwd_col >= 0) & (fwd_col < cols)
    has_bwd = (bwd_col >= 0) & (bwd_col < cols)

    load_count = []

    def load(src, dst):
        load_count.append(dst)
        return pltpu.make_async_copy(src, dst, load_sem.at[len(load_count) - 1])

    k1, k2 = 9 * c1, 9 * c2
    pair = 2 * c0
    x_loads = [load(x_hbm.at[:, q], raw.at[q]) for q in range(PAIRS)]
    w1d_loads = [load(b1d_h, b1d.at[0]), load(b1c_h, b1c.at[0])]
    w1c_loads = []
    for p in BOTH:
        lanes = pl.ds(p * c1, c1)
        for kh in range(3):
            w1d_loads.append(load(w1d_h.at[kh], w1d.at[pl.ds((kh + 2 * p) * 2 * pair + c0, 3 * c0), lanes]))
        w1c_loads.append(load(w1c_h, w1c.at[pl.ds(p * 3 * c1, k1), lanes]))
        w1c_loads.append(load(wp1_h, w1c.at[pl.ds(12 * c1 + p * pair, c0), lanes]))
    w2d_loads = [load(w2d_h, w2d), load(b2d_h, b2d.at[0])]
    w2c_loads = [load(w2c_h, w2c.at[pl.ds(0, k2)]), load(wp2_h, w2c.at[pl.ds(k2, c1)]), load(b2c_h, b2c.at[0])]
    w3d_loads = [load(w3d_h, w3r), load(b3d_h, b3d.at[0]), load(wp3_h, wp3r)]
    w3c_loads = [load(w3c_h.at[:, pl.ds(0, c2)], w3c), load(w3c_h.at[:, pl.ds(c2, c3 - c2)], w3e), load(b3c_h, b3c.at[0])]
    for copy in x_loads:
        copy.start()

    def row_refs(name, slots, down, side):
        ref = refs[name]
        last = ref.shape[1] - (2 if ROW_SEM[name][0] == "y" else 1)
        own_at, halo_at = (last, 0) if down else (1, last + 1)
        at = own_at if side == OWN else halo_at
        subs = 1 if len(ref.shape) == 4 else ref.shape[2]
        if subs == 1:
            return ref.at[slots, at]
        return ref.at[slots, at, subs - 1 if down else 0]

    refs = dict(x=xs, y1=y1, z1=z1, y2=y2, z2=z2, y3=y3)
    ROW_SEM = {}
    for name, kind, width in (("x", "x", PAIRS), ("y1", "y", PAIRS), ("z1", "z", PAIRS), ("y2", "y", 2), ("z2", "z", 2), ("y3", "y", 1)):
        ROW_SEM[name] = (kind, width, 2 * MAX_PLAN * len(ROW_SEM))

    def directions(name):
        return (True, False) if ROW_SEM[name][0] == "y" else (True,)

    def dot(lhs, rhs):
        return jnp.dot(lhs, rhs, preferred_element_type=F32)

    def zero_slot(ref, idx):
        ref[idx] = jnp.zeros(ref.shape[1:], ref.dtype)

    def dot(lhs, rhs):
        return jnp.dot(lhs, rhs, preferred_element_type=F32)

    def zero_slot(ref, idx):
        def body(i, carry):
            ref[idx, i] = jnp.zeros(ref.shape[2:], ref.dtype)
            return carry
        loop(ref.shape[1], body)

    for name in ROW_SEM:
        for down in directions(name):
            edge = row_refs(name, slice(None), down, HALO)
            edge[...] = jnp.zeros(edge.shape, BF16)

    @pl.when(col == cols - 1)
    def _():
        for ref in (y1, y2, y3):
            zero_slot(ref, ref.shape[0] - 1)

    barrier = pltpu.get_barrier_semaphore()
    around = 0
    for step in range(-1, 2):
        for dist in NEAR:
            near_row, near_col = row + step, col + dist
            ok = (near_row >= 0) & (near_row < rows) & (near_col >= 0) & (near_col < cols)
            around = around + ok.astype(jnp.int32)

            @pl.when(ok)
            def _():
                pl.semaphore_signal(barrier, inc=1, device_id={"row": near_row, "col": near_col}, device_id_type=pl.DeviceIdType.MESH)

    @pl.when(col == 0)
    def _():
        for ref in (y1, y2, y3):
            zero_slot(ref, 1 - s)
        for ref in (z1, z2):
            zero_slot(ref, 2 - 2 * s)

    @pl.when(first_extra)
    def _():
        zero_slot(xs, 0)

    def zero_xh(first, size):
        def body(i, carry):
            for half in BOTH:
                xh[half, i, pl.ds(first, size)] = jnp.zeros((size, hh), BF16)
            return carry
        loop(n, body)

    @pl.when(is0)
    def _():
        zero_xh(0, c0)

    @pl.when(jnp.logical_not(has_bwd))
    def _():
        zero_xh(0, pair)

    def unit_where(size, source):
        at = lax.broadcasted_iota(jnp.int32, (size, size), 0)
        return (at == source(lax.broadcasted_iota(jnp.int32, (size, size), 1))).astype(F32).astype(BF16)

    eye[...] = unit_where(h, lambda at: at)
    mix[...] = unit_where(n * BLOCK, lambda at: (at & (BLOCK - 1)) * n + (at >> BLOCK.bit_length() - 1))

    def zero_part(ref, first, size, p):
        ref[pl.ds(first, size), pl.ds(p * c1, c1)] = jnp.zeros((size, c1), BF16)

    for p in BOTH:
        for kh in range(5):
            tap_at = kh * 2 * pair
            used = 2 * p <= kh < 2 * p + 3
            zero_part(w1d, tap_at, c0 if used else 2 * pair, p)
        zero_part(w1c, (1 - p) * k1, 3 * c1, p)
        proj_at = 12 * c1
        zero_part(w1c, proj_at + (1 - p) * pair, pair, p)
        zero_part(w1c, proj_at + p * pair + c0, c0, p)
    for copy in x_loads:
        copy.wait()
    pl.semaphore_wait(barrier, around)

    def remote(src, dst, send_sem, recv_sem, to_row, to_col):
        return pltpu.make_async_remote_copy(src_ref=src, dst_ref=dst, send_sem=send_sem, recv_sem=recv_sem,
                                            device_id={"row": to_row, "col": to_col}, device_id_type=pl.DeviceIdType.MESH)

    def x_copy(shift, half):
        lanes = pl.ds(half * hh, hh)
        if shift == 0:
            src, dst = raw.at[PAIRS - 1, :, pl.ds(c0, c0), lanes], xh.at[half, :, pl.ds(c0, c0)]
        else:
            src, dst = raw.at[0, :, :, lanes], xh.at[half]
        return remote(src, dst, x_sem.at[half], x_sem.at[2 + half], row, fwd_col)

    for shift in SHIFTS:
        @pl.when(has_fwd & (s == shift))
        def _():
            for half in BOTH:
                x_copy(shift, half).start()

    def y_copy(ref, width, rows_per, sem0, forward, chunk, nch):
        to_right = is0 if forward else jnp.logical_not(is0)
        src_slot = jnp.where(to_right, width + 1, 2)
        dst_slot = jnp.where(to_right, 1, width + 2)
        part = pl.ds(1 + chunk * rows_per, rows_per)
        sem = sem0 + (0 if forward else nch) + chunk
        return remote(ref.at[src_slot, part], ref.at[dst_slot, part], col_send.at[sem], col_recv.at[sem], row, fwd_col if forward else bwd_col)

    def y_recv(ref, width, rows_per, sem0, forward, chunk, nch):
        to_right = is0 if forward else jnp.logical_not(is0)
        dst_slot = jnp.where(to_right, 1, width + 2)
        part = pl.ds(1 + chunk * rows_per, rows_per)
        sem = sem0 + (0 if forward else nch) + chunk
        return remote(ref.at[dst_slot, part], ref.at[dst_slot, part], col_send.at[sem], col_recv.at[sem], row, bwd_col if forward else fwd_col)

    def z_copy(ref, width, rows_per, sem0, chunk):
        src_slot = jnp.where(is0, width + 2, 2)
        dst_slot = jnp.where(is0, 2, width + 2)
        part = pl.ds(1 + chunk * rows_per, rows_per)
        sem = sem0 + chunk
        return remote(ref.at[src_slot, part], ref.at[dst_slot, part], col_send.at[sem], col_recv.at[sem], row, fwd_col)

    def z_recv(ref, width, rows_per, sem0, chunk):
        dst_slot = jnp.where(is0, 2, width + 2)
        part = pl.ds(1 + chunk * rows_per, rows_per)
        sem = sem0 + chunk
        return remote(ref.at[dst_slot, part], ref.at[dst_slot, part], col_send.at[sem], col_recv.at[sem], row, bwd_col)

    SEM_Y1, SEM_Z1, SEM_Y2, SEM_Z2, SEM_Y3 = (i * 2 * NCH for i in range(5))

    def row_messages(name, act, ways=None):
        kind, width, sem0 = ROW_SEM[name]
        for down in ways or directions(name):
            for s_send, s_recv in zip(SHIFTS, reversed(SHIFTS)):
                step = 1 if down else -1
                for i, (dist, src, dst, count, extra) in enumerate(row_plan(kind, width, s_send, s_recv)):
                    sem = sem0 + i + (0 if down else MAX_PLAN)
                    if act == "recv":
                        from_row, from_col = row - step, col - dist
                        ok = (s == s_recv) & (from_row >= 0) & (from_row < rows) & (from_col >= 0) & (from_col < cols)
                        if extra:
                            ok = ok & (from_col == 0)

                        @pl.when(ok)
                        def _():
                            ref = row_refs(name, pl.ds(dst, count), down, HALO)
                            remote(ref, ref, row_send.at[sem], row_recv.at[sem], from_row, from_col).wait_recv()
                    else:
                        to_row, to_col = row + step, col + dist
                        ok = (s == s_send) & (to_row >= 0) & (to_row < rows) & (to_col >= 0) & (to_col < cols)
                        if extra:
                            ok = ok & (col == 0)

                        @pl.when(ok)
                        def _():
                            copy = remote(row_refs(name, pl.ds(src, count), down, OWN), row_refs(name, pl.ds(dst, count), down, HALO),
                                          row_send.at[sem], row_recv.at[sem], to_row, to_col)
                            if act == "send":
                                copy.start()
                            else:
                                copy.wait_send()

    def send_edges(name, chunk, nch):
        @pl.when(chunk == 0)
        def _():
            row_messages(name, "send", UP)

        @pl.when(chunk == nch - 1)
        def _():
            row_messages(name, "send", DOWN)

    def to_rows(value):
        return value.astype(BF16).reshape(BLOCK // 4, 4, n, pair)

    def turn_group(q):
        def turn(i, carry):
            for j in range(UNROLL):
                at = i * UNROLL + j
                block = raw[pl.ds(q, 2), at].reshape(2 * pair, h)
                turned[at] = lax.dot_general(eye[...], block, NT, preferred_element_type=F32).astype(BF16)
            return carry
        loop(n // UNROLL, turn)

        def place(i, carry):
            for j in range(UNROLL):
                at = i * UNROLL + j
                block = turned[:, pl.ds(at * BLOCK, BLOCK), :].reshape(n * BLOCK, 2 * pair)
                moved = dot(mix[...], block)
                for side in BOTH:
                    xs[q + 2 - s + side, pl.ds(1 + at * (BLOCK // 4), BLOCK // 4)] = to_rows(moved[:, side * pair:(side + 1) * pair])
            return carry
        loop(h // BLOCK // UNROLL, place)

    def turn_halo(half):
        slot = jnp.where(is0, 1, PAIRS + 1)
        unit = eye[:hh, :hh]
        many = min(UNROLL, n // 2)

        def turn(i, carry):
            for j in range(many):
                at = 2 * (i * many + j)
                block = xh[half, pl.ds(at, 2)].reshape(2 * pair, hh)
                both = lax.dot_general(unit, block, NT, preferred_element_type=F32).astype(BF16)
                for side in BOTH:
                    turned[at + side, :hh, :pair] = both[:, side * pair:(side + 1) * pair]
            return carry
        loop(n // 2 // many, turn)

        def place(i):
            blocks = [turned[:, pl.ds((2 * i + j) * BLOCK, BLOCK), :pair].reshape(n * BLOCK, pair) for j in BOTH]
            moved = dot(mix[...], jnp.concatenate(blocks, axis=1))
            for j in BOTH:
                first = 1 + half * (h4 // 2) + (2 * i + j) * (BLOCK // 4)
                xs[slot, pl.ds(first, BLOCK // 4)] = to_rows(moved[:, j * pair:(j + 1) * pair])
        for i in range(hh // BLOCK // 2):
            place(i)

    for copy in w1d_loads + w1c_loads + w2d_loads + w2c_loads + w3d_loads + w3c_loads:
        copy.start()

    def flat(value):
        return value.reshape(value.shape[0] * n, value.shape[-1])

    def parts(first, count):
        size = count // 2
        return tuple((first + i * size, size) for i in BOTH)

    def dot_nt(lhs, rhs):
        return lax.dot_general(lhs, rhs, NT, preferred_element_type=F32)

    def rows_down(at):
        return (at - 1, 1), (at, 0), (at, 1)

    def whole(c):
        return ((1 + c * ch3, ch3),)

    def own_col(t, width):
        return jnp.where(is0, width - 1 - t, t)

    def phase(width, nch, item):
        def body(at, carry):
            item(lax.div(at, nch) - 1, lax.rem(at, nch))
            return carry
        lax.fori_loop((t_first + 1) * nch, (width + 1) * nch, body, 0)

    def y1_job(t, c):
        k = own_col(t, PAIRS)
        at = 1 + c * ch
        taps = []
        for kh in range(5):
            first, sub = (at - 1, 3) if kh == 0 else (at, kh - 1)
            for side in (1, 2):
                taps.append(flat(xs[k + side, pl.ds(first, ch), sub]))
        acc = dot(jnp.concatenate(taps, axis=1), w1d[...])
        void = last_void & (t == 3)
        for p in BOTH:
            val = relu(acc[:, p * c1:(p + 1) * c1] + b1d[...])
            val = jnp.where(void, 0.0, val)
            y1[k + 2, pl.ds(at, ch), p] = val.astype(BF16).reshape(ch, n, c1)

    def own_group(group, carry):
        turn_group(2 * group)
        return carry
    loop(PAIRS // 2, own_group)
    row_messages("x", "send")
    for copy in w1d_loads:
        copy.wait()
    def turn_weight(i, carry):
        for j in range(3):
            tap = 3 * i + j
            w3d[tap] = dot_nt(eye[:c2, :c2], w3r[tap]).astype(BF16)
        return carry

    def turn_weights():
        for copy in w3d_loads:
            copy.wait()
        loop(3, turn_weight)

    early = 3 - t_first

    def y1_item(item, carry):
        @pl.when(item == lax.div(3 * early, 2))
        def _():
            row_messages("x", "recv")

        half = item - 2 * early

        @pl.when(half >= 0)
        def _():
            for shift in SHIFTS:
                @pl.when(has_bwd & (s == shift))
                def _():
                    ref = xh.at[half, :, pl.ds(c0, c0)] if shift == 0 else xh.at[half]
                    remote(ref, ref, x_sem.at[half], x_sem.at[2 + half], row, bwd_col).wait_recv()
            turn_halo(half)

        jobs = []
        for j in BOTH:
            at = 2 * item + j
            t = jnp.where(at < 3 * early, lax.div(at, 3) + t_first, jnp.where(half >= 0, 3, at - 3 * early + t_first))
            c = jnp.where(at < 3 * early, lax.rem(at, 3) + 1, jnp.where(half >= 0, at - NCH * early, 0))
            jobs.append((t, c))
        for t, c in jobs:
            y1_job(t, c)
        send_edges("y1", half, 2)

        for t, c in jobs:
            @pl.when((t == 0) & has_fwd)
            def _():
                y_copy(y1, PAIRS, ch, SEM_Y1, True, c, NCH).start()

            @pl.when((t == 3) & has_bwd)
            def _():
                y_copy(y1, PAIRS, ch, SEM_Y1, False, c, NCH).start()
        return carry
    loop(2 * (PAIRS - t_first), y1_item)
    for copy in w1c_loads:
        copy.wait()

    def wait_halo(ref, width, rows_per, sem0, forward, half, nch):
        exists = has_bwd if forward else has_fwd

        split = nch - nch // 4
        for part in BOTH:
            @pl.when(exists & (half == part))
            def _():
                for c in range(split, nch) if part else range(split):
                    y_recv(ref, width, rows_per, sem0, forward, c, nch).wait_recv()

    def z1_job(t, c):
        k = own_col(t, PAIRS)
        at = 1 + c * ch
        taps = []
        for first, sub in ((at - 1, 1), (at, 0), (at, 1), (at + 1, 0)):
            for side in AROUND:
                taps.append(flat(y1[k + side, pl.ds(first, ch), sub]))
        for sub in (0, 2):
            taps.append(flat(xs[k + 2, pl.ds(at, ch), sub]))
        acc = dot(jnp.concatenate(taps, axis=1), w1c[...])
        for p in BOTH:
            val = relu(acc[:, p * c1:(p + 1) * c1] + b1c[...])
            z1[k + 3 - s, pl.ds(at, ch), p] = val.astype(BF16).reshape(ch, n, c1)

    extra = -t_first

    def z1_item(item, carry):
        inner = item - extra
        edge = inner - NCH - extra
        more = (inner < 0) | (extra == 1) & (inner == NCH)

        @pl.when(inner == 2)
        def _():
            row_messages("y1", "recv")

        half = lax.rem(edge, 2)
        far = edge >= 2

        @pl.when((edge == 0) & is0)
        def _():
            turn_weights()

        @pl.when((edge >= 0) & (edge < 2))
        def _():
            wait_halo(y1, PAIRS, ch, SEM_Y1, False, half, NCH)

        @pl.when(far)
        def _():
            wait_halo(y1, PAIRS, ch, SEM_Y1, True, half, NCH)

        mid = jnp.where(inner < 2, inner + 1, jnp.where(inner == 2, 0, inner))
        edge_col = jnp.where(far, 3, 0)
        for j in BOTH:
            t = jnp.where(more, -1, jnp.where(edge >= 0, edge_col, j + 1))
            c = jnp.where(more, jnp.where(inner < 0, j + 1, 3 * j), jnp.where(edge >= 0, 2 * half + j, mid))
            z1_job(t, c)

        @pl.when((edge >= 0) & (edge < 2) & has_fwd)
        def _():
            for j in BOTH:
                z_copy(z1, PAIRS, ch, SEM_Z1, 2 * half + j).start()
        return carry
    loop(2 * (NCH + extra), z1_item)
    row_messages("z1", "send")
    for copy in w2d_loads:
        copy.wait()

    def y2_job(t, at, size):
        k = own_col(t, 2)
        taps = []
        for first, sub in rows_down(at):
            for side in range(3):
                taps.append(flat(z1[2 * k + 2 + side, pl.ds(first, size), sub]))
        acc = dot(jnp.concatenate(taps, axis=1), w2d[...])
        val = relu(acc + b2d[...])
        val = jnp.where(last_void & (t == 1), 0.0, val)
        y2[k + 2, pl.ds(at, size)] = val.astype(BF16).reshape(size, n, c2)

    def y2_inner(item, carry):
        t = t_first + lax.div(item, 2)
        late = lax.rem(item, 2)

        @pl.when(item == 1)
        def _():
            row_messages("z1", "recv")

        chunks = (1 + 2 * late, 2 - 2 * late)
        for c in chunks:
            y2_job(t, 1 + c * ch, ch)

        @pl.when((t == 0) & has_fwd)
        def _():
            for c in chunks:
                y_copy(y2, 2, ch, SEM_Y2, True, c, NCH).start()
        return carry
    loop(2 + 2 * extra, y2_inner)

    def y2_edge(c, carry):
        @pl.when(has_bwd)
        def _():
            z_recv(z1, PAIRS, ch, SEM_Z1, c).wait_recv()

        for at, size in parts(1 + c * ch, ch):
            y2_job(jnp.int32(1), at, size)

        send_edges("y2", c, NCH)

        @pl.when(has_bwd)
        def _():
            y_copy(y2, 2, ch, SEM_Y2, False, c, NCH).start()
        return carry
    loop(NCH, y2_edge)
    for copy in w2c_loads:
        copy.wait()

    def z2_job(t, c):
        k = own_col(t, 2)
        at = 1 + c * ch
        taps = []
        for first in (at - 1, at, at + 1):
            for side in AROUND:
                taps.append(flat(y2[k + side, pl.ds(first, ch)]))
        taps.append(flat(z1[2 * k + 3, pl.ds(at, ch), 0]))
        acc = dot(jnp.concatenate(taps, axis=1), w2c[...])
        val = relu(acc + b2c[...]).astype(BF16).reshape(ch // 2, 2, n, c2)
        z2[k + 3 - s, pl.ds(1 + c * (ch // 2), ch // 2)] = val

    @pl.when(jnp.logical_not(is0))
    def _():
        turn_weights()

    row_messages("y2", "recv")

    def z2_item(item, carry):
        edge = item - 2 * extra
        half = lax.rem(item, 2)
        near = (edge >= 0) & (edge < 2)

        @pl.when(near)
        def _():
            wait_halo(y2, 2, ch, SEM_Y2, False, half, NCH)

        @pl.when(edge >= 2)
        def _():
            wait_halo(y2, 2, ch, SEM_Y2, True, half, NCH)

        for j in BOTH:
            z2_job(lax.div(edge + 2, 2) - 1, 2 * half + j)

        @pl.when(near & has_fwd)
        def _():
            for j in BOTH:
                z_copy(z2, 2, ch // 2, SEM_Z2, 2 * half + j).start()
        return carry
    loop(NCH + 2 * extra, z2_item)
    row_messages("z2", "send")

    def y3_item(t, c):
        k = t

        @pl.when((t == t_first) & (c == 0))
        def _():
            row_messages("z2", "recv")

        @pl.when((t == 0) & has_bwd)
        def _():
            for j in range(NCH // NCH3):
                z_recv(z2, 2, ch // 2, SEM_Z2, c * (NCH // NCH3) + j).wait_recv()

        for at, size in whole(c):
            taps = [flat(z2[2 * k + 2 + side, pl.ds(first, size), sub]) for first, sub in rows_down(at) for side in range(3)]
            acc = dot(jnp.concatenate(taps, axis=1), w3d[...].reshape(k2, c3)) + b3d[...]
            val = jnp.where(last_void & (t == 0), 0.0, relu(acc))
            y3[k + 2, pl.ds(at, size)] = val.astype(BF16).reshape(size, n, c3)

        @pl.when(t == 0)
        def _():
            send_edges("y3", c, NCH3)

        @pl.when((t == 0) & has_fwd)
        def _():
            y_copy(y3, 1, ch3, SEM_Y3, True, c, NCH3).start()

        @pl.when((t == 0) & has_bwd)
        def _():
            y_copy(y3, 1, ch3, SEM_Y3, False, c, NCH3).start()
    phase(1, NCH3, y3_item)
    for copy in w3c_loads:
        copy.wait()

    ships = (s == 1) & has_bwd
    low, mid = ch3 - 1, ch3 // 2
    z3_parts = ((0, low), (low, mid), (low + mid, mid + 1))
    n_parts = len(z3_parts)

    def ship(c, to_col):
        part = pl.ds(*z3_parts[c])
        return remote(zo.at[1, part], out_hbm.at[part], out_sem.at[c], out_sem.at[n_parts + c], row, to_col)

    keep = jnp.where(is0, 1, 0)

    def put(c):
        part = pl.ds(*z3_parts[c])
        return pltpu.make_async_copy(zo.at[keep, part], out_hbm.at[part], out_sem.at[2 * n_parts + c])

    def z3_col(i, carry):
        k = t_first + i

        @pl.when(i == 0)
        def _():
            row_messages("y3", "recv")

        for c, (first, size) in enumerate(z3_parts):
            if c < NCH3:
                @pl.when(k == 0)
                def _():
                    for forward, exists in ((False, has_fwd), (True, has_bwd)):
                        @pl.when(exists)
                        def _():
                            y_recv(y3, 1, ch3, SEM_Y3, forward, c, NCH3).wait_recv()

            acc = dot_nt(flat(z2[2 * k + 3, pl.ds(1 + first, size), 0]), wp3r[...]) + b3c[...]
            taps = [flat(y3[k + side, pl.ds(first + down, size)]) for down in range(3) for side in AROUND]
            acc = acc + dot(jnp.concatenate([tap[:, :c2] for tap in taps], axis=1), w3c[...].reshape(k2, c3))
            acc = acc + dot(jnp.concatenate([tap[:, c2:] for tap in taps], axis=1), w3e[...].reshape(9 * (c3 - c2), c3))
            zo[k + 1, pl.ds(first, size)] = relu(acc).astype(BF16).reshape(size, n, c3)

            @pl.when((k == 0) & ships)
            def _():
                ship(c, bwd_col).start()

            @pl.when(((k == 0) & is0) | (k == -1))
            def _():
                put(c).start()
        return carry
    loop(1 + extra, z3_col)

    for shift in SHIFTS:
        @pl.when(has_fwd & (s == shift))
        def _():
            for half in BOTH:
                x_copy(shift, half).wait_send()

    def drain(c, carry):
        @pl.when(has_fwd)
        def _():
            y_copy(y1, PAIRS, ch, SEM_Y1, True, c, NCH).wait_send()
            z_copy(z1, PAIRS, ch, SEM_Z1, c).wait_send()
            y_copy(y2, 2, ch, SEM_Y2, True, c, NCH).wait_send()
            z_copy(z2, 2, ch // 2, SEM_Z2, c).wait_send()

        @pl.when(has_bwd)
        def _():
            y_copy(y1, PAIRS, ch, SEM_Y1, False, c, NCH).wait_send()
            y_copy(y2, 2, ch, SEM_Y2, False, c, NCH).wait_send()
        return carry
    loop(NCH, drain)

    def drain3(c):
        @pl.when(has_fwd)
        def _():
            y_copy(y3, 1, ch3, SEM_Y3, True, c, NCH3).wait_send()

        @pl.when(has_bwd)
        def _():
            y_copy(y3, 1, ch3, SEM_Y3, False, c, NCH3).wait_send()
    for c in range(NCH3):
        drain3(c)

    def drain_out(c):
        @pl.when(ships)
        def _():
            ship(c, bwd_col).wait_send()

        @pl.when((s == 1) & has_fwd)
        def _():
            ship(c, fwd_col).wait_recv()

        @pl.when(is0 | first_extra)
        def _():
            put(c).wait()
    for c in range(n_parts):
        drain_out(c)
    for name in ROW_SEM:
        row_messages(name, "sent")


def solution(mesh):
    rows = mesh.shape["row"]
    cols = mesh.shape["col"]
    tile_spec = P("batch", "row", "col")

    def local_blocks(x, w1d, b1d, w1c, b1c, wp1, w2d, b2d, w2c, b2c, wp2, w3d, b3d, w3c, b3c, wp3):
        n, h, w, c0 = x.shape
        c1, c2, c3 = w1d.shape[3], w2d.shape[3], w3d.shape[3]
        h4, h8 = h // 4, h // 8
        dims = (n, h, c0, c1, c2, c3, rows, cols)
        pair = 2 * c0
        xt = jnp.moveaxis(x, 1, 3).reshape(n, PAIRS, pair, h)
        args = (xt, w1d.reshape(3, 3 * c0, c1), w1c.reshape(9 * c1, c1), wp1, w2d.reshape(9 * c1, c2), w2c.reshape(9 * c2, c2), wp2,
                jnp.swapaxes(w3d.reshape(9, c2, c3), 1, 2), w3c.reshape(9, c3, c3), wp3.T,
                b1d, b1c, b2d, b2c, b3d, b3c)
        vm = pltpu.VMEM
        dma = pltpu.SemaphoreType.DMA
        flops = 14 * x.size * (c0 + c1)
        out = pl.pallas_call(
            functools.partial(kernel, dims),
            out_shape=jax.ShapeDtypeStruct((h8, n, c3), BF16),
            in_specs=[pl.BlockSpec(memory_space=pl.ANY)] * len(args),
            out_specs=pl.BlockSpec(memory_space=pl.ANY),
            scratch_shapes=[
                vm(shape, BF16) for shape in (
                    (PAIRS, n, pair, h), (2, n, pair, h // 2), (n, h, 2 * pair), (h, h), (n * BLOCK, n * BLOCK),
                    (6, h4 + 1, 4, n, pair), (7, h4 + 2, 2, n, c1), (7, h4 + 1, 2, n, c1),
                    (5, h4 + 2, n, c2), (5, h8 + 1, 2, n, c2), (4, h8 + 2, n, c3), (2, h8, n, c3),
                    (10 * pair, 2 * c1), (12 * c1 + 2 * pair, 2 * c1), (9 * c1, c2), (9 * c2 + c1, c2),
                    (9, c3, c2), (9, c2, c3), (9, c2, c3), (9, c3 - c2, c3), (c3, c2))
            ] + [vm((1, width), F32) for width in (c1, c1, c2, c2, c3, c3)] + [
                dma((count,)) for count in (32, 4, 10 * NCH, 10 * NCH, 12 * MAX_PLAN, 12 * MAX_PLAN, 5 * NCH3)],
            compiler_params=pltpu.CompilerParams(collective_id=0, has_side_effects=True, vmem_limit_bytes=63 << 20),
            cost_estimate=pl.CostEstimate(flops=flops, bytes_accessed=x.size * 4, transcendentals=0),
        )(*args)
        return jnp.swapaxes(out, 0, 1).reshape(n, h8, 1, c3)

    return jax.shard_map(local_blocks, mesh=mesh, in_specs=(tile_spec,) + (P(),) * 15, out_specs=tile_spec, check_vma=False)
```

```python
import functools

import jax
import jax.numpy as jnp
from jax import lax
from jax.experimental import pallas as pl
from jax.experimental.pallas import tpu as pltpu
from jax.sharding import PartitionSpec as P

BF16 = jnp.bfloat16
F32 = jnp.float32
SHIFTS = (0, 1)
NCH = 4
NCH3 = 2
PAIRS = 4
MAX_PLAN = 5
BLOCK = 16
UNROLL = 8
OWN, HALO = BOTH = range(2)
AROUND = (1, 2, 3)
NEAR = range(-2, 3)
UP, DOWN = (False,), (True,)
NT = (((1,), (1,)), ((), ()))


def relu(value):
    return jnp.maximum(value, 0.0)


def loop(count, body):
    lax.fori_loop(0, count, body, 0)


def row_plan(kind, width, s_send, s_recv):
    if kind == "x":
        own = (0, width - 1)
        need = (-1, width - 1) if s_recv == 0 else (0, width)
        src_at, dst_at = 2 - s_send, 2 - s_recv
    elif kind == "y":
        own = (s_send, width - 1 + s_send)
        need = (s_recv - 1, s_recv + width)
        src_at, dst_at = 2 - s_send, 2 - s_recv
    else:
        own = (s_send, width - 1 + s_send)
        need = (-1, width - 1) if s_recv == 0 else (0, width + 1)
        src_at, dst_at = 3 - 2 * s_send, 3 - 2 * s_recv
    plan = []
    for dist in NEAR:
        lo = max(own[0], width * dist + need[0])
        hi = min(own[1], width * dist + need[1])
        if lo <= hi:
            plan.append((dist, lo + src_at, lo - width * dist + dst_at, hi - lo + 1, False))
        if kind != "x" and s_send == 1 and s_recv == 0 and dist >= 0 and need[0] + width * dist <= 0 <= need[1] + width * dist:
            plan.append((dist, src_at, dst_at - width * dist, 1, True))
    return plan


def kernel(dims, x_hbm, w1d_h, w1c_h, wp1_h, w2d_h, w2c_h, wp2_h, w3d_h, w3c_h, wp3_h, b1d_h, b1c_h, b2d_h, b2c_h, b3d_h, b3c_h, out_hbm,
           raw, xh, turned, eye, mix, xs, y1, z1, y2, z2, y3, zo, w1d, w1c, w2d, w2c, w3r, w3d, w3c, w3e, wp3r,
           b1d, b1c, b2d, b2c, b3d, b3c, load_sem, x_sem, col_send, col_recv, row_send, row_recv, out_sem):
    n, h, c0, c1, c2, c3, rows, cols = dims
    h4, h8 = h // 4, h // 8
    ch, ch3 = h4 // NCH, h8 // NCH3
    hh = h // 2
    row = lax.axis_index("row")
    col = lax.axis_index("col")
    s = lax.rem(row, 2)
    is0 = s == 0
    first_extra = (s == 1) & (col == 0)
    last_void = (s == 1) & (col == cols - 1)
    t_first = jnp.where(first_extra, -1, 0)
    fwd_col = jnp.where(is0, col + 1, col - 1)
    bwd_col = jnp.where(is0, col - 1, col + 1)
    has_fwd = (fwd_col >= 0) & (fwd_col < cols)
    has_bwd = (bwd_col >= 0) & (bwd_col < cols)

    load_count = []

    def load(src, dst):
        load_count.append(dst)
        return pltpu.make_async_copy(src, dst, load_sem.at[len(load_count) - 1])

    k1, k2 = 9 * c1, 9 * c2
    pair = 2 * c0
    x_loads = [load(x_hbm.at[:, q], raw.at[q]) for q in range(PAIRS)]
    w1d_loads = [load(b1d_h, b1d.at[0]), load(b1c_h, b1c.at[0])]
    w1c_loads = []
    for p in BOTH:
        lanes = pl.ds(p * c1, c1)
        for kh in range(3):
            w1d_loads.append(load(w1d_h.at[kh], w1d.at[pl.ds((kh + 2 * p) * 2 * pair + c0, 3 * c0), lanes]))
        w1c_loads.append(load(w1c_h, w1c.at[pl.ds(p * 3 * c1, k1), lanes]))
        w1c_loads.append(load(wp1_h, w1c.at[pl.ds(12 * c1 + p * pair, c0), lanes]))
    w2d_loads = [load(w2d_h, w2d), load(b2d_h, b2d.at[0])]
    w2c_loads = [load(w2c_h, w2c.at[pl.ds(0, k2)]), load(wp2_h, w2c.at[pl.ds(k2, c1)]), load(b2c_h, b2c.at[0])]
    w3d_loads = [load(w3d_h, w3r), load(b3d_h, b3d.at[0]), load(wp3_h, wp3r)]
    w3c_loads = [load(w3c_h.at[:, pl.ds(0, c2)], w3c), load(w3c_h.at[:, pl.ds(c2, c3 - c2)], w3e), load(b3c_h, b3c.at[0])]
    for copy in x_loads:
        copy.start()

    def row_refs(name, slots, down, side):
        ref = refs[name]
        last = ref.shape[1] - (2 if ROW_SEM[name][0] == "y" else 1)
        own_at, halo_at = (last, 0) if down else (1, last + 1)
        at = own_at if side == OWN else halo_at
        subs = 1 if len(ref.shape) == 4 else ref.shape[2]
        if subs == 1:
            return ref.at[slots, at]
        return ref.at[slots, at, subs - 1 if down else 0]

    refs = dict(x=xs, y1=y1, z1=z1, y2=y2, z2=z2, y3=y3)
    ROW_SEM = {}
    for name, kind, width in (("x", "x", PAIRS), ("y1", "y", PAIRS), ("z1", "z", PAIRS), ("y2", "y", 2), ("z2", "z", 2), ("y3", "y", 1)):
        ROW_SEM[name] = (kind, width, 2 * MAX_PLAN * len(ROW_SEM))

    def directions(name):
        return (True, False) if ROW_SEM[name][0] == "y" else (True,)

    def dot(lhs, rhs):
        return jnp.dot(lhs, rhs, preferred_element_type=F32)

    def zero_slot(ref, idx):
        ref[idx] = jnp.zeros(ref.shape[1:], ref.dtype)

    def dot(lhs, rhs):
        return jnp.dot(lhs, rhs, preferred_element_type=F32)

    def zero_slot(ref, idx):
        def body(i, carry):
            ref[idx, i] = jnp.zeros(ref.shape[2:], ref.dtype)
            return carry
        loop(ref.shape[1], body)

    for name in ROW_SEM:
        for down in directions(name):
            edge = row_refs(name, slice(None), down, HALO)
            edge[...] = jnp.zeros(edge.shape, BF16)

    @pl.when(col == cols - 1)
    def _():
        for ref in (y1, y2, y3):
            zero_slot(ref, ref.shape[0] - 1)

    barrier = pltpu.get_barrier_semaphore()
    around = 0
    for step in range(-1, 2):
        for dist in NEAR:
            near_row, near_col = row + step, col + dist
            ok = (near_row >= 0) & (near_row < rows) & (near_col >= 0) & (near_col < cols)
            around = around + ok.astype(jnp.int32)

            @pl.when(ok)
            def _():
                pl.semaphore_signal(barrier, inc=1, device_id={"row": near_row, "col": near_col}, device_id_type=pl.DeviceIdType.MESH)

    @pl.when(col == 0)
    def _():
        for ref in (y1, y2, y3):
            zero_slot(ref, 1 - s)
        for ref in (z1, z2):
            zero_slot(ref, 2 - 2 * s)

    @pl.when(first_extra)
    def _():
        zero_slot(xs, 0)

    def zero_xh(first, size):
        def body(i, carry):
            for half in BOTH:
                xh[half, i, pl.ds(first, size)] = jnp.zeros((size, hh), BF16)
            return carry
        loop(n, body)

    @pl.when(is0)
    def _():
        zero_xh(0, c0)

    @pl.when(jnp.logical_not(has_bwd))
    def _():
        zero_xh(0, pair)

    def unit_where(size, source):
        at = lax.broadcasted_iota(jnp.int32, (size, size), 0)
        return (at == source(lax.broadcasted_iota(jnp.int32, (size, size), 1))).astype(F32).astype(BF16)

    eye[...] = unit_where(h, lambda at: at)
    mix[...] = unit_where(n * BLOCK, lambda at: (at & (BLOCK - 1)) * n + (at >> BLOCK.bit_length() - 1))

    def zero_part(ref, first, size, p):
        ref[pl.ds(first, size), pl.ds(p * c1, c1)] = jnp.zeros((size, c1), BF16)

    for p in BOTH:
        for kh in range(5):
            tap_at = kh * 2 * pair
            used = 2 * p <= kh < 2 * p + 3
            zero_part(w1d, tap_at, c0 if used else 2 * pair, p)
        zero_part(w1c, (1 - p) * k1, 3 * c1, p)
        proj_at = 12 * c1
        zero_part(w1c, proj_at + (1 - p) * pair, pair, p)
        zero_part(w1c, proj_at + p * pair + c0, c0, p)
    for copy in x_loads:
        copy.wait()
    pl.semaphore_wait(barrier, around)

    def remote(src, dst, send_sem, recv_sem, to_row, to_col):
        return pltpu.make_async_remote_copy(src_ref=src, dst_ref=dst, send_sem=send_sem, recv_sem=recv_sem,
                                            device_id={"row": to_row, "col": to_col}, device_id_type=pl.DeviceIdType.MESH)

    def x_copy(shift, half):
        lanes = pl.ds(half * hh, hh)
        if shift == 0:
            src, dst = raw.at[PAIRS - 1, :, pl.ds(c0, c0), lanes], xh.at[half, :, pl.ds(c0, c0)]
        else:
            src, dst = raw.at[0, :, :, lanes], xh.at[half]
        return remote(src, dst, x_sem.at[half], x_sem.at[2 + half], row, fwd_col)

    for shift in SHIFTS:
        @pl.when(has_fwd & (s == shift))
        def _():
            for half in BOTH:
                x_copy(shift, half).start()

    def y_copy(ref, width, rows_per, sem0, forward, chunk, nch):
        to_right = is0 if forward else jnp.logical_not(is0)
        src_slot = jnp.where(to_right, width + 1, 2)
        dst_slot = jnp.where(to_right, 1, width + 2)
        part = pl.ds(1 + chunk * rows_per, rows_per)
        sem = sem0 + (0 if forward else nch) + chunk
        return remote(ref.at[src_slot, part], ref.at[dst_slot, part], col_send.at[sem], col_recv.at[sem], row, fwd_col if forward else bwd_col)

    def y_recv(ref, width, rows_per, sem0, forward, chunk, nch):
        to_right = is0 if forward else jnp.logical_not(is0)
        dst_slot = jnp.where(to_right, 1, width + 2)
        part = pl.ds(1 + chunk * rows_per, rows_per)
        sem = sem0 + (0 if forward else nch) + chunk
        return remote(ref.at[dst_slot, part], ref.at[dst_slot, part], col_send.at[sem], col_recv.at[sem], row, bwd_col if forward else fwd_col)

    def z_copy(ref, width, rows_per, sem0, chunk):
        src_slot = jnp.where(is0, width + 2, 2)
        dst_slot = jnp.where(is0, 2, width + 2)
        part = pl.ds(1 + chunk * rows_per, rows_per)
        sem = sem0 + chunk
        return remote(ref.at[src_slot, part], ref.at[dst_slot, part], col_send.at[sem], col_recv.at[sem], row, fwd_col)

    def z_recv(ref, width, rows_per, sem0, chunk):
        dst_slot = jnp.where(is0, 2, width + 2)
        part = pl.ds(1 + chunk * rows_per, rows_per)
        sem = sem0 + chunk
        return remote(ref.at[dst_slot, part], ref.at[dst_slot, part], col_send.at[sem], col_recv.at[sem], row, bwd_col)

    SEM_Y1, SEM_Z1, SEM_Y2, SEM_Z2, SEM_Y3 = (i * 2 * NCH for i in range(5))

    def row_messages(name, act, ways=None):
        kind, width, sem0 = ROW_SEM[name]
        for down in ways or directions(name):
            for s_send, s_recv in zip(SHIFTS, reversed(SHIFTS)):
                step = 1 if down else -1
                for i, (dist, src, dst, count, extra) in enumerate(row_plan(kind, width, s_send, s_recv)):
                    sem = sem0 + i + (0 if down else MAX_PLAN)
                    if act == "recv":
                        from_row, from_col = row - step, col - dist
                        ok = (s == s_recv) & (from_row >= 0) & (from_row < rows) & (from_col >= 0) & (from_col < cols)
                        if extra:
                            ok = ok & (from_col == 0)

                        @pl.when(ok)
                        def _():
                            ref = row_refs(name, pl.ds(dst, count), down, HALO)
                            remote(ref, ref, row_send.at[sem], row_recv.at[sem], from_row, from_col).wait_recv()
                    else:
                        to_row, to_col = row + step, col + dist
                        ok = (s == s_send) & (to_row >= 0) & (to_row < rows) & (to_col >= 0) & (to_col < cols)
                        if extra:
                            ok = ok & (col == 0)

                        @pl.when(ok)
                        def _():
                            copy = remote(row_refs(name, pl.ds(src, count), down, OWN), row_refs(name, pl.ds(dst, count), down, HALO),
                                          row_send.at[sem], row_recv.at[sem], to_row, to_col)
                            if act == "send":
                                copy.start()
                            else:
                                copy.wait_send()

    def send_edges(name, chunk, nch):
        @pl.when(chunk == 0)
        def _():
            row_messages(name, "send", UP)

        @pl.when(chunk == nch - 1)
        def _():
            row_messages(name, "send", DOWN)

    def to_rows(value):
        return value.astype(BF16).reshape(BLOCK // 4, 4, n, pair)

    def turn_group(q):
        def turn(i, carry):
            for j in range(UNROLL):
                at = i * UNROLL + j
                block = raw[pl.ds(q, 2), at].reshape(2 * pair, h)
                turned[at] = lax.dot_general(eye[...], block, NT, preferred_element_type=F32).astype(BF16)
            return carry
        loop(n // UNROLL, turn)

        def place(i, carry):
            for j in range(UNROLL):
                at = i * UNROLL + j
                block = turned[:, pl.ds(at * BLOCK, BLOCK), :].reshape(n * BLOCK, 2 * pair)
                moved = dot(mix[...], block)
                for side in BOTH:
                    xs[q + 2 - s + side, pl.ds(1 + at * (BLOCK // 4), BLOCK // 4)] = to_rows(moved[:, side * pair:(side + 1) * pair])
            return carry
        loop(h // BLOCK // UNROLL, place)

    def turn_halo(half):
        slot = jnp.where(is0, 1, PAIRS + 1)
        unit = eye[:hh, :hh]
        many = min(UNROLL, n // 2)

        def turn(i, carry):
            for j in range(many):
                at = 2 * (i * many + j)
                block = xh[half, pl.ds(at, 2)].reshape(2 * pair, hh)
                both = lax.dot_general(unit, block, NT, preferred_element_type=F32).astype(BF16)
                for side in BOTH:
                    turned[at + side, :hh, :pair] = both[:, side * pair:(side + 1) * pair]
            return carry
        loop(n // 2 // many, turn)

        def place(i):
            blocks = [turned[:, pl.ds((2 * i + j) * BLOCK, BLOCK), :pair].reshape(n * BLOCK, pair) for j in BOTH]
            moved = dot(mix[...], jnp.concatenate(blocks, axis=1))
            for j in BOTH:
                first = 1 + half * (h4 // 2) + (2 * i + j) * (BLOCK // 4)
                xs[slot, pl.ds(first, BLOCK // 4)] = to_rows(moved[:, j * pair:(j + 1) * pair])
        for i in range(hh // BLOCK // 2):
            place(i)

    for copy in w1d_loads + w1c_loads + w2d_loads + w2c_loads + w3d_loads + w3c_loads:
        copy.start()

    def flat(value):
        return value.reshape(value.shape[0] * n, value.shape[-1])

    def parts(first, count):
        size = count // 2
        return tuple((first + i * size, size) for i in BOTH)

    def dot_nt(lhs, rhs):
        return lax.dot_general(lhs, rhs, NT, preferred_element_type=F32)

    def rows_down(at):
        return (at - 1, 1), (at, 0), (at, 1)

    def whole(c):
        return ((1 + c * ch3, ch3),)

    def own_col(t, width):
        return jnp.where(is0, width - 1 - t, t)

    def phase(width, nch, item):
        def body(at, carry):
            item(lax.div(at, nch) - 1, lax.rem(at, nch))
            return carry
        lax.fori_loop((t_first + 1) * nch, (width + 1) * nch, body, 0)

    def y1_job(t, c):
        k = own_col(t, PAIRS)
        at = 1 + c * ch
        taps = []
        for kh in range(5):
            first, sub = (at - 1, 3) if kh == 0 else (at, kh - 1)
            for side in (1, 2):
                taps.append(flat(xs[k + side, pl.ds(first, ch), sub]))
        acc = dot(jnp.concatenate(taps, axis=1), w1d[...])
        void = last_void & (t == 3)
        for p in BOTH:
            val = relu(acc[:, p * c1:(p + 1) * c1] + b1d[...])
            val = jnp.where(void, 0.0, val)
            y1[k + 2, pl.ds(at, ch), p] = val.astype(BF16).reshape(ch, n, c1)

    def own_group(group, carry):
        turn_group(2 * group)
        return carry
    loop(PAIRS // 2, own_group)
    row_messages("x", "send")
    for copy in w1d_loads:
        copy.wait()
    def turn_weight(i, carry):
        for j in range(3):
            tap = 3 * i + j
            w3d[tap] = dot_nt(eye[:c2, :c2], w3r[tap]).astype(BF16)
        return carry

    def turn_weights():
        for copy in w3d_loads:
            copy.wait()
        loop(3, turn_weight)

    early = 3 - t_first

    def y1_item(item, carry):
        @pl.when(item == lax.div(3 * early, 2))
        def _():
            row_messages("x", "recv")

        half = item - 2 * early

        @pl.when(half >= 0)
        def _():
            for shift in SHIFTS:
                @pl.when(has_bwd & (s == shift))
                def _():
                    ref = xh.at[half, :, pl.ds(c0, c0)] if shift == 0 else xh.at[half]
                    remote(ref, ref, x_sem.at[half], x_sem.at[2 + half], row, bwd_col).wait_recv()
            turn_halo(half)

        jobs = []
        for j in BOTH:
            at = 2 * item + j
            t = jnp.where(at < 3 * early, lax.div(at, 3) + t_first, jnp.where(half >= 0, 3, at - 3 * early + t_first))
            c = jnp.where(at < 3 * early, lax.rem(at, 3) + 1, jnp.where(half >= 0, at - NCH * early, 0))
            jobs.append((t, c))
        for t, c in jobs:
            y1_job(t, c)
        send_edges("y1", half, 2)

        for t, c in jobs:
            @pl.when((t == 0) & has_fwd)
            def _():
                y_copy(y1, PAIRS, ch, SEM_Y1, True, c, NCH).start()

            @pl.when((t == 3) & has_bwd)
            def _():
                y_copy(y1, PAIRS, ch, SEM_Y1, False, c, NCH).start()
        return carry
    loop(2 * (PAIRS - t_first), y1_item)
    for copy in w1c_loads:
        copy.wait()

    def wait_halo(ref, width, rows_per, sem0, forward, half, nch):
        exists = has_bwd if forward else has_fwd

        split = nch - nch // 4
        for part in BOTH:
            @pl.when(exists & (half == part))
            def _():
                for c in range(split, nch) if part else range(split):
                    y_recv(ref, width, rows_per, sem0, forward, c, nch).wait_recv()

    def z1_job(t, c):
        k = own_col(t, PAIRS)
        at = 1 + c * ch
        taps = []
        for first, sub in ((at - 1, 1), (at, 0), (at, 1), (at + 1, 0)):
            for side in AROUND:
                taps.append(flat(y1[k + side, pl.ds(first, ch), sub]))
        for sub in (0, 2):
            taps.append(flat(xs[k + 2, pl.ds(at, ch), sub]))
        acc = dot(jnp.concatenate(taps, axis=1), w1c[...])
        for p in BOTH:
            val = relu(acc[:, p * c1:(p + 1) * c1] + b1c[...])
            z1[k + 3 - s, pl.ds(at, ch), p] = val.astype(BF16).reshape(ch, n, c1)

    extra = -t_first

    def z1_item(item, carry):
        inner = item - extra
        edge = inner - NCH - extra
        more = (inner < 0) | (extra == 1) & (inner == NCH)

        @pl.when(inner == 2)
        def _():
            row_messages("y1", "recv")

        half = lax.rem(edge, 2)
        far = edge >= 2

        @pl.when((edge == 0) & is0)
        def _():
            turn_weights()

        @pl.when((edge >= 0) & (edge < 2))
        def _():
            wait_halo(y1, PAIRS, ch, SEM_Y1, False, half, NCH)

        @pl.when(far)
        def _():
            wait_halo(y1, PAIRS, ch, SEM_Y1, True, half, NCH)

        mid = jnp.where(inner < 2, inner + 1, jnp.where(inner == 2, 0, inner))
        edge_col = jnp.where(far, 3, 0)
        for j in BOTH:
            t = jnp.where(more, -1, jnp.where(edge >= 0, edge_col, j + 1))
            c = jnp.where(more, jnp.where(inner < 0, j + 1, 3 * j), jnp.where(edge >= 0, 2 * half + j, mid))
            z1_job(t, c)

        @pl.when((edge >= 0) & (edge < 2) & has_fwd)
        def _():
            for j in BOTH:
                z_copy(z1, PAIRS, ch, SEM_Z1, 2 * half + j).start()
        return carry
    loop(2 * (NCH + extra), z1_item)
    row_messages("z1", "send")
    for copy in w2d_loads:
        copy.wait()

    def y2_job(t, at, size):
        k = own_col(t, 2)
        taps = []
        for first, sub in rows_down(at):
            for side in range(3):
                taps.append(flat(z1[2 * k + 2 + side, pl.ds(first, size), sub]))
        acc = dot(jnp.concatenate(taps, axis=1), w2d[...])
        val = relu(acc + b2d[...])
        val = jnp.where(last_void & (t == 1), 0.0, val)
        y2[k + 2, pl.ds(at, size)] = val.astype(BF16).reshape(size, n, c2)

    def y2_inner(item, carry):
        t = t_first + lax.div(item, 2)
        late = lax.rem(item, 2)

        @pl.when(item == 1)
        def _():
            row_messages("z1", "recv")

        chunks = (1 + 2 * late, 2 - 2 * late)
        for c in chunks:
            y2_job(t, 1 + c * ch, ch)

        @pl.when((t == 0) & has_fwd)
        def _():
            for c in chunks:
                y_copy(y2, 2, ch, SEM_Y2, True, c, NCH).start()
        return carry
    loop(2 + 2 * extra, y2_inner)

    def y2_edge(c, carry):
        @pl.when(has_bwd)
        def _():
            z_recv(z1, PAIRS, ch, SEM_Z1, c).wait_recv()

        for at, size in parts(1 + c * ch, ch):
            y2_job(jnp.int32(1), at, size)

        send_edges("y2", c, NCH)

        @pl.when(has_bwd)
        def _():
            y_copy(y2, 2, ch, SEM_Y2, False, c, NCH).start()
        return carry
    loop(NCH, y2_edge)
    for copy in w2c_loads:
        copy.wait()

    def z2_job(t, c):
        k = own_col(t, 2)
        at = 1 + c * ch
        taps = []
        for first in (at - 1, at, at + 1):
            for side in AROUND:
                taps.append(flat(y2[k + side, pl.ds(first, ch)]))
        taps.append(flat(z1[2 * k + 3, pl.ds(at, ch), 0]))
        acc = dot(jnp.concatenate(taps, axis=1), w2c[...])
        val = relu(acc + b2c[...]).astype(BF16).reshape(ch // 2, 2, n, c2)
        z2[k + 3 - s, pl.ds(1 + c * (ch // 2), ch // 2)] = val

    @pl.when(jnp.logical_not(is0))
    def _():
        turn_weights()

    row_messages("y2", "recv")

    def z2_item(item, carry):
        edge = item - 2 * extra
        half = lax.rem(item, 2)
        near = (edge >= 0) & (edge < 2)

        @pl.when(near)
        def _():
            wait_halo(y2, 2, ch, SEM_Y2, False, half, NCH)

        @pl.when(edge >= 2)
        def _():
            wait_halo(y2, 2, ch, SEM_Y2, True, half, NCH)

        for j in BOTH:
            z2_job(lax.div(edge + 2, 2) - 1, 2 * half + j)

        @pl.when(near & has_fwd)
        def _():
            for j in BOTH:
                z_copy(z2, 2, ch // 2, SEM_Z2, 2 * half + j).start()
        return carry
    loop(NCH + 2 * extra, z2_item)
    row_messages("z2", "send")

    def y3_item(t, c):
        k = t

        @pl.when((t == t_first) & (c == 0))
        def _():
            row_messages("z2", "recv")

        @pl.when((t == 0) & has_bwd)
        def _():
            for j in range(NCH // NCH3):
                z_recv(z2, 2, ch // 2, SEM_Z2, c * (NCH // NCH3) + j).wait_recv()

        for at, size in whole(c):
            taps = [flat(z2[2 * k + 2 + side, pl.ds(first, size), sub]) for first, sub in rows_down(at) for side in range(3)]
            acc = dot(jnp.concatenate(taps, axis=1), w3d[...].reshape(k2, c3)) + b3d[...]
            val = jnp.where(last_void & (t == 0), 0.0, relu(acc))
            y3[k + 2, pl.ds(at, size)] = val.astype(BF16).reshape(size, n, c3)

        @pl.when(t == 0)
        def _():
            send_edges("y3", c, NCH3)

        @pl.when((t == 0) & has_fwd)
        def _():
            y_copy(y3, 1, ch3, SEM_Y3, True, c, NCH3).start()

        @pl.when((t == 0) & has_bwd)
        def _():
            y_copy(y3, 1, ch3, SEM_Y3, False, c, NCH3).start()
    phase(1, NCH3, y3_item)
    for copy in w3c_loads:
        copy.wait()

    ships = (s == 1) & has_bwd
    low, mid = ch3 - 1, ch3 // 2
    z3_parts = ((0, low), (low, mid), (low + mid, mid + 1))
    n_parts = len(z3_parts)

    def ship(c, to_col):
        part = pl.ds(*z3_parts[c])
        return remote(zo.at[1, part], out_hbm.at[part], out_sem.at[c], out_sem.at[n_parts + c], row, to_col)

    keep = jnp.where(is0, 1, 0)

    def put(c):
        part = pl.ds(*z3_parts[c])
        return pltpu.make_async_copy(zo.at[keep, part], out_hbm.at[part], out_sem.at[2 * n_parts + c])

    def z3_col(i, carry):
        k = -i

        @pl.when(i == 0)
        def _():
            row_messages("y3", "recv")

        for c, (first, size) in enumerate(z3_parts):
            if c < NCH3:
                @pl.when(k == 0)
                def _():
                    for forward, exists in ((False, has_fwd), (True, has_bwd)):
                        @pl.when(exists)
                        def _():
                            y_recv(y3, 1, ch3, SEM_Y3, forward, c, NCH3).wait_recv()

            acc = dot_nt(flat(z2[2 * k + 3, pl.ds(1 + first, size), 0]), wp3r[...]) + b3c[...]
            taps = [flat(y3[k + side, pl.ds(first + down, size)]) for down in range(3) for side in AROUND]
            acc = acc + dot(jnp.concatenate([tap[:, :c2] for tap in taps], axis=1), w3c[...].reshape(k2, c3))
            acc = acc + dot(jnp.concatenate([tap[:, c2:] for tap in taps], axis=1), w3e[...].reshape(9 * (c3 - c2), c3))
            zo[k + 1, pl.ds(first, size)] = relu(acc).astype(BF16).reshape(size, n, c3)

            @pl.when((k == 0) & ships)
            def _():
                ship(c, bwd_col).start()

            @pl.when(((k == 0) & is0) | (k == -1))
            def _():
                put(c).start()
        return carry
    loop(1 + extra, z3_col)

    for shift in SHIFTS:
        @pl.when(has_fwd & (s == shift))
        def _():
            for half in BOTH:
                x_copy(shift, half).wait_send()

    def drain(c, carry):
        @pl.when(has_fwd)
        def _():
            y_copy(y1, PAIRS, ch, SEM_Y1, True, c, NCH).wait_send()
            z_copy(z1, PAIRS, ch, SEM_Z1, c).wait_send()
            y_copy(y2, 2, ch, SEM_Y2, True, c, NCH).wait_send()
            z_copy(z2, 2, ch // 2, SEM_Z2, c).wait_send()

        @pl.when(has_bwd)
        def _():
            y_copy(y1, PAIRS, ch, SEM_Y1, False, c, NCH).wait_send()
            y_copy(y2, 2, ch, SEM_Y2, False, c, NCH).wait_send()
        return carry
    loop(NCH, drain)

    def drain3(c):
        @pl.when(has_fwd)
        def _():
            y_copy(y3, 1, ch3, SEM_Y3, True, c, NCH3).wait_send()

        @pl.when(has_bwd)
        def _():
            y_copy(y3, 1, ch3, SEM_Y3, False, c, NCH3).wait_send()
    for c in range(NCH3):
        drain3(c)

    def drain_out(c):
        @pl.when(ships)
        def _():
            ship(c, bwd_col).wait_send()

        @pl.when((s == 1) & has_fwd)
        def _():
            ship(c, fwd_col).wait_recv()

        @pl.when(is0 | first_extra)
        def _():
            put(c).wait()
    for c in range(n_parts):
        drain_out(c)
    for name in ROW_SEM:
        row_messages(name, "sent")


def solution(mesh):
    rows = mesh.shape["row"]
    cols = mesh.shape["col"]
    tile_spec = P("batch", "row", "col")

    def local_blocks(x, w1d, b1d, w1c, b1c, wp1, w2d, b2d, w2c, b2c, wp2, w3d, b3d, w3c, b3c, wp3):
        n, h, w, c0 = x.shape
        c1, c2, c3 = w1d.shape[3], w2d.shape[3], w3d.shape[3]
        h4, h8 = h // 4, h // 8
        dims = (n, h, c0, c1, c2, c3, rows, cols)
        pair = 2 * c0
        xt = jnp.moveaxis(x, 1, 3).reshape(n, PAIRS, pair, h)
        args = (xt, w1d.reshape(3, 3 * c0, c1), w1c.reshape(9 * c1, c1), wp1, w2d.reshape(9 * c1, c2), w2c.reshape(9 * c2, c2), wp2,
                jnp.swapaxes(w3d.reshape(9, c2, c3), 1, 2), w3c.reshape(9, c3, c3), wp3.T,
                b1d, b1c, b2d, b2c, b3d, b3c)
        vm = pltpu.VMEM
        dma = pltpu.SemaphoreType.DMA
        flops = 14 * x.size * (c0 + c1)
        out = pl.pallas_call(
            functools.partial(kernel, dims),
            out_shape=jax.ShapeDtypeStruct((h8, n, c3), BF16),
            in_specs=[pl.BlockSpec(memory_space=pl.ANY)] * len(args),
            out_specs=pl.BlockSpec(memory_space=pl.ANY),
            scratch_shapes=[
                vm(shape, BF16) for shape in (
                    (PAIRS, n, pair, h), (2, n, pair, h // 2), (n, h, 2 * pair), (h, h), (n * BLOCK, n * BLOCK),
                    (6, h4 + 1, 4, n, pair), (7, h4 + 2, 2, n, c1), (7, h4 + 1, 2, n, c1),
                    (5, h4 + 2, n, c2), (5, h8 + 1, 2, n, c2), (4, h8 + 2, n, c3), (2, h8, n, c3),
                    (10 * pair, 2 * c1), (12 * c1 + 2 * pair, 2 * c1), (9 * c1, c2), (9 * c2 + c1, c2),
                    (9, c3, c2), (9, c2, c3), (9, c2, c3), (9, c3 - c2, c3), (c3, c2))
            ] + [vm((1, width), F32) for width in (c1, c1, c2, c2, c3, c3)] + [
                dma((count,)) for count in (32, 4, 10 * NCH, 10 * NCH, 12 * MAX_PLAN, 12 * MAX_PLAN, 5 * NCH3)],
            compiler_params=pltpu.CompilerParams(collective_id=0, has_side_effects=True, vmem_limit_bytes=63 << 20),
            cost_estimate=pl.CostEstimate(flops=flops, bytes_accessed=x.size * 4, transcendentals=0),
        )(*args)
        return jnp.swapaxes(out, 0, 1).reshape(n, h8, 1, c3)

    return jax.shard_map(local_blocks, mesh=mesh, in_specs=(tile_spec,) + (P(),) * 15, out_specs=tile_spec, check_vma=False)
```
